32 devices in a mesh: grp: 2 (over x), tp: 16 (over z, y, core).
Axes of the slice: x: 2, y: 2, z: 4, core: 2. Of those that a mesh axis runs over, the one named last changes fastest.
Arguments:
- hidden: bfloat16 [1024, 16384], P('grp', 'tp'), parts along dimension 0, may hold values from -36 to 36
- norm_gain: float32 [16384], P('tp'), may hold values from 0.3 to 10, as said below
- prefix: int32 [2], P('grp'), parts along dimension 0, may hold values from 0 to 8192
- w_query: bfloat16 [16384, 2048], P(None, 'tp'), may hold values from -0.046875 to 0.046875
- w_kv: bfloat16 [256, 16384], P('tp'), may hold values from -0.046875 to 0.046875
- w_scale: float32 [2304], P('tp'), may hold values from 0.25 to 4
Outputs:
- queries: bfloat16 [1024, 2048], P('grp', 'tp'), parts along dimension 0
- keys: bfloat16 [1024, 2048], P('grp', 'tp'), parts along dimension 0
- values: bfloat16 [1024, 2048], P('grp', 'tp'), parts along dimension 0
- payload: bfloat16 [1024, 16384], P('grp', 'tp'), parts along dimension 0
- row_scale: float32 [1024], P('grp'), parts along dimension 0
The draws below stay inside these ranges and needn't reach their ends.
There are 2 independent parts, one for each index of `grp`. The reference program is written for one: setup_inputs(seed, part) draws one part's arguments, and reference() takes and returns one part's arrays. A program takes and returns all parts, laid end to end along the dimension named above; an argument that names none is the same for every part. Nothing has to cross between parts.
Inputs may be any that keep to these rules, and one draw needn't show every extreme that they name: `norm_gain`: positive.
All inputs are finite; a program needn't handle non-finite values. Where the reference program divides by a largest or mean magnitude, that divisor is 1e-20 or more.
Results may differ from the reference program's by a relative error of at most 0.012.
Values may be sent and summed in bfloat16 or wider, within the bound.
A program may use at most 64 MiB of HBM per device.

```python
import math
import jax
import jax.numpy as jnp
from jax import lax

D = 16384
HD = 128
HQ_DEV = 1
KV_COLS_DEV = 8
TOKENS = 512
PREFIX_MAX = 8192
H = 16
KVH = 1
COLS_DEV = 144
N_TP = 16


def draw_norm_gain(key, part):
    columns = jnp.arange(D, dtype=jnp.float32)
    rising = 1.0 + 2.0 * columns / (D - 1)
    rough = jnp.exp(jax.random.uniform(key, (D,), jnp.float32, -0.7, 0.7))
    return rising * rough


def draw_hidden(key, part):
    columns = jnp.arange(D, dtype=jnp.float32) / (D - 1)
    noise = jax.random.normal(jax.random.fold_in(key, 11), (TOKENS, D), jnp.float32)
    noise = jnp.clip(noise, -6.0, 6.0)
    column_scale = 0.5 + columns
    values = noise * column_scale[None, :]
    return values.astype(jnp.bfloat16)


def steps_of(stream_key, shape, split, smallest, top_value):
    factor_of, own = 1.0, jax.random.fold_in(stream_key, 6)
    for position, blocks in split:
        steps = jnp.exp(jax.random.uniform(jax.random.fold_in(own, position), (blocks,), jnp.float32, smallest / len(split), top_value / len(split)))
        factor_of = factor_of * jnp.repeat(steps, shape[position] // blocks).reshape([-1 if axis == position else 1 for axis in range(len(shape))])
    return factor_of


def bell_draw(own_key, dims, scale, bound, shards=(), kind=jnp.bfloat16):
    level = steps_of(own_key, dims, shards, -0.22, 0.18) if shards else 1.0
    array = jax.random.normal(own_key, dims, jnp.float32) * scale * level
    return jnp.minimum(jnp.maximum(array, -bound), bound).astype(kind)


def setup_inputs(seed: int = 0, part: int = 0) -> dict:
    splits = jax.random.split(jax.random.key(seed), 7)
    part_keys = jax.random.split(jax.random.fold_in(splits[6], part), 7)
    return {
        "hidden": draw_hidden(jax.random.fold_in(jax.random.fold_in(splits[6], part), 71), part),
        "norm_gain": draw_norm_gain(jax.random.fold_in(splits[6], 71), part),
        "prefix": jax.random.randint(part_keys[2], (1,), 0, PREFIX_MAX + 1).astype(jnp.int32),
        "w_query": bell_draw(splits[3], (D, H * HD), D ** -0.5, 0.046875, ((1, 16),)),
        "w_kv": bell_draw(splits[4], (N_TP * 2 * KV_COLS_DEV, D), D ** -0.5, 0.046875, ((0, 16),)),
        "w_scale": jnp.clip(jnp.exp(math.log(4.0) - 2.7725887 * jax.random.uniform(splits[5], (N_TP * COLS_DEV,), jnp.float32) ** steps_of(splits[5], (N_TP * COLS_DEV,), ((0, 16),), -0.2, 0.2)), 0.25, 4.0),
    }


norm_eps = 1e-05
tiny_eps = 1e-06
rope_base = 500000.0

def rotate(matrix, positions, offset):
    count, width = matrix.shape
    pairs = matrix.reshape(count, width // 2, 2)
    columns = offset + 2 * jnp.arange(width // 2, dtype=jnp.int32)
    pair_index = (columns % HD // 2).astype(jnp.float32)
    inverse_freq = jnp.power(jnp.float32(rope_base), -(2.0 * pair_index) / HD)
    angle = positions.astype(jnp.float32)[:, None] * inverse_freq[None, :]
    cosine = jnp.cos(angle)
    sine = jnp.sin(angle)
    first = pairs[:, :, 0]
    second = pairs[:, :, 1]
    turned = jnp.stack([first * cosine - second * sine, second * cosine + first * sine], axis=-1)
    return turned.reshape(count, width)

def repeat_heads(matrix):
    heads = matrix.reshape(TOKENS, KVH, 1, HD)
    spread = jnp.broadcast_to(heads, (TOKENS, KVH, N_TP // KVH, HD)).reshape(TOKENS, N_TP, 1, HD)
    spread = jnp.broadcast_to(spread, (TOKENS, N_TP, HQ_DEV, HD))
    return spread.reshape(TOKENS, N_TP * HQ_DEV * HD)

def head_order(blocks):
    pieces = N_TP // KVH
    grouped = blocks.reshape(TOKENS, pieces, KVH, KV_COLS_DEV)
    return jnp.transpose(grouped, (0, 2, 1, 3)).reshape(TOKENS, KVH * HD)

def reference(hidden, norm_gain, prefix, w_query, w_kv, w_scale):
    widened = hidden.astype(jnp.float32)
    square_sum = lax.optimization_barrier(jnp.sum(widened * widened, axis=1))
    inverse = 1.0 / jnp.sqrt(square_sum / D + norm_eps)
    weighted = widened * norm_gain[None, :]
    normed = weighted * inverse[:, None]
    row_scale = lax.optimization_barrier(jnp.max(jnp.abs(normed), axis=1)) + tiny_eps
    payload = (normed / row_scale[:, None]).astype(jnp.bfloat16)
    qwidth = HQ_DEV * HD
    query_raw = jnp.dot(payload, w_query, preferred_element_type=jnp.float32)
    kv_raw = jnp.dot(payload, w_kv.T, preferred_element_type=jnp.float32)
    raw = jnp.concatenate([query_raw.reshape(TOKENS, N_TP, qwidth), kv_raw.reshape(TOKENS, N_TP, 2 * KV_COLS_DEV)], axis=2)
    blocks = raw * row_scale[:, None, None] * w_scale.reshape(1, N_TP, COLS_DEV)
    query_cols = blocks[:, :, :qwidth].reshape(TOKENS, N_TP * qwidth)
    key_cols = head_order(blocks[:, :, qwidth:qwidth + KV_COLS_DEV])
    value_cols = head_order(blocks[:, :, qwidth + KV_COLS_DEV:])
    positions = prefix[0] + jnp.arange(TOKENS, dtype=jnp.int32)
    queries = rotate(query_cols, positions, 0).astype(jnp.bfloat16)
    rotated_keys = rotate(key_cols, positions, 0).astype(jnp.bfloat16)
    value_round = value_cols.astype(jnp.bfloat16)
    keys = repeat_heads(rotated_keys)
    values = repeat_heads(value_round)
    return (queries, keys, values, payload, row_scale)
```

```python
import functools

import jax
import jax.numpy as jnp
import numpy as np
from jax import lax
from jax.experimental import pallas as pl
from jax.experimental.pallas import tpu as pltpu
from jax.sharding import PartitionSpec as P

HD = 128
KV_COLS_DEV = 8
norm_eps = 1e-05
tiny_eps = 1e-06
rope_base = 500000.0
PIECES = 2
GRID_PIECES = 4


def ring_order(chips):
    cols = 1
    while (2 * cols) * (2 * cols) <= chips and chips % (2 * cols) == 0:
        cols *= 2
    rows = chips // cols
    if cols < 2 or rows % 2:
        return list(range(chips))
    order = [0]
    for row in range(rows):
        span = range(1, cols) if row % 2 == 0 else range(cols - 1, 0, -1)
        order += [row * cols + col for col in span]
    order += [row * cols for row in range(rows - 1, 0, -1)]
    return order


def lookup(table, index):
    total = jnp.int32(0)
    for key, value in enumerate(table):
        total = total + jnp.where(index == key, jnp.int32(value), jnp.int32(0))
    return total


def spread(row):
    return jnp.transpose(jnp.broadcast_to(row, (128, 128)))


def kernel(
    n, width, prefix_ref, h_ref, gain_ref, freq_ref, qscale_ref, kvscale_ref, wq_hbm, wkv_hbm,
    q_out, k_out, v_out, payload_out, rs_out,
    gath, wq, wkv, acc, kvacc, part_q, part_kv, stat_own, stats, kv_own, kv_all, inv_col, cosine, sine,
    send_sem, recv_sem, st_send, st_recv, kv_send, kv_recv,
    wl_sem, wkl_sem, wr_send, wr_recv, wkr_send, wkr_recv, ex_send, ex_recv,
):
    me = lax.axis_index("tp")
    chips = n // 2
    core = lax.rem(me, 2)
    chip = me // 2
    mate = me + 1 - 2 * core
    count, depth = h_ref.shape
    half = count // 2
    rows = half // PIECES
    pieces = HD // KV_COLS_DEV
    kv_heads = n // pieces
    order = ring_order(chips)
    place = [order.index(c) for c in range(chips)]
    pos = lookup(place, chip)
    succ = 2 * lookup(order, lax.rem(pos + 1, chips)) + core
    pred = 2 * lookup(order, lax.rem(pos + chips - 1, chips)) + core

    barrier = pltpu.get_barrier_semaphore()

    def greet(d, carry):
        pl.semaphore_signal(barrier, inc=1, device_id={"tp": lax.rem(me + d, n)})
        return carry

    lax.fori_loop(1, n, greet, 0)

    own_wq = pltpu.make_async_copy(wq_hbm.at[:, core], wq.at[:, :, pl.ds(0, HD)], wl_sem)
    own_wq.start()

    def kv_local(k):
        cols = pl.ds(pl.multiple_of((2 * k + core) * depth, 128), depth)
        return pltpu.make_async_copy(wkv_hbm.at[:, cols], wkv.at[k, pl.ds(0, 16)], wkl_sem.at[k])

    def kv_remote(k):
        cols = pl.ds(pl.multiple_of((2 * k + 1 - core) * depth, 128), depth)
        return pltpu.make_async_remote_copy(
            wkv_hbm.at[:, cols], wkv.at[k, pl.ds(16, 16)], wkr_send.at[k], wkr_recv.at[k],
            device_id={"tp": mate},
        )

    mate_wq = pltpu.make_async_remote_copy(
        wq_hbm.at[:, 1 - core], wq.at[:, :, pl.ds(HD, HD)], wr_send, wr_recv, device_id={"tp": mate}
    )
    lax.fori_loop(0, chips, lambda k, c: (kv_local(k).start(), c)[1], 0)

    gain = gain_ref[...]
    for r in range(count // 128):
        block = pl.ds(r * 128, 128)
        wide = h_ref[block, :].astype(jnp.float32)
        weighted = wide * gain
        gath[0, block, :] = weighted.astype(jnp.bfloat16)
        square = jnp.sum(wide * wide, axis=1, keepdims=True)
        top = jnp.max(jnp.abs(weighted), axis=1, keepdims=True)
        stat_own[pl.ds(r, 1), :] = jnp.transpose(jnp.broadcast_to(square, (128, 128)))[0:1, :]
        stat_own[pl.ds(4 + r, 1), :] = jnp.transpose(jnp.broadcast_to(top, (128, 128)))[0:1, :]
    stats[me] = stat_own[...]

    pl.semaphore_wait(barrier, n - 1)

    def hop(step, way, piece):
        block = pl.ds(way * half + piece * rows, rows)
        return pltpu.make_async_remote_copy(
            gath.at[step, block], gath.at[step + 1, block],
            send_sem.at[step, way, piece], recv_sem.at[step, way, piece],
            device_id={"tp": succ if way == 0 else pred},
        )

    def multiply(step, way, piece):
        block = pl.ds(way * half + piece * rows, rows)
        shift = chips - step if way == 0 else step
        owner = lookup(order, lax.rem(pos + shift, chips))
        left = gath[step, block, :]
        acc[block, :] += jnp.dot(left, wq[owner], preferred_element_type=jnp.float32)
        kvacc[block, :] += lax.dot_general(
            left, wkv[owner], (((1,), (1,)), ((), ())), preferred_element_type=jnp.float32
        )

    for piece in range(PIECES):
        for way in range(2):
            hop(0, way, piece).start()
    mate_wq.start()
    lax.fori_loop(0, chips, lambda k, c: (kv_remote(k).start(), c)[1], 0)

    def stat_copy(d):
        return pltpu.make_async_remote_copy(
            stat_own, stats.at[me], st_send.at[d], st_recv.at[d], device_id={"tp": lax.rem(me + d, n)}
        )

    lax.fori_loop(1, n, lambda d, c: (stat_copy(d).start(), c)[1], 0)

    acc[...] = jnp.zeros_like(acc)
    kvacc[...] = jnp.zeros_like(kvacc)
    token = lax.broadcasted_iota(jnp.int32, (128, HD), 0) + prefix_ref[0]
    freq = freq_ref[...]
    even = lax.rem(lax.broadcasted_iota(jnp.int32, (128, HD), 1), 2) == 0
    for r in range(count // 128):
        angle = (token + r * 128).astype(jnp.float32) * freq
        cosine[pl.ds(r * 128, 128), :] = jnp.cos(angle)
        turn = jnp.sin(angle)
        sine[pl.ds(r * 128, 128), :] = jnp.where(even, -turn, turn)

    lax.fori_loop(1, n, lambda d, c: (stat_copy(d).wait(), c)[1], 0)
    everything = stats[...]
    inverse = 1.0 / jnp.sqrt(jnp.sum(everything[:, 0:4, :], axis=0) / width + norm_eps)
    row_scale = jnp.max(everything[:, 4:8, :], axis=0) * inverse + tiny_eps
    rs_out[...] = row_scale
    for r in range(count // 128):
        block = pl.ds(r * 128, 128)
        inv = spread(inverse[r : r + 1, :])
        inv_col[block, :] = inv
        scale = spread(row_scale[r : r + 1, :])
        for j in range(depth // 128):
            lanes = pl.ds(j * 128, 128)
            weighted = h_ref[block, lanes].astype(jnp.float32) * gain[:, j * 128 : j * 128 + 128]
            payload_out[block, lanes] = (weighted * inv / scale).astype(jnp.bfloat16)

    own_wq.wait()
    lax.fori_loop(0, chips, lambda k, c: (kv_local(k).wait(), c)[1], 0)
    mate_wq.wait()
    lax.fori_loop(0, chips, lambda k, c: (kv_remote(k).wait(), c)[1], 0)

    for piece in range(PIECES):
        for way in range(2):
            multiply(0, way, piece)

    def ring_step(step, carry):
        for piece in range(PIECES):
            for way in range(2):
                hop(step - 1, way, piece).wait_recv()
                hop(step, way, piece).start()
                multiply(step, way, piece)
        return carry

    lax.fori_loop(1, chips - 1, ring_step, 0)
    for piece in range(PIECES):
        for way in range(2):
            hop(chips - 2, way, piece).wait_recv()
            multiply(chips - 1, way, piece)

    ex_kv = pltpu.make_async_remote_copy(
        kvacc, part_kv, ex_send.at[0], ex_recv.at[0], device_id={"tp": mate}
    )
    ex_q = pltpu.make_async_remote_copy(
        acc.at[:, pl.ds(HD, HD)], part_q, ex_send.at[1], ex_recv.at[1], device_id={"tp": mate}
    )
    ex_kv.start()
    ex_q.start()

    def drain(step, carry):
        for piece in range(PIECES):
            for way in range(2):
                hop(step, way, piece).wait_send()
        return carry

    lax.fori_loop(0, chips - 1, drain, 0)
    ex_kv.wait()
    kvscale = kvscale_ref[...]
    for r in range(count // 128):
        block = pl.ds(r * 128, 128)
        cols = (kvacc[block, 0:16] + part_kv[block, 16:32]) * inv_col[block, 0:16] * kvscale
        cols = jnp.concatenate([cols, jnp.zeros((128, 112), jnp.float32)], axis=1)
        kv_own[:, block] = jnp.transpose(cols)[0:16, :].astype(jnp.bfloat16)

    my_head = me * kv_heads // n
    group = lax.rem(me, kv_heads)
    slot = me // kv_heads

    def kv_copy(i):
        return pltpu.make_async_remote_copy(
            kv_own, kv_all.at[slot], kv_send.at[i], kv_recv.at[slot],
            device_id={"tp": group * pieces + i},
        )

    def kv_arrival(i):
        return pltpu.make_async_remote_copy(
            kv_own, kv_all.at[i], kv_send.at[i], kv_recv.at[i], device_id={"tp": mate}
        )

    def kv_start(i, carry):
        @pl.when(group * pieces + i != me)
        def _():
            kv_copy(i).start()

        return carry

    def kv_wait(i, carry):
        @pl.when(group * pieces + i != me)
        def _():
            kv_copy(i).wait_send()

        @pl.when(i * kv_heads + my_head != me)
        def _():
            kv_arrival(i).wait_recv()

        return carry

    @pl.when(my_head == group)
    def _():
        kv_all[slot] = kv_own[...]

    lax.fori_loop(0, pieces, kv_start, 0)

    def rotated(x, block):
        swapped = jnp.where(even, pltpu.roll(x, HD - 1, 1), pltpu.roll(x, 1, 1))
        return (x * cosine[block, :] + swapped * sine[block, :]).astype(jnp.bfloat16)

    ex_q.wait()
    qscale = qscale_ref[...]
    for r in range(count // 128):
        block = pl.ds(r * 128, 128)
        x = (acc[block, 0:HD] + part_q[block, :]) * inv_col[block, :] * qscale
        q_out[block, :] = rotated(x, block)

    lax.fori_loop(0, pieces, kv_wait, 0)
    for r in range(count // 128):
        block = pl.ds(r * 128, 128)
        both = kv_all[:, :, block].astype(jnp.float32)
        keys = jnp.transpose(both[:, 0:KV_COLS_DEV, :].reshape(HD, 128))
        k_out[block, :] = rotated(keys, block)
        values = jnp.transpose(both[:, KV_COLS_DEV:, :].reshape(HD, 128))
        v_out[block, :] = values.astype(jnp.bfloat16)


def grid_kernel(
    width, prefix_ref, h_hbm, gain_hbm, freq_ref, scale_hbm, wq_hbm, wkv_hbm,
    q_out, k_out, v_out, payload_out, rs_out,
    gath, wq, wkv, wq2, wkv2, acc, kvacc, part_q, part_kv, far_q, far_kv, got_q, got_kv,
    stat_own, stats, kv_own, kv_all, inv_col, cosine, sine,
    send_sem, recv_sem, st_send, st_recv, kv_send, kv_recv,
    wl_sem, wkl_sem, wr_send, wr_recv, wkr_send, wkr_recv,
    wz_send, wz_recv, wx_send, wx_recv, ex_send, ex_recv,
    h_ref, gain_ref, scale_ref, in_sem,
):
    n = 16
    chips = 8
    me = lax.axis_index("tp")
    side = lax.axis_index("grp")
    core = lax.rem(me, 2)
    chip = me // 2
    y = lax.rem(chip, 2)
    z = chip // 2
    mate = me + 1 - 2 * core
    is_end = (z == 0) | (z == 3)
    is_mid = (z == 1) | (z == 2)
    inner = z + 1 - 2 * lax.rem(z, 2)
    neighbour = me + 4 * (inner - z)
    across = me + 4 * (3 - 2 * z)
    beside = me + 2 - 4 * y
    count, depth = h_ref.shape
    loads = [pltpu.make_async_copy(gain_hbm, gain_ref, in_sem.at[0])]
    for r in range(count // 128):
        block = pl.ds(r * 128, 128)
        loads.append(pltpu.make_async_copy(h_hbm.at[block], h_ref.at[block], in_sem.at[r + 1]))
    loads.append(pltpu.make_async_copy(scale_hbm, scale_ref, in_sem.at[count // 128 + 1]))
    for load in loads:
        load.start()
    rows = count // GRID_PIECES
    owners = [2 * z + y, 2 * (3 - z) + y, 2 * z + 1 - y, 2 * (3 - z) + 1 - y]
    theirs = [2 * inner + y, 2 * (3 - inner) + y, 2 * inner + 1 - y, 2 * (3 - inner) + 1 - y]

    barrier = pltpu.get_barrier_semaphore()

    def greet(d, carry):
        pl.semaphore_signal(barrier, inc=1, device_id={"tp": lax.rem(me + d, n)})
        return carry

    lax.fori_loop(1, n, greet, 0)
    pl.semaphore_signal(barrier, inc=1, device_id={"grp": 1 - side, "tp": me})

    own_wq = pltpu.make_async_copy(wq_hbm.at[:, core], wq.at[:, :, pl.ds(0, HD)], wl_sem)
    own_wq.start()

    def kv_local(k):
        cols = pl.ds(pl.multiple_of((2 * k + core) * depth, 128), depth)
        return pltpu.make_async_copy(wkv_hbm.at[:, cols], wkv.at[k, pl.ds(0, 16)], wkl_sem.at[k])

    def kv_remote(k):
        cols = pl.ds(pl.multiple_of((2 * k + 1 - core) * depth, 128), depth)
        return pltpu.make_async_remote_copy(
            wkv_hbm.at[:, cols], wkv.at[k, pl.ds(16, 16)], wkr_send.at[k], wkr_recv.at[k],
            device_id={"tp": mate},
        )

    mate_wq = pltpu.make_async_remote_copy(
        wq_hbm.at[:, 1 - core], wq.at[:, :, pl.ds(HD, HD)], wr_send, wr_recv, device_id={"tp": mate}
    )
    lax.fori_loop(0, chips, lambda k, c: (kv_local(k).start(), c)[1], 0)

    loads[0].wait()
    gain = gain_ref[...]
    for r in range(count // 128):
        block = pl.ds(r * 128, 128)
        loads[r + 1].wait()
        wide = h_ref[block, :].astype(jnp.float32)
        weighted = wide * gain
        gath[0, block, :] = weighted.astype(jnp.bfloat16)
        square = jnp.sum(wide * wide, axis=1, keepdims=True)
        top = jnp.max(jnp.abs(weighted), axis=1, keepdims=True)
        stat_own[pl.ds(r, 1), :] = jnp.transpose(jnp.broadcast_to(square, (128, 128)))[0:1, :]
        stat_own[pl.ds(4 + r, 1), :] = jnp.transpose(jnp.broadcast_to(top, (128, 128)))[0:1, :]
    stats[me] = stat_own[...]
    loads[-1].wait()

    pl.semaphore_wait(barrier, n)

    def move(kind, source, target, piece, device):
        block = pl.ds(piece * rows, rows)
        return pltpu.make_async_remote_copy(
            gath.at[source, block], gath.at[target, block],
            send_sem.at[kind, piece], recv_sem.at[target, piece], device_id={"tp": device},
        )

    def beside_own(p):
        return move(0, 0, 2, p, beside)

    def beside_far(p):
        return move(1, 1, 3, p, beside)

    def end_up(p):
        return move(2, 0, 4, p, neighbour)

    def mid_across(p):
        return move(2, 0, 1, p, across)

    def relay_across(p):
        return move(3, 4, 5, p, across)

    def relay_down(p):
        return move(4, 5, 1, p, neighbour)

    def part_of(ref, kv_ref, at, part):
        if part == 2:
            return kv_ref.at[at]
        return ref.at[at, :, pl.ds(part * HD, HD)]

    def weights_z(i, part):
        block = jnp.where(side == 0, theirs[2 * i], theirs[2 * i + 1])
        return pltpu.make_async_remote_copy(
            part_of(wq, wkv, block, part), part_of(wq2, wkv2, 2 * i + side, part),
            wz_send.at[i, part], wz_recv.at[i, part], device_id={"tp": neighbour},
        )

    def weights_x(i, part):
        piece = part_of(wq2, wkv2, 2 * i + side, part)
        return pltpu.make_async_remote_copy(
            piece, piece, wx_send.at[i, part], wx_recv.at[i, part],
            device_id={"grp": 1 - side, "tp": me},
        )

    def weights_pass(i, part):
        weights_z(i, part).wait_recv()
        weights_x(i, part).start()

    def stat_copy(d):
        return pltpu.make_async_remote_copy(
            stat_own, stats.at[me], st_send.at[d], st_recv.at[d], device_id={"tp": lax.rem(me + d, n)}
        )

    everyone = range(GRID_PIECES)
    early = GRID_PIECES // 2

    @pl.when(is_end)
    def _():
        for p in everyone:
            end_up(p).start()

    @pl.when(is_mid)
    def _():
        for p in everyone[:early]:
            mid_across(p).start()

    for p in everyone:
        beside_own(p).start()
    own_wq.wait()
    mate_wq.start()
    lax.fori_loop(0, chips, lambda k, c: (kv_remote(k).start(), c)[1], 0)
    for i in range(2):
        weights_z(i, 0).start()
    lax.fori_loop(1, n, lambda d, c: (stat_copy(d).start(), c)[1], 0)

    acc[...] = jnp.zeros_like(acc)
    kvacc[...] = jnp.zeros_like(kvacc)

    def product(slot, p, mine):
        block = pl.ds(p * rows, rows)
        left = gath[slot, block, :]
        right, right_kv = (wq[owners[slot]], wkv[owners[slot]]) if mine else (wq2[slot], wkv2[slot])
        lanes = pl.ds(0 if mine else 2 * HD, 2 * HD)
        kv_lanes = pl.ds(0 if mine else 32, 32)
        acc[block, lanes] += jnp.dot(left, right, preferred_element_type=jnp.float32)
        kvacc[block, kv_lanes] += lax.dot_general(
            left, right_kv, (((1,), (1,)), ((), ())), preferred_element_type=jnp.float32
        )

    def both(slot, p):
        product(slot, p, True)
        product(slot, p, False)

    def whole(slot, mine):
        for p in everyone:
            product(slot, p, mine)

    even = lax.rem(lax.broadcasted_iota(jnp.int32, (128, HD), 1), 2) == 0

    def tables():
        token = lax.broadcasted_iota(jnp.int32, (128, HD), 0) + prefix_ref[0]
        freq = freq_ref[...]
        for r in range(count // 128):
            angle = (token + r * 128).astype(jnp.float32) * freq
            cosine[pl.ds(r * 128, 128), :] = jnp.cos(angle)
            turn = jnp.sin(angle)
            sine[pl.ds(r * 128, 128), :] = jnp.where(even, -turn, turn)

    def row_statistics():
        lax.fori_loop(1, n, lambda d, c: (stat_copy(d).wait(), c)[1], 0)
        everything = stats[...]
        inverse = 1.0 / jnp.sqrt(jnp.sum(everything[:, 0:4, :], axis=0) / width + norm_eps)
        row_scale = jnp.max(everything[:, 4:8, :], axis=0) * inverse + tiny_eps
        rs_out[...] = row_scale
        for r in range(count // 128):
            block = pl.ds(r * 128, 128)
            inv = spread(inverse[r : r + 1, :])
            inv_col[block, :] = inv
            scale = spread(row_scale[r : r + 1, :])
            for j in range(depth // 128):
                lanes = pl.ds(j * 128, 128)
                weighted = h_ref[block, lanes].astype(jnp.float32) * gain_ref[:, lanes]
                payload_out[block, lanes] = (weighted * inv / scale).astype(jnp.bfloat16)

    def mate_weights():
        mate_wq.wait()
        lax.fori_loop(0, chips, lambda k, c: (kv_local(k).wait(), c)[1], 0)
        lax.fori_loop(0, chips, lambda k, c: (kv_remote(k).wait(), c)[1], 0)
        for i in range(2):
            weights_z(i, 1).start()
            weights_z(i, 2).start()

    def weights_settle():
        for i in range(2):
            for part in range(3):
                weights_x(i, part).wait()

    def own_beside():
        for p in everyone:
            beside_own(p).wait_recv()
        whole(2, True)

    @pl.when(is_mid)
    def _():
        mate_weights()
        for p in everyone[:early]:
            end_up(p).wait_recv()
            relay_across(p).start()
            mid_across(p).wait_recv()
            beside_far(p).start()
        tables()
        for p in everyone[early:]:
            end_up(p).wait_recv()
            relay_across(p).start()
            if p == GRID_PIECES - 1:
                for late in everyone[early:]:
                    mid_across(late).start()
            relay_across(p - early).wait_recv()
            relay_down(p - early).start()
        row_statistics()
        whole(0, True)
        for p in everyone[early:]:
            relay_across(p).wait_recv()
            relay_down(p).start()
        for i in range(2):
            weights_pass(i, 0)
        own_beside()
        for p in everyone[early:]:
            mid_across(p).wait_recv()
            beside_far(p).start()
        for i in range(2):
            weights_pass(i, 1)
            weights_pass(i, 2)
        whole(1, True)
        for p in everyone:
            beside_far(p).wait_recv()
            product(3, p, True)
        weights_settle()
        for slot in range(4):
            whole(slot, False)

    @pl.when(is_end)
    def _():
        mate_weights()
        tables()
        for i in range(2):
            weights_pass(i, 0)
        row_statistics()
        whole(0, True)
        weights_pass(0, 1)
        weights_pass(0, 2)
        own_beside()
        weights_pass(1, 1)
        weights_pass(1, 2)
        for p in everyone:
            relay_down(p).wait_recv()
            beside_far(p).start()
            product(1, p, True)
            if p == early:
                weights_settle()
                whole(0, False)
                whole(2, False)
        whole(1, False)
        for p in everyone:
            beside_far(p).wait_recv()
            both(3, p)

    def swap(source, target, i):
        return pltpu.make_async_remote_copy(
            source, target, ex_send.at[i], ex_recv.at[i], device_id={"tp": mate}
        )

    def hand(source, target, i):
        return pltpu.make_async_remote_copy(
            source, target, ex_send.at[i], ex_recv.at[i], device_id={"tp": neighbour}
        )

    swaps = [
        swap(acc.at[:, pl.ds(3 * HD, HD)], part_q.at[1], 0),
        swap(kvacc, part_kv, 1),
        swap(acc.at[:, pl.ds(HD, HD)], part_q.at[0], 2),
    ]
    hands = [hand(far_kv, got_kv, 3), hand(far_q, got_q, 4)]
    swaps[1].start()
    swaps[0].start()
    swaps[2].start()
    swaps[1].wait()
    pad = jnp.zeros((128, 112), jnp.float32)

    def kv_rows(block, low):
        cols = kvacc[block, low : low + 16] + part_kv[block, low + 16 : low + 32]
        return jnp.transpose(jnp.concatenate([cols, pad], axis=1))[0:16, :]

    for r in range(count // 128):
        block = pl.ds(r * 128, 128)
        far_kv[:, block] = kv_rows(block, 32)
    swaps[0].wait()
    for r in range(count // 128):
        block = pl.ds(r * 128, 128)
        far_q[block, :] = (acc[block, 2 * HD : 3 * HD] + part_q[1, block, :]).astype(jnp.bfloat16)
    hands[0].start()
    hands[1].start()

    for p in everyone:
        beside_own(p).wait_send()
        beside_far(p).wait_send()
    for i in range(2):
        for part in range(3):
            weights_z(i, part).wait_send()

    @pl.when(is_end)
    def _():
        for p in everyone:
            end_up(p).wait_send()

    @pl.when(is_mid)
    def _():
        for p in everyone:
            mid_across(p).wait_send()
            relay_across(p).wait_send()
            relay_down(p).wait_send()

    kv_scale = jnp.concatenate([scale_ref[:, HD:], jnp.zeros((1, 112), jnp.float32)], axis=1)
    kv_scale = spread(kv_scale)[0:16, :]
    hands[0].wait()
    for r in range(count // 128):
        block = pl.ds(r * 128, 128)
        inv = jnp.transpose(inv_col[block, :])[0:1, :]
        mine = (kv_rows(block, 0) + got_kv[:, block]) * inv * kv_scale
        kv_own[:, block] = mine.astype(jnp.bfloat16)
    kv_all[me] = kv_own[...]

    def kv_copy(d):
        return pltpu.make_async_remote_copy(
            kv_own, kv_all.at[me], kv_send.at[d], kv_recv.at[d], device_id={"tp": lax.rem(me + d, n)}
        )

    lax.fori_loop(1, n, lambda d, c: (kv_copy(d).start(), c)[1], 0)

    def rotated(x, block):
        swapped = jnp.where(even, pltpu.roll(x, HD - 1, 1), pltpu.roll(x, 1, 1))
        return (x * cosine[block, :] + swapped * sine[block, :]).astype(jnp.bfloat16)

    swaps[2].wait()
    hands[1].wait()
    qscale = scale_ref[:, 0:HD]
    for r in range(count // 128):
        block = pl.ds(r * 128, 128)
        x = acc[block, 0:HD] + part_q[0, block, :] + got_q[block, :].astype(jnp.float32)
        q_out[block, :] = rotated(x * inv_col[block, :] * qscale, block)

    lax.fori_loop(1, n, lambda d, c: (kv_copy(d).wait(), c)[1], 0)
    for r in range(count // 128):
        block = pl.ds(r * 128, 128)
        pair = kv_all[:, :, block].astype(jnp.float32)
        keys = jnp.transpose(pair[:, 0:KV_COLS_DEV, :].reshape(HD, 128))
        k_out[block, :] = rotated(keys, block)
        values = jnp.transpose(pair[:, KV_COLS_DEV:, :].reshape(HD, 128))
        v_out[block, :] = values.astype(jnp.bfloat16)


def grid_scratch(count, depth):
    dma = pltpu.SemaphoreType.DMA
    bf16, f32 = jnp.bfloat16, jnp.float32
    return [
        pltpu.VMEM((6, count, depth), bf16),
        pltpu.VMEM((8, depth, 2 * HD), bf16),
        pltpu.VMEM((8, 32, depth), bf16),
        pltpu.VMEM((4, depth, 2 * HD), bf16),
        pltpu.VMEM((4, 32, depth), bf16),
        pltpu.VMEM((count, 4 * HD), f32),
        pltpu.VMEM((count, 64), f32),
        pltpu.VMEM((2, count, HD), f32),
        pltpu.VMEM((count, 64), f32),
        pltpu.VMEM((count, HD), bf16),
        pltpu.VMEM((16, count), f32),
        pltpu.VMEM((count, HD), bf16),
        pltpu.VMEM((16, count), f32),
        pltpu.VMEM((8, 128), f32),
        pltpu.VMEM((16, 8, 128), f32),
        pltpu.VMEM((16, count), bf16),
        pltpu.VMEM((16, 16, count), bf16),
        pltpu.VMEM((count, HD), f32),
        pltpu.VMEM((count, HD), f32),
        pltpu.VMEM((count, HD), f32),
        dma((5, GRID_PIECES)),
        dma((6, GRID_PIECES)),
        dma((16,)),
        dma((16,)),
        dma((16,)),
        dma((16,)),
        dma,
        dma((8,)),
        dma,
        dma,
        dma((8,)),
        dma((8,)),
        dma((2, 3)),
        dma((2, 3)),
        dma((2, 3)),
        dma((2, 3)),
        dma((5,)),
        dma((5,)),
        pltpu.VMEM((count, depth), bf16),
        pltpu.VMEM((1, depth), f32),
        pltpu.VMEM((1, HD + 2 * KV_COLS_DEV), f32),
        dma((count // 128 + 2,)),
    ]


def finish_kernel(*refs):
    sources, targets, sems = refs[0:5], refs[5:10], refs[10]
    outs = [pltpu.make_async_copy(sources[i], targets[i], sems.at[i]) for i in range(5)]
    for copy in outs:
        copy.start()
    for copy in outs:
        copy.wait()


def finish(*arrays):
    return pl.pallas_call(
        finish_kernel,
        out_shape=tuple(jax.ShapeDtypeStruct(a.shape, a.dtype) for a in arrays),
        in_specs=[pl.BlockSpec(memory_space=pltpu.VMEM)] * 5,
        out_specs=(pl.BlockSpec(memory_space=pltpu.HBM),) * 5,
        scratch_shapes=[pltpu.SemaphoreType.DMA((5,))], compiler_params=pltpu.CompilerParams(vmem_limit_bytes=2 * 1024 * 1024),
    )(*arrays)


def local(n, groups, hidden, norm_gain, prefix, w_query, w_kv, w_scale):
    count, depth = hidden.shape
    chips = n // 2
    width = depth * n
    grid = n == 16 and groups == 2 and n * KV_COLS_DEV == HD
    pair_index = np.arange(HD) // 2
    freq = jnp.asarray(np.power(rope_base, -(2.0 * pair_index) / HD)[None, :], jnp.float32)
    pieces = HD // KV_COLS_DEV
    vmem = pl.BlockSpec(memory_space=pltpu.VMEM)
    hbm = pl.BlockSpec(memory_space=pltpu.HBM if grid else pl.ANY)
    dma = pltpu.SemaphoreType.DMA
    bf16, f32 = jnp.bfloat16, jnp.float32
    queries, keys, values, payload, row_scale = pl.pallas_call(
        functools.partial(grid_kernel, width) if grid else functools.partial(kernel, n, width),
        out_shape=(
            pltpu.VMEM((count, HD), bf16),
            pltpu.VMEM((count, HD), bf16),
            pltpu.VMEM((count, HD), bf16),
            pltpu.VMEM((count, depth), bf16),
            pltpu.VMEM((count // 128, 128), f32),
        ),
        in_specs=[pl.BlockSpec(memory_space=pltpu.SMEM)]
        + ([hbm, hbm, vmem] + [hbm] * 3 if grid else [vmem] * 5 + [hbm] * 2),
        out_specs=(vmem,) * 5,
        scratch_shapes=grid_scratch(count, depth) if grid else [
            pltpu.VMEM((chips, count, depth), bf16),
            pltpu.VMEM((chips, depth, 2 * HD), bf16),
            pltpu.VMEM((chips, 32, depth), bf16),
            pltpu.VMEM((count, 2 * HD), f32),
            pltpu.VMEM((count, 32), f32),
            pltpu.VMEM((count, HD), f32),
            pltpu.VMEM((count, 32), f32),
            pltpu.VMEM((8, 128), f32),
            pltpu.VMEM((n, 8, 128), f32),
            pltpu.VMEM((2 * KV_COLS_DEV, count), bf16),
            pltpu.VMEM((pieces, 2 * KV_COLS_DEV, count), bf16),
            pltpu.VMEM((count, HD), f32),
            pltpu.VMEM((count, HD), f32),
            pltpu.VMEM((count, HD), f32),
            dma((chips, 2, PIECES)),
            dma((chips, 2, PIECES)),
            dma((n,)),
            dma((n,)),
            dma((pieces,)),
            dma((pieces,)),
            dma,
            dma((chips,)),
            dma,
            dma,
            dma((chips,)),
            dma((chips,)),
            dma((2,)),
            dma((2,)),
        ],
        compiler_params=pltpu.CompilerParams(
            collective_id=0, has_side_effects=True, vmem_limit_bytes=(58 if grid else 48) * 1024 * 1024
        ),
    )(
        prefix,
        hidden,
        norm_gain[None, :],
        freq,
        *([w_scale[None, :]] if grid else [w_scale[None, :HD], w_scale[None, HD:]]),
        w_query.reshape(chips, 2, depth, HD),
        w_kv,
    )
    queries, keys, values, payload, row_scale = finish(queries, keys, values, payload, row_scale)
    return queries, keys, values, payload, row_scale.reshape(count)


def solution(mesh):
    return jax.shard_map(
        functools.partial(local, mesh.shape["tp"], mesh.shape["grp"]),
        mesh=mesh,
        in_specs=(P("grp", "tp"), P("tp"), P("grp"), P(None, "tp"), P("tp", None), P("tp")),
        out_specs=(P("grp", "tp"), P("grp", "tp"), P("grp", "tp"), P("grp", "tp"), P("grp")),
        check_vma=False,
    )
```

```python
import functools

import jax
import jax.numpy as jnp
import numpy as np
from jax import lax
from jax.experimental import pallas as pl
from jax.experimental.pallas import tpu as pltpu
from jax.sharding import PartitionSpec as P

HD = 128
KV_COLS_DEV = 8
norm_eps = 1e-05
tiny_eps = 1e-06
rope_base = 500000.0
PIECES = 2
GRID_PIECES = 4


def ring_order(chips):
    cols = 1
    while (2 * cols) * (2 * cols) <= chips and chips % (2 * cols) == 0:
        cols *= 2
    rows = chips // cols
    if cols < 2 or rows % 2:
        return list(range(chips))
    order = [0]
    for row in range(rows):
        span = range(1, cols) if row % 2 == 0 else range(cols - 1, 0, -1)
        order += [row * cols + col for col in span]
    order += [row * cols for row in range(rows - 1, 0, -1)]
    return order


def lookup(table, index):
    total = jnp.int32(0)
    for key, value in enumerate(table):
        total = total + jnp.where(index == key, jnp.int32(value), jnp.int32(0))
    return total


def spread(row):
    return jnp.transpose(jnp.broadcast_to(row, (128, 128)))


def kernel(
    n, width, prefix_ref, h_ref, gain_ref, freq_ref, qscale_ref, kvscale_ref, wq_hbm, wkv_hbm,
    q_out, k_out, v_out, payload_out, rs_out,
    gath, wq, wkv, acc, kvacc, part_q, part_kv, stat_own, stats, kv_own, kv_all, inv_col, cosine, sine,
    send_sem, recv_sem, st_send, st_recv, kv_send, kv_recv,
    wl_sem, wkl_sem, wr_send, wr_recv, wkr_send, wkr_recv, ex_send, ex_recv,
):
    me = lax.axis_index("tp")
    chips = n // 2
    core = lax.rem(me, 2)
    chip = me // 2
    mate = me + 1 - 2 * core
    count, depth = h_ref.shape
    half = count // 2
    rows = half // PIECES
    pieces = HD // KV_COLS_DEV
    kv_heads = n // pieces
    order = ring_order(chips)
    place = [order.index(c) for c in range(chips)]
    pos = lookup(place, chip)
    succ = 2 * lookup(order, lax.rem(pos + 1, chips)) + core
    pred = 2 * lookup(order, lax.rem(pos + chips - 1, chips)) + core

    barrier = pltpu.get_barrier_semaphore()

    def greet(d, carry):
        pl.semaphore_signal(barrier, inc=1, device_id={"tp": lax.rem(me + d, n)})
        return carry

    lax.fori_loop(1, n, greet, 0)

    own_wq = pltpu.make_async_copy(wq_hbm.at[:, core], wq.at[:, :, pl.ds(0, HD)], wl_sem)
    own_wq.start()

    def kv_local(k):
        cols = pl.ds(pl.multiple_of((2 * k + core) * depth, 128), depth)
        return pltpu.make_async_copy(wkv_hbm.at[:, cols], wkv.at[k, pl.ds(0, 16)], wkl_sem.at[k])

    def kv_remote(k):
        cols = pl.ds(pl.multiple_of((2 * k + 1 - core) * depth, 128), depth)
        return pltpu.make_async_remote_copy(
            wkv_hbm.at[:, cols], wkv.at[k, pl.ds(16, 16)], wkr_send.at[k], wkr_recv.at[k],
            device_id={"tp": mate},
        )

    mate_wq = pltpu.make_async_remote_copy(
        wq_hbm.at[:, 1 - core], wq.at[:, :, pl.ds(HD, HD)], wr_send, wr_recv, device_id={"tp": mate}
    )
    lax.fori_loop(0, chips, lambda k, c: (kv_local(k).start(), c)[1], 0)

    gain = gain_ref[...]
    for r in range(count // 128):
        block = pl.ds(r * 128, 128)
        wide = h_ref[block, :].astype(jnp.float32)
        weighted = wide * gain
        gath[0, block, :] = weighted.astype(jnp.bfloat16)
        square = jnp.sum(wide * wide, axis=1, keepdims=True)
        top = jnp.max(jnp.abs(weighted), axis=1, keepdims=True)
        stat_own[pl.ds(r, 1), :] = jnp.transpose(jnp.broadcast_to(square, (128, 128)))[0:1, :]
        stat_own[pl.ds(4 + r, 1), :] = jnp.transpose(jnp.broadcast_to(top, (128, 128)))[0:1, :]
    stats[me] = stat_own[...]

    pl.semaphore_wait(barrier, n - 1)

    def hop(step, way, piece):
        block = pl.ds(way * half + piece * rows, rows)
        return pltpu.make_async_remote_copy(
            gath.at[step, block], gath.at[step + 1, block],
            send_sem.at[step, way, piece], recv_sem.at[step, way, piece],
            device_id={"tp": succ if way == 0 else pred},
        )

    def multiply(step, way, piece):
        block = pl.ds(way * half + piece * rows, rows)
        shift = chips - step if way == 0 else step
        owner = lookup(order, lax.rem(pos + shift, chips))
        left = gath[step, block, :]
        acc[block, :] += jnp.dot(left, wq[owner], preferred_element_type=jnp.float32)
        kvacc[block, :] += lax.dot_general(
            left, wkv[owner], (((1,), (1,)), ((), ())), preferred_element_type=jnp.float32
        )

    for piece in range(PIECES):
        for way in range(2):
            hop(0, way, piece).start()
    mate_wq.start()
    lax.fori_loop(0, chips, lambda k, c: (kv_remote(k).start(), c)[1], 0)

    def stat_copy(d):
        return pltpu.make_async_remote_copy(
            stat_own, stats.at[me], st_send.at[d], st_recv.at[d], device_id={"tp": lax.rem(me + d, n)}
        )

    lax.fori_loop(1, n, lambda d, c: (stat_copy(d).start(), c)[1], 0)

    acc[...] = jnp.zeros_like(acc)
    kvacc[...] = jnp.zeros_like(kvacc)
    token = lax.broadcasted_iota(jnp.int32, (128, HD), 0) + prefix_ref[0]
    freq = freq_ref[...]
    even = lax.rem(lax.broadcasted_iota(jnp.int32, (128, HD), 1), 2) == 0
    for r in range(count // 128):
        angle = (token + r * 128).astype(jnp.float32) * freq
        cosine[pl.ds(r * 128, 128), :] = jnp.cos(angle)
        turn = jnp.sin(angle)
        sine[pl.ds(r * 128, 128), :] = jnp.where(even, -turn, turn)

    lax.fori_loop(1, n, lambda d, c: (stat_copy(d).wait(), c)[1], 0)
    everything = stats[...]
    inverse = 1.0 / jnp.sqrt(jnp.sum(everything[:, 0:4, :], axis=0) / width + norm_eps)
    row_scale = jnp.max(everything[:, 4:8, :], axis=0) * inverse + tiny_eps
    rs_out[...] = row_scale
    for r in range(count // 128):
        block = pl.ds(r * 128, 128)
        inv = spread(inverse[r : r + 1, :])
        inv_col[block, :] = inv
        scale = spread(row_scale[r : r + 1, :])
        for j in range(depth // 128):
            lanes = pl.ds(j * 128, 128)
            weighted = h_ref[block, lanes].astype(jnp.float32) * gain[:, j * 128 : j * 128 + 128]
            payload_out[block, lanes] = (weighted * inv / scale).astype(jnp.bfloat16)

    own_wq.wait()
    lax.fori_loop(0, chips, lambda k, c: (kv_local(k).wait(), c)[1], 0)
    mate_wq.wait()
    lax.fori_loop(0, chips, lambda k, c: (kv_remote(k).wait(), c)[1], 0)

    for piece in range(PIECES):
        for way in range(2):
            multiply(0, way, piece)

    def ring_step(step, carry):
        for piece in range(PIECES):
            for way in range(2):
                hop(step - 1, way, piece).wait_recv()
                hop(step, way, piece).start()
                multiply(step, way, piece)
        return carry

    lax.fori_loop(1, chips - 1, ring_step, 0)
    for piece in range(PIECES):
        for way in range(2):
            hop(chips - 2, way, piece).wait_recv()
            multiply(chips - 1, way, piece)

    ex_kv = pltpu.make_async_remote_copy(
        kvacc, part_kv, ex_send.at[0], ex_recv.at[0], device_id={"tp": mate}
    )
    ex_q = pltpu.make_async_remote_copy(
        acc.at[:, pl.ds(HD, HD)], part_q, ex_send.at[1], ex_recv.at[1], device_id={"tp": mate}
    )
    ex_kv.start()
    ex_q.start()

    def drain(step, carry):
        for piece in range(PIECES):
            for way in range(2):
                hop(step, way, piece).wait_send()
        return carry

    lax.fori_loop(0, chips - 1, drain, 0)
    ex_kv.wait()
    kvscale = kvscale_ref[...]
    for r in range(count // 128):
        block = pl.ds(r * 128, 128)
        cols = (kvacc[block, 0:16] + part_kv[block, 16:32]) * inv_col[block, 0:16] * kvscale
        cols = jnp.concatenate([cols, jnp.zeros((128, 112), jnp.float32)], axis=1)
        kv_own[:, block] = jnp.transpose(cols)[0:16, :].astype(jnp.bfloat16)

    my_head = me * kv_heads // n
    group = lax.rem(me, kv_heads)
    slot = me // kv_heads

    def kv_copy(i):
        return pltpu.make_async_remote_copy(
            kv_own, kv_all.at[slot], kv_send.at[i], kv_recv.at[slot],
            device_id={"tp": group * pieces + i},
        )

    def kv_arrival(i):
        return pltpu.make_async_remote_copy(
            kv_own, kv_all.at[i], kv_send.at[i], kv_recv.at[i], device_id={"tp": mate}
        )

    def kv_start(i, carry):
        @pl.when(group * pieces + i != me)
        def _():
            kv_copy(i).start()

        return carry

    def kv_wait(i, carry):
        @pl.when(group * pieces + i != me)
        def _():
            kv_copy(i).wait_send()

        @pl.when(i * kv_heads + my_head != me)
        def _():
            kv_arrival(i).wait_recv()

        return carry

    @pl.when(my_head == group)
    def _():
        kv_all[slot] = kv_own[...]

    lax.fori_loop(0, pieces, kv_start, 0)

    def rotated(x, block):
        swapped = jnp.where(even, pltpu.roll(x, HD - 1, 1), pltpu.roll(x, 1, 1))
        return (x * cosine[block, :] + swapped * sine[block, :]).astype(jnp.bfloat16)

    ex_q.wait()
    qscale = qscale_ref[...]
    for r in range(count // 128):
        block = pl.ds(r * 128, 128)
        x = (acc[block, 0:HD] + part_q[block, :]) * inv_col[block, :] * qscale
        q_out[block, :] = rotated(x, block)

    lax.fori_loop(0, pieces, kv_wait, 0)
    for r in range(count // 128):
        block = pl.ds(r * 128, 128)
        both = kv_all[:, :, block].astype(jnp.float32)
        keys = jnp.transpose(both[:, 0:KV_COLS_DEV, :].reshape(HD, 128))
        k_out[block, :] = rotated(keys, block)
        values = jnp.transpose(both[:, KV_COLS_DEV:, :].reshape(HD, 128))
        v_out[block, :] = values.astype(jnp.bfloat16)


def grid_kernel(
    width, prefix_ref, h_hbm, gain_hbm, freq_ref, scale_hbm, wq_hbm, wkv_hbm,
    q_out, k_out, v_out, payload_out, rs_out,
    gath, wq, wkv, acc, kvacc, q_give, q_got, kv_give, kv_got,
    stat_own, stats, kv_own, kv_all, inv_row, inv_col, cosine, sine,
    h_ref, gain_ref, scale_ref, in_sem, own_sem,
    st_send, st_recv, w_send, w_recv, wx_send, wx_recv, act_send, act_recv, mate_send, mate_recv,
    pq_send, pq_recv, pkv_send, pkv_recv, kv_send, kv_recv,
):
    n = 16
    me = lax.axis_index("tp")
    side = lax.axis_index("grp")
    core = lax.rem(me, 2)
    chip = me // 2
    y = lax.rem(chip, 2)
    z = chip // 2
    mate = me + 1 - 2 * core
    is_end = (z == 0) | (z == 3)
    is_mid = (z == 1) | (z == 2)
    inner = z + 1 - 2 * lax.rem(z, 2)
    across = me + 4 * (3 - 2 * z)
    beside = me + 2 - 4 * y
    peers = [me, beside, me + 4 * (inner - z), beside + 4 * (inner - z)]
    places = [(z, y), (z, 1 - y), (inner, y), (inner, 1 - y)]
    count, depth = h_ref.shape
    kv_cols = 2 * KV_COLS_DEV
    rows = count // GRID_PIECES
    everyone = range(GRID_PIECES)

    loads = [pltpu.make_async_copy(gain_hbm, gain_ref, in_sem.at[0])]
    for r in range(count // 128):
        block = pl.ds(r * 128, 128)
        loads.append(pltpu.make_async_copy(h_hbm.at[block], h_ref.at[block], in_sem.at[r + 1]))
    loads.append(pltpu.make_async_copy(scale_hbm, scale_ref, in_sem.at[count // 128 + 1]))
    for load in loads:
        load.start()

    barrier = pltpu.get_barrier_semaphore()

    def greet(d, carry):
        pl.semaphore_signal(barrier, inc=1, device_id={"tp": lax.rem(me + d, n)})
        return carry

    lax.fori_loop(1, n, greet, 0)
    pl.semaphore_signal(barrier, inc=1, device_id={"grp": 1 - side, "tp": me})

    def weights(s, k, part):
        zt, yt = places[s]
        block = 2 * (2 * (zt + k * (3 - 2 * zt)) + yt) + part % 2
        if part < 2:
            return wq_hbm.at[block], wq.at[k, part, :, pl.ds(s * HD, HD)]
        cols = pl.ds(pl.multiple_of(block * depth, 128), depth)
        return wkv_hbm.at[:, cols], wkv.at[k, part - 2, pl.ds(s * kv_cols, kv_cols)]

    def weights_own(k, part):
        source, target = weights(0, k, part)
        return pltpu.make_async_copy(source, target, own_sem.at[part // 2])

    def weights_to(s, k, part):
        source, target = weights(s, k, part)
        return pltpu.make_async_remote_copy(
            source, target, w_send.at[(s > 1) * 2 + part // 2],
            w_recv.at[part // 2 if s == 1 else 4 * s - 6 + part], device_id={"tp": peers[s]},
        )

    def weights_all(send_sem, recv_sem, part):
        whole = wq.at[:, :, :, pl.ds(0, HD)] if part < 2 else wkv.at[:, :, pl.ds(0, kv_cols)]
        return pltpu.make_async_remote_copy(
            whole, whole, send_sem, recv_sem, device_id={"tp": peers[1]}
        )

    def weights_twin(s, part):
        piece = weights(s, side, part)[1]
        return pltpu.make_async_remote_copy(
            piece, piece, wx_send.at[part // 2], wx_recv.at[part // 2],
            device_id={"grp": 1 - side, "tp": me},
        )

    for k in range(2):
        for part in range(4):
            weights_own(k, part).start()

    loads[0].wait()
    gain = gain_ref[...]
    for r in range(count // 128):
        block = pl.ds(r * 128, 128)
        loads[r + 1].wait()
        wide = h_ref[block, :].astype(jnp.float32)
        weighted = wide * gain
        gath[core, block, :] = weighted.astype(jnp.bfloat16)
        square = jnp.sum(wide * wide, axis=1, keepdims=True)
        top = jnp.max(jnp.abs(weighted), axis=1, keepdims=True)
        stat_own[pl.ds(r, 1), :] = jnp.transpose(jnp.broadcast_to(square, (128, 128)))[0:1, :]
        stat_own[pl.ds(4 + r, 1), :] = jnp.transpose(jnp.broadcast_to(top, (128, 128)))[0:1, :]
    stats[me] = stat_own[...]
    loads[-1].wait()

    pl.semaphore_wait(barrier, n)

    def stat_copy(d):
        return pltpu.make_async_remote_copy(
            stat_own, stats.at[me], st_send, st_recv, device_id={"tp": lax.rem(me + d, n)}
        )

    def stat_all():
        others = stats.at[pl.ds(1, n - 1)]
        return pltpu.make_async_remote_copy(others, others, st_send, st_recv, device_id={"tp": mate})

    def act_mate():
        return pltpu.make_async_remote_copy(
            gath.at[core], gath.at[core], mate_send, mate_recv.at[GRID_PIECES],
            device_id={"tp": mate},
        )

    def act_across(p):
        block = pl.ds(p * rows, rows)
        return pltpu.make_async_remote_copy(
            gath.at[core, block], gath.at[2 + core, block], act_send, act_recv.at[p],
            device_id={"tp": across},
        )

    def act_pass(p):
        block = pl.ds(p * rows, rows)
        piece = gath.at[2 + core, block]
        return pltpu.make_async_remote_copy(
            piece, piece, mate_send, mate_recv.at[p], device_id={"tp": mate}
        )

    forwarded = [(s, part) for part in (2, 3, 0, 1) for s in (2, 3)]
    lax.fori_loop(1, n, lambda d, c: (stat_copy(d).start(), c)[1], 0)
    for s, part in forwarded:
        weights_to(s, side, part).start()
    for p in everyone:
        act_across(p).start()
    act_mate().start()
    for k in range(2):
        for part in range(4):
            weights_to(1, k, part).start()

    even = lax.rem(lax.broadcasted_iota(jnp.int32, (128, HD), 1), 2) == 0
    token = lax.broadcasted_iota(jnp.int32, (128, HD), 0) + prefix_ref[0]
    freq = freq_ref[...]
    for r in range(count // 128):
        angle = (token + r * 128).astype(jnp.float32) * freq
        cosine[pl.ds(r * 128, 128), :] = jnp.cos(angle)
        turn = jnp.sin(angle)
        sine[pl.ds(r * 128, 128), :] = jnp.where(even, -turn, turn)

    stat_all().wait()
    everything = stats[...]
    inverse = 1.0 / jnp.sqrt(jnp.sum(everything[:, 0:4, :], axis=0) / width + norm_eps)
    row_scale = jnp.max(everything[:, 4:8, :], axis=0) * inverse + tiny_eps
    rs_out[...] = row_scale
    inv_row[...] = inverse
    for r in range(count // 128):
        block = pl.ds(r * 128, 128)
        inv = spread(inverse[r : r + 1, :])
        inv_col[block, :] = inv
        scale = spread(row_scale[r : r + 1, :])
        for j in range(depth // 128):
            lanes = pl.ds(j * 128, 128)
            weighted = h_ref[block, lanes].astype(jnp.float32) * gain_ref[:, lanes]
            payload_out[block, lanes] = (weighted * inv / scale).astype(jnp.bfloat16)

    for s, part in forwarded:
        weights_to(s, side, part).wait_recv()
        weights_twin(s, part).start()

    @pl.when(is_mid)
    def _():
        for p in everyone:
            act_across(p).wait_recv()
            act_pass(p).start()

    act_mate().wait_recv()
    for part in (0, 2):
        whole = weights_all(own_sem.at[part // 2], own_sem.at[part // 2], part)
        whole.wait_recv()
        weights_all(w_send.at[part // 2], w_recv.at[part // 2], part).wait()
        weights_all(wx_send.at[part // 2], wx_recv.at[part // 2], part).wait()

    def product(slot, block, k, half):
        return jnp.dot(gath[slot, block, :], wq[k, half], preferred_element_type=jnp.float32)

    def kv_product(slot, block, k, half):
        return lax.dot_general(
            wkv[k, half], gath[slot, block, :], (((1,), (1,)), ((), ())), preferred_element_type=jnp.float32
        )

    for p in everyone:
        block = pl.ds(p * rows, rows)
        kvacc[p] = kv_product(0, block, 0, 0) + kv_product(1, block, 0, 1)
        acc[block, :] = product(0, block, 0, 0) + product(1, block, 0, 1)

    def q_partial(s, p):
        block = pl.ds(p * rows, rows)
        return pltpu.make_async_remote_copy(
            q_give.at[s - 1, block], q_got.at[s - 1, block], pq_send, pq_recv.at[p],
            device_id={"tp": peers[s]},
        )

    def kv_partial(s, p):
        return pltpu.make_async_remote_copy(
            kv_give.at[s - 1, p], kv_got.at[s - 1, p], pkv_send, pkv_recv.at[p],
            device_id={"tp": peers[s]},
        )

    def near(p):
        block = pl.ds(p * rows, rows)
        kvacc[p] += kv_product(2 + core, block, 1, core)
        acc[block, :] += product(2 + core, block, 1, core)

    def far(p):
        block = pl.ds(p * rows, rows)
        act_pass(p).wait_recv()
        pair = kvacc[p] + kv_product(3 - core, block, 1, 1 - core)
        kvacc[p] = pair
        for s in range(1, 4):
            kv_give[s - 1, p] = pair[s * kv_cols : (s + 1) * kv_cols, :]
        for s in range(1, 4):
            kv_partial(s, p).start()
        whole = acc[block, :] + product(3 - core, block, 1, 1 - core)
        acc[block, 0:HD] = whole[:, 0:HD]
        for s in range(1, 4):
            q_give[s - 1, block, :] = whole[:, s * HD : (s + 1) * HD].astype(jnp.bfloat16)
        for s in range(1, 4):
            q_partial(s, p).start()

    kv_scale = jnp.concatenate([scale_ref[:, HD:], jnp.zeros((1, 128 - kv_cols), jnp.float32)], axis=1)
    kv_scale = spread(kv_scale)[0:kv_cols, :]
    qscale = scale_ref[:, 0:HD]

    def kv_copy(p, d):
        return pltpu.make_async_remote_copy(
            kv_own.at[p], kv_all.at[me, p], kv_send, kv_recv.at[p], device_id={"tp": lax.rem(me + d, n)}
        )

    def every(ref, send_sem, recv_sem):
        return pltpu.make_async_remote_copy(ref, ref, send_sem, recv_sem, device_id={"tp": mate})

    def kv_reduce(p):
        total = kvacc[p, 0:kv_cols, :]
        every(kv_got.at[:, p], pkv_send, pkv_recv.at[p]).wait_recv()
        for s in range(1, 4):
            total = total + kv_got[s - 1, p]
        mine = (total * inv_row[p : p + 1, :] * kv_scale).astype(jnp.bfloat16)
        kv_own[p] = mine
        kv_all[me, p] = mine
        lax.fori_loop(1, n, lambda d, c: (kv_copy(p, d).start(), c)[1], 0)

    def rotated(x, block):
        swapped = jnp.where(even, pltpu.roll(x, HD - 1, 1), pltpu.roll(x, 1, 1))
        return (x * cosine[block, :] + swapped * sine[block, :]).astype(jnp.bfloat16)

    def q_reduce(p):
        block = pl.ds(p * rows, rows)
        x = acc[block, 0:HD]
        every(q_got.at[:, block], pq_send, pq_recv.at[p]).wait_recv()
        for s in range(1, 4):
            x = x + q_got[s - 1, block, :].astype(jnp.float32)
        q_out[block, :] = rotated(x * inv_col[block, :] * qscale, block)

    def heads(p):
        block = pl.ds(p * rows, rows)
        every(kv_all.at[pl.ds(1, n - 1), p], kv_send, kv_recv.at[p]).wait_recv()
        pair = kv_all[:, p].astype(jnp.float32)
        keys = jnp.transpose(pair[:, 0:KV_COLS_DEV, :].reshape(HD, 128))
        k_out[block, :] = rotated(keys, block)
        values = jnp.transpose(pair[:, KV_COLS_DEV:, :].reshape(HD, 128))
        v_out[block, :] = values.astype(jnp.bfloat16)

    last = GRID_PIECES - 1

    @pl.when(is_mid)
    def _():
        for p in everyone:
            near(p)
        for p in everyone:
            far(p)
        for p in range(last):
            kv_reduce(p)

    @pl.when(is_end)
    def _():
        for p in everyone:
            act_across(p).wait_recv()
            act_pass(p).start()
            near(p)
            far(p)
            if p:
                kv_reduce(p - 1)

    every(gath.at[0], act_send, act_send).wait_send()
    every(gath.at[pl.ds(0, 2)], mate_send, mate_send).wait_send()
    for part in (0, 2):
        weights_all(w_send.at[2 + part // 2], w_send.at[2 + part // 2], part).wait_send()

    for p in range(last):
        q_reduce(p)
    kv_reduce(last)
    for p in range(last):
        heads(p)
    q_reduce(last)
    every(kv_give, pkv_send, pkv_send).wait_send()
    every(q_give, pq_send, pq_send).wait_send()
    every(kv_all.at[pl.ds(1, n - 1)], kv_send, kv_send).wait_send()
    heads(last)


def grid_scratch(count, depth):
    dma = pltpu.SemaphoreType.DMA
    bf16, f32 = jnp.bfloat16, jnp.float32
    pieces, kv_cols = GRID_PIECES, 2 * KV_COLS_DEV
    rows = count // pieces
    return [
        pltpu.VMEM((4, count, depth), bf16),
        pltpu.VMEM((2, 2, depth, 4 * HD), bf16),
        pltpu.VMEM((2, 2, 4 * kv_cols, depth), bf16),
        pltpu.VMEM((count, 4 * HD), f32),
        pltpu.VMEM((pieces, 4 * kv_cols, rows), f32),
        pltpu.VMEM((3, count, HD), bf16),
        pltpu.VMEM((3, count, HD), bf16),
        pltpu.VMEM((3, pieces, kv_cols, rows), f32),
        pltpu.VMEM((3, pieces, kv_cols, rows), f32),
        pltpu.VMEM((8, 128), f32),
        pltpu.VMEM((16, 8, 128), f32),
        pltpu.VMEM((pieces, kv_cols, rows), bf16),
        pltpu.VMEM((16, pieces, kv_cols, rows), bf16),
        pltpu.VMEM((count // 128, 128), f32),
        pltpu.VMEM((count, HD), f32),
        pltpu.VMEM((count, HD), f32),
        pltpu.VMEM((count, HD), f32),
        pltpu.VMEM((count, depth), bf16),
        pltpu.VMEM((1, depth), f32),
        pltpu.VMEM((1, HD + kv_cols), f32),
        dma((count // 128 + 2,)),
        dma((2,)),
        dma,
        dma,
        dma((4,)),
        dma((10,)),
        dma((2,)),
        dma((2,)),
        dma,
        dma((pieces,)),
        dma,
        dma((pieces + 1,)),
        dma,
        dma((pieces,)),
        dma,
        dma((pieces,)),
        dma,
        dma((pieces,)),
    ]


def finish_kernel(*refs):
    sources, targets, sems = refs[0:5], refs[5:10], refs[10]
    outs = [pltpu.make_async_copy(sources[i], targets[i], sems.at[i]) for i in range(5)]
    for copy in outs:
        copy.start()
    for copy in outs:
        copy.wait()


def finish(*arrays):
    return pl.pallas_call(
        finish_kernel,
        out_shape=tuple(jax.ShapeDtypeStruct(a.shape, a.dtype) for a in arrays),
        in_specs=[pl.BlockSpec(memory_space=pltpu.VMEM)] * 5,
        out_specs=(pl.BlockSpec(memory_space=pltpu.HBM),) * 5,
        scratch_shapes=[pltpu.SemaphoreType.DMA((5,))], compiler_params=pltpu.CompilerParams(vmem_limit_bytes=2 * 1024 * 1024),
    )(*arrays)


def local(n, groups, hidden, norm_gain, prefix, w_query, w_kv, w_scale):
    count, depth = hidden.shape
    chips = n // 2
    width = depth * n
    grid = n == 16 and groups == 2 and n * KV_COLS_DEV == HD and count == 128 * GRID_PIECES
    pair_index = np.arange(HD) // 2
    freq = jnp.asarray(np.power(rope_base, -(2.0 * pair_index) / HD)[None, :], jnp.float32)
    pieces = HD // KV_COLS_DEV
    vmem = pl.BlockSpec(memory_space=pltpu.VMEM)
    hbm = pl.BlockSpec(memory_space=pltpu.HBM if grid else pl.ANY)
    dma = pltpu.SemaphoreType.DMA
    bf16, f32 = jnp.bfloat16, jnp.float32
    queries, keys, values, payload, row_scale = pl.pallas_call(
        functools.partial(grid_kernel, width) if grid else functools.partial(kernel, n, width),
        out_shape=(
            pltpu.VMEM((count, HD), bf16),
            pltpu.VMEM((count, HD), bf16),
            pltpu.VMEM((count, HD), bf16),
            pltpu.VMEM((count, depth), bf16),
            pltpu.VMEM((count // 128, 128), f32),
        ),
        in_specs=[pl.BlockSpec(memory_space=pltpu.SMEM)]
        + ([hbm, hbm, vmem] + [hbm] * 3 if grid else [vmem] * 5 + [hbm] * 2),
        out_specs=(vmem,) * 5,
        scratch_shapes=grid_scratch(count, depth) if grid else [
            pltpu.VMEM((chips, count, depth), bf16),
            pltpu.VMEM((chips, depth, 2 * HD), bf16),
            pltpu.VMEM((chips, 32, depth), bf16),
            pltpu.VMEM((count, 2 * HD), f32),
            pltpu.VMEM((count, 32), f32),
            pltpu.VMEM((count, HD), f32),
            pltpu.VMEM((count, 32), f32),
            pltpu.VMEM((8, 128), f32),
            pltpu.VMEM((n, 8, 128), f32),
            pltpu.VMEM((2 * KV_COLS_DEV, count), bf16),
            pltpu.VMEM((pieces, 2 * KV_COLS_DEV, count), bf16),
            pltpu.VMEM((count, HD), f32),
            pltpu.VMEM((count, HD), f32),
            pltpu.VMEM((count, HD), f32),
            dma((chips, 2, PIECES)),
            dma((chips, 2, PIECES)),
            dma((n,)),
            dma((n,)),
            dma((pieces,)),
            dma((pieces,)),
            dma,
            dma((chips,)),
            dma,
            dma,
            dma((chips,)),
            dma((chips,)),
            dma((2,)),
            dma((2,)),
        ],
        compiler_params=pltpu.CompilerParams(
            collective_id=0, has_side_effects=True, vmem_limit_bytes=(60 if grid else 48) * 1024 * 1024
        ),
    )(
        prefix,
        hidden,
        norm_gain[None, :],
        freq,
        *([w_scale[None, :]] if grid else [w_scale[None, :HD], w_scale[None, HD:]]),
        w_query.reshape(n, depth, HD) if grid else w_query.reshape(chips, 2, depth, HD),
        w_kv,
    )
    queries, keys, values, payload, row_scale = finish(queries, keys, values, payload, row_scale)
    return queries, keys, values, payload, row_scale.reshape(count)


def solution(mesh):
    return jax.shard_map(
        functools.partial(local, mesh.shape["tp"], mesh.shape["grp"]),
        mesh=mesh,
        in_specs=(P("grp", "tp"), P("tp"), P("grp"), P(None, "tp"), P("tp", None), P("tp")),
        out_specs=(P("grp", "tp"), P("grp", "tp"), P("grp", "tp"), P("grp", "tp"), P("grp")),
        check_vma=False,
    )
```

```python
import functools

import jax
import jax.numpy as jnp
import numpy as np
from jax import lax
from jax.experimental import pallas as pl
from jax.experimental.pallas import tpu as pltpu
from jax.sharding import PartitionSpec as P

HD = 128
KV_COLS_DEV = 8
norm_eps = 1e-05
tiny_eps = 1e-06
rope_base = 500000.0
PIECES = 2
GRID_PIECES = 4
LATE = 384


def ring_order(chips):
    cols = 1
    while (2 * cols) * (2 * cols) <= chips and chips % (2 * cols) == 0:
        cols *= 2
    rows = chips // cols
    if cols < 2 or rows % 2:
        return list(range(chips))
    order = [0]
    for row in range(rows):
        span = range(1, cols) if row % 2 == 0 else range(cols - 1, 0, -1)
        order += [row * cols + col for col in span]
    order += [row * cols for row in range(rows - 1, 0, -1)]
    return order


def lookup(table, index):
    total = jnp.int32(0)
    for key, value in enumerate(table):
        total = total + jnp.where(index == key, jnp.int32(value), jnp.int32(0))
    return total


def spread(row):
    return jnp.transpose(jnp.broadcast_to(row, (128, 128)))


def kernel(
    n, width, prefix_ref, h_ref, gain_ref, freq_ref, qscale_ref, kvscale_ref, wq_hbm, wkv_hbm,
    q_out, k_out, v_out, payload_out, rs_out,
    gath, wq, wkv, acc, kvacc, part_q, part_kv, stat_own, stats, kv_own, kv_all, inv_col, cosine, sine,
    send_sem, recv_sem, st_send, st_recv, kv_send, kv_recv,
    wl_sem, wkl_sem, wr_send, wr_recv, wkr_send, wkr_recv, ex_send, ex_recv,
):
    me = lax.axis_index("tp")
    chips = n // 2
    core = lax.rem(me, 2)
    chip = me // 2
    mate = me + 1 - 2 * core
    count, depth = h_ref.shape
    half = count // 2
    rows = half // PIECES
    pieces = HD // KV_COLS_DEV
    kv_heads = n // pieces
    order = ring_order(chips)
    place = [order.index(c) for c in range(chips)]
    pos = lookup(place, chip)
    succ = 2 * lookup(order, lax.rem(pos + 1, chips)) + core
    pred = 2 * lookup(order, lax.rem(pos + chips - 1, chips)) + core

    barrier = pltpu.get_barrier_semaphore()

    def greet(d, carry):
        pl.semaphore_signal(barrier, inc=1, device_id={"tp": lax.rem(me + d, n)})
        return carry

    lax.fori_loop(1, n, greet, 0)

    own_wq = pltpu.make_async_copy(wq_hbm.at[:, core], wq.at[:, :, pl.ds(0, HD)], wl_sem)
    own_wq.start()

    def kv_local(k):
        cols = pl.ds(pl.multiple_of((2 * k + core) * depth, 128), depth)
        return pltpu.make_async_copy(wkv_hbm.at[:, cols], wkv.at[k, pl.ds(0, 16)], wkl_sem.at[k])

    def kv_remote(k):
        cols = pl.ds(pl.multiple_of((2 * k + 1 - core) * depth, 128), depth)
        return pltpu.make_async_remote_copy(
            wkv_hbm.at[:, cols], wkv.at[k, pl.ds(16, 16)], wkr_send.at[k], wkr_recv.at[k],
            device_id={"tp": mate},
        )

    mate_wq = pltpu.make_async_remote_copy(
        wq_hbm.at[:, 1 - core], wq.at[:, :, pl.ds(HD, HD)], wr_send, wr_recv, device_id={"tp": mate}
    )
    lax.fori_loop(0, chips, lambda k, c: (kv_local(k).start(), c)[1], 0)

    gain = gain_ref[...]
    for r in range(count // 128):
        block = pl.ds(r * 128, 128)
        wide = h_ref[block, :].astype(jnp.float32)
        weighted = wide * gain
        gath[0, block, :] = weighted.astype(jnp.bfloat16)
        square = jnp.sum(wide * wide, axis=1, keepdims=True)
        top = jnp.max(jnp.abs(weighted), axis=1, keepdims=True)
        stat_own[pl.ds(r, 1), :] = jnp.transpose(jnp.broadcast_to(square, (128, 128)))[0:1, :]
        stat_own[pl.ds(4 + r, 1), :] = jnp.transpose(jnp.broadcast_to(top, (128, 128)))[0:1, :]
    stats[me] = stat_own[...]

    pl.semaphore_wait(barrier, n - 1)

    def hop(step, way, piece):
        block = pl.ds(way * half + piece * rows, rows)
        return pltpu.make_async_remote_copy(
            gath.at[step, block], gath.at[step + 1, block],
            send_sem.at[step, way, piece], recv_sem.at[step, way, piece],
            device_id={"tp": succ if way == 0 else pred},
        )

    def multiply(step, way, piece):
        block = pl.ds(way * half + piece * rows, rows)
        shift = chips - step if way == 0 else step
        owner = lookup(order, lax.rem(pos + shift, chips))
        left = gath[step, block, :]
        acc[block, :] += jnp.dot(left, wq[owner], preferred_element_type=jnp.float32)
        kvacc[block, :] += lax.dot_general(
            left, wkv[owner], (((1,), (1,)), ((), ())), preferred_element_type=jnp.float32
        )

    for piece in range(PIECES):
        for way in range(2):
            hop(0, way, piece).start()
    mate_wq.start()
    lax.fori_loop(0, chips, lambda k, c: (kv_remote(k).start(), c)[1], 0)

    def stat_copy(d):
        return pltpu.make_async_remote_copy(
            stat_own, stats.at[me], st_send.at[d], st_recv.at[d], device_id={"tp": lax.rem(me + d, n)}
        )

    lax.fori_loop(1, n, lambda d, c: (stat_copy(d).start(), c)[1], 0)

    acc[...] = jnp.zeros_like(acc)
    kvacc[...] = jnp.zeros_like(kvacc)
    token = lax.broadcasted_iota(jnp.int32, (128, HD), 0) + prefix_ref[0]
    freq = freq_ref[...]
    even = lax.rem(lax.broadcasted_iota(jnp.int32, (128, HD), 1), 2) == 0
    for r in range(count // 128):
        angle = (token + r * 128).astype(jnp.float32) * freq
        cosine[pl.ds(r * 128, 128), :] = jnp.cos(angle)
        turn = jnp.sin(angle)
        sine[pl.ds(r * 128, 128), :] = jnp.where(even, -turn, turn)

    lax.fori_loop(1, n, lambda d, c: (stat_copy(d).wait(), c)[1], 0)
    everything = stats[...]
    inverse = 1.0 / jnp.sqrt(jnp.sum(everything[:, 0:4, :], axis=0) / width + norm_eps)
    row_scale = jnp.max(everything[:, 4:8, :], axis=0) * inverse + tiny_eps
    rs_out[...] = row_scale
    for r in range(count // 128):
        block = pl.ds(r * 128, 128)
        inv = spread(inverse[r : r + 1, :])
        inv_col[block, :] = inv
        scale = spread(row_scale[r : r + 1, :])
        for j in range(depth // 128):
            lanes = pl.ds(j * 128, 128)
            weighted = h_ref[block, lanes].astype(jnp.float32) * gain[:, j * 128 : j * 128 + 128]
            payload_out[block, lanes] = (weighted * inv / scale).astype(jnp.bfloat16)

    own_wq.wait()
    lax.fori_loop(0, chips, lambda k, c: (kv_local(k).wait(), c)[1], 0)
    mate_wq.wait()
    lax.fori_loop(0, chips, lambda k, c: (kv_remote(k).wait(), c)[1], 0)

    for piece in range(PIECES):
        for way in range(2):
            multiply(0, way, piece)

    def ring_step(step, carry):
        for piece in range(PIECES):
            for way in range(2):
                hop(step - 1, way, piece).wait_recv()
                hop(step, way, piece).start()
                multiply(step, way, piece)
        return carry

    lax.fori_loop(1, chips - 1, ring_step, 0)
    for piece in range(PIECES):
        for way in range(2):
            hop(chips - 2, way, piece).wait_recv()
            multiply(chips - 1, way, piece)

    ex_kv = pltpu.make_async_remote_copy(
        kvacc, part_kv, ex_send.at[0], ex_recv.at[0], device_id={"tp": mate}
    )
    ex_q = pltpu.make_async_remote_copy(
        acc.at[:, pl.ds(HD, HD)], part_q, ex_send.at[1], ex_recv.at[1], device_id={"tp": mate}
    )
    ex_kv.start()
    ex_q.start()

    def drain(step, carry):
        for piece in range(PIECES):
            for way in range(2):
                hop(step, way, piece).wait_send()
        return carry

    lax.fori_loop(0, chips - 1, drain, 0)
    ex_kv.wait()
    kvscale = kvscale_ref[...]
    for r in range(count // 128):
        block = pl.ds(r * 128, 128)
        cols = (kvacc[block, 0:16] + part_kv[block, 16:32]) * inv_col[block, 0:16] * kvscale
        cols = jnp.concatenate([cols, jnp.zeros((128, 112), jnp.float32)], axis=1)
        kv_own[:, block] = jnp.transpose(cols)[0:16, :].astype(jnp.bfloat16)

    my_head = me * kv_heads // n
    group = lax.rem(me, kv_heads)
    slot = me // kv_heads

    def kv_copy(i):
        return pltpu.make_async_remote_copy(
            kv_own, kv_all.at[slot], kv_send.at[i], kv_recv.at[slot],
            device_id={"tp": group * pieces + i},
        )

    def kv_arrival(i):
        return pltpu.make_async_remote_copy(
            kv_own, kv_all.at[i], kv_send.at[i], kv_recv.at[i], device_id={"tp": mate}
        )

    def kv_start(i, carry):
        @pl.when(group * pieces + i != me)
        def _():
            kv_copy(i).start()

        return carry

    def kv_wait(i, carry):
        @pl.when(group * pieces + i != me)
        def _():
            kv_copy(i).wait_send()

        @pl.when(i * kv_heads + my_head != me)
        def _():
            kv_arrival(i).wait_recv()

        return carry

    @pl.when(my_head == group)
    def _():
        kv_all[slot] = kv_own[...]

    lax.fori_loop(0, pieces, kv_start, 0)

    def rotated(x, block):
        swapped = jnp.where(even, pltpu.roll(x, HD - 1, 1), pltpu.roll(x, 1, 1))
        return (x * cosine[block, :] + swapped * sine[block, :]).astype(jnp.bfloat16)

    ex_q.wait()
    qscale = qscale_ref[...]
    for r in range(count // 128):
        block = pl.ds(r * 128, 128)
        x = (acc[block, 0:HD] + part_q[block, :]) * inv_col[block, :] * qscale
        q_out[block, :] = rotated(x, block)

    lax.fori_loop(0, pieces, kv_wait, 0)
    for r in range(count // 128):
        block = pl.ds(r * 128, 128)
        both = kv_all[:, :, block].astype(jnp.float32)
        keys = jnp.transpose(both[:, 0:KV_COLS_DEV, :].reshape(HD, 128))
        k_out[block, :] = rotated(keys, block)
        values = jnp.transpose(both[:, KV_COLS_DEV:, :].reshape(HD, 128))
        v_out[block, :] = values.astype(jnp.bfloat16)


def grid_kernel(
    width, prefix_ref, h_hbm, gain_hbm, freq_hbm, scale_hbm, wq_hbm, wkv_hbm,
    q_out, k_out, v_out, payload_out, rs_out,
    gath, wq, wkv, wq_late, acc, kvacc, q_give, q_got, kv_give, kv_got,
    stat_own, stat_mate, stats, kv_own, kv_all, kv_tail, inv_row, inv_col, cosine, sine,
    h_ref, gain_ref, scale_ref, freq_ref, in_sem, own_sem, late_send, late_recv,
    st_send, st_recv, w_send, w_recv, wx_recv, wy_recv, act_send, act_recv, mate_send, mate_recv,
    pq_send, pq_recv, pkv_send, pkv_recv, kv_send, kv_recv,
):
    n = 16
    me = lax.axis_index("tp")
    side = lax.axis_index("grp")
    core = lax.rem(me, 2)
    chip = me // 2
    y = lax.rem(chip, 2)
    z = chip // 2
    mate = me + 1 - 2 * core
    is_end = (z == 0) | (z == 3)
    is_mid = (z == 1) | (z == 2)
    inner = z + 1 - 2 * lax.rem(z, 2)
    across = me + 4 * (3 - 2 * z)
    beside = me + 2 - 4 * y
    peers = [me, beside, me + 4 * (inner - z), beside + 4 * (inner - z)]
    places = [(z, y), (z, 1 - y), (inner, y), (inner, 1 - y)]
    count, depth = h_ref.shape
    kv_cols = 2 * KV_COLS_DEV
    rows = count // GRID_PIECES
    everyone = range(GRID_PIECES)
    last = GRID_PIECES - 1

    barrier = pltpu.get_barrier_semaphore()

    def greet(d, carry):
        pl.semaphore_signal(barrier, inc=1, device_id={"tp": lax.rem(me + d, n)})
        return carry

    lax.fori_loop(1, n, greet, 0)
    pl.semaphore_signal(barrier, inc=1, device_id={"grp": 1 - side, "tp": me})

    loads = [pltpu.make_async_copy(gain_hbm, gain_ref, in_sem.at[0])]
    for r in range(count // 128):
        block = pl.ds(r * 128, 128)
        loads.append(pltpu.make_async_copy(h_hbm.at[block], h_ref.at[block], in_sem.at[r + 1]))
    loads.append(pltpu.make_async_copy(scale_hbm, scale_ref, in_sem.at[count // 128 + 1]))
    loads.append(pltpu.make_async_copy(freq_hbm, freq_ref, in_sem.at[count // 128 + 2]))
    for load in loads:
        load.start()

    def weights(s, k, half, kv):
        zt, yt = places[s]
        block = 2 * (2 * (zt + k * (3 - 2 * zt)) + yt) + half
        if not kv:
            first = pl.ds(0, depth - LATE if s == 2 and k else depth)
            return wq_hbm.at[block, first], wq.at[k, half, first, pl.ds(s * HD, HD)]
        cols = pl.ds(pl.multiple_of(block * depth, 128), depth)
        return wkv_hbm.at[:, cols], wkv.at[k, half, pl.ds(s * kv_cols, kv_cols)]

    def weights_own(k, half, kv):
        source, target = weights(0, k, half, kv)
        return pltpu.make_async_copy(source, target, own_sem.at[k, kv])

    def weights_beside(k, half, kv):
        source, target = weights(1, k, half, kv)
        return pltpu.make_async_remote_copy(
            source, target, w_send.at[kv], wy_recv.at[k, kv], device_id={"tp": beside}
        )

    def weights_far(s, k, kv):
        source, target = weights(s, k, side, kv)
        return pltpu.make_async_remote_copy(
            source, target, w_send.at[4 if kv else 2 + k], w_recv.at[s - 2, k, kv], device_id={"tp": peers[s]}
        )

    def weights_twin(s, k, kv):
        piece = weights(s, k, side, kv)[1]
        return pltpu.make_async_remote_copy(
            piece, piece, w_send.at[7 if kv else 5 + k], wx_recv.at[k, kv], device_id={"grp": 1 - side, "tp": me}
        )

    def weights_late(half):
        block = 2 * (2 * (inner + 3 - 2 * inner) + y) + half
        return pltpu.make_async_remote_copy(
            wq_hbm.at[block, pl.ds(depth - LATE, LATE)], wq_late.at[half], late_send, late_recv,
            device_id={"tp": peers[2]},
        )

    def every(ref, send_sem, recv_sem):
        return pltpu.make_async_remote_copy(ref, ref, send_sem, recv_sem, device_id={"tp": mate})

    def shared_q(k):
        return wq.at[k, :, pl.ds(0, depth - k * LATE // 2), pl.ds(0, HD)]

    def weights_arrive(k):
        for kv in (1, 0):
            whole = wkv.at[k, :, pl.ds(0, kv_cols)] if kv else wq.at[k, :, :, pl.ds(0, HD)]
            for sem in (own_sem, wy_recv):
                every(whole, sem.at[k, kv], sem.at[k, kv]).wait_recv()
            every(whole if kv else shared_q(k), wx_recv.at[k, kv], wx_recv.at[k, kv]).wait_recv()

    for k in range(2):
        for half in range(2):
            for kv in range(2):
                weights_own(k, half, kv).start()

    wq[1, :, depth - LATE :, 2 * HD : 3 * HD] = jnp.zeros((2, LATE, HD), jnp.bfloat16)
    loads[0].wait()
    gain = gain_ref[...]
    for r in range(count // 128):
        block = pl.ds(r * 128, 128)
        loads[r + 1].wait()
        wide = h_ref[block, :].astype(jnp.float32)
        weighted = wide * gain
        gath[core, block, :] = weighted.astype(jnp.bfloat16)
        square = jnp.sum(wide * wide, axis=1, keepdims=True)
        top = jnp.max(jnp.abs(weighted), axis=1, keepdims=True)
        stat_own[pl.ds(r, 1), :] = jnp.transpose(jnp.broadcast_to(square, (128, 128)))[0:1, :]
        stat_own[pl.ds(4 + r, 1), :] = jnp.transpose(jnp.broadcast_to(top, (128, 128)))[0:1, :]
    loads[-2].wait()
    loads[-1].wait()

    pl.semaphore_wait(barrier, n)

    def stat_pair():
        return pltpu.make_async_remote_copy(
            stat_own, stat_mate, st_send.at[0], st_recv.at[0], device_id={"tp": mate}
        )

    def stat_copy(d):
        return pltpu.make_async_remote_copy(
            stats.at[chip], stats.at[chip], st_send.at[1], st_recv.at[1],
            device_id={"tp": lax.rem(me + 2 * d, n)},
        )

    def stat_all():
        others = stats.at[pl.ds(1, n // 2 - 1)]
        return pltpu.make_async_remote_copy(
            others, others, st_send.at[1], st_recv.at[1], device_id={"tp": mate}
        )

    def act_mate():
        return pltpu.make_async_remote_copy(
            gath.at[core], gath.at[core], mate_send, mate_recv.at[GRID_PIECES],
            device_id={"tp": mate},
        )

    def act_across(p):
        block = pl.ds(p * rows, rows)
        return pltpu.make_async_remote_copy(
            gath.at[core, block], gath.at[2 + core, block], act_send, act_recv.at[p],
            device_id={"tp": across},
        )

    def act_pass(p):
        block = pl.ds(p * rows, rows)
        piece = gath.at[2 + core, block]
        return pltpu.make_async_remote_copy(
            piece, piece, mate_send, mate_recv.at[p], device_id={"tp": mate}
        )

    forwarded = [(s, k, kv) for k in (0, 1) for kv in (1, 0) for s in (2, 3)]
    def weights_beside_all(k, kv):
        for half in range(2):
            weights_beside(k, half, kv).start()

    stat_pair().start()
    for each in forwarded[:2]:
        weights_far(*each).start()
    weights_beside_all(0, 1)
    stat_pair().wait()
    mine, other = stat_own[...], stat_mate[...]
    stats[chip, 0:4] = mine[0:4] + other[0:4]
    stats[chip, 4:8] = jnp.maximum(mine[4:8], other[4:8])
    lax.fori_loop(1, n // 2, lambda d, c: (stat_copy(d).start(), c)[1], 0)
    for each in forwarded[2:]:
        weights_far(*each).start()

    @pl.when(is_mid)
    def _():
        for p in everyone:
            act_across(p).start()

    act_mate().start()
    weights_beside_all(0, 0)
    weights_beside_all(1, 1)
    weights_beside_all(1, 0)

    even = lax.rem(lax.broadcasted_iota(jnp.int32, (128, HD), 1), 2) == 0
    token = lax.broadcasted_iota(jnp.int32, (128, HD), 0) + prefix_ref[0]
    freq = freq_ref[...]
    for r in range(count // 128):
        angle = (token + r * 128).astype(jnp.float32) * freq
        cosine[pl.ds(r * 128, 128), :] = jnp.cos(angle)
        turn = jnp.sin(angle)
        sine[pl.ds(r * 128, 128), :] = jnp.where(even, -turn, turn)

    for each in forwarded[:-1]:
        weights_far(*each).wait_recv()
        weights_twin(*each).start()

    @pl.when(is_end)
    def _():
        for p in everyone:
            act_across(p).start()

    weights_far(*forwarded[-1]).wait_recv()
    weights_twin(*forwarded[-1]).start()

    stat_all().wait()
    everything = stats[...]
    inverse = 1.0 / jnp.sqrt(jnp.sum(everything[:, 0:4, :], axis=0) / width + norm_eps)
    row_scale = jnp.max(everything[:, 4:8, :], axis=0) * inverse + tiny_eps
    rs_out[...] = row_scale
    inv_row[...] = inverse
    for r in range(count // 128):
        block = pl.ds(r * 128, 128)
        inv = spread(inverse[r : r + 1, :])
        inv_col[block, :] = inv
        scale = spread(row_scale[r : r + 1, :])
        for j in range(depth // 128):
            lanes = pl.ds(j * 128, 128)
            weighted = h_ref[block, lanes].astype(jnp.float32) * gain_ref[:, lanes]
            payload_out[block, lanes] = (weighted * inv / scale).astype(jnp.bfloat16)

    @pl.when(is_mid)
    def _():
        for p in everyone:
            act_across(p).wait_recv()
            act_pass(p).start()

    act_mate().wait_recv()
    weights_arrive(0)

    def product(slot, block, k, half):
        return jnp.dot(gath[slot, block, :], wq[k, half], preferred_element_type=jnp.float32)

    def kv_product(slot, block, k, half):
        return lax.dot_general(
            wkv[k, half], gath[slot, block, :], (((1,), (1,)), ((), ())), preferred_element_type=jnp.float32
        )

    for p in everyone:
        block = pl.ds(p * rows, rows)
        kvacc[p] = kv_product(0, block, 0, 0) + kv_product(1, block, 0, 1)
        acc[block, :] = product(0, block, 0, 0) + product(1, block, 0, 1)

    weights_arrive(1)

    def q_beside(p):
        block = pl.ds(p * rows, rows)
        return pltpu.make_async_remote_copy(
            q_give.at[pl.ds(0, 2), block], q_got.at[pl.ds(0, 2), block], pq_send.at[0], pq_recv.at[0, p],
            device_id={"tp": beside},
        )

    def q_along(p):
        block = pl.ds(p * rows, rows)
        return pltpu.make_async_remote_copy(
            q_give.at[2, block], q_got.at[2, block], pq_send.at[1], pq_recv.at[1, p],
            device_id={"tp": peers[2]},
        )

    def kv_partial(s, p):
        return pltpu.make_async_remote_copy(
            kv_give.at[s - 1, p], kv_got.at[s - 1, p], pkv_send, pkv_recv.at[p],
            device_id={"tp": peers[s]},
        )

    def near(p):
        block = pl.ds(p * rows, rows)
        kvacc[p] += kv_product(2 + core, block, 1, core)
        acc[block, :] += product(2 + core, block, 1, core)

    def far(p):
        block = pl.ds(p * rows, rows)
        act_pass(p).wait_recv()
        pair = kvacc[p] + kv_product(3 - core, block, 1, 1 - core)
        kvacc[p] = pair
        for s in range(1, 4):
            kv_give[s - 1, p] = pair[s * kv_cols : (s + 1) * kv_cols, :].astype(jnp.bfloat16)
        for s in range(1, 4):
            kv_partial(s, p).start()
        whole = acc[block, :] + product(3 - core, block, 1, 1 - core)
        acc[block, :] = whole
        q_give[0, block, :] = whole[:, HD : 2 * HD].astype(jnp.bfloat16)
        q_give[1, block, :] = whole[:, 3 * HD :].astype(jnp.bfloat16)
        q_beside(p).start()

    def late_arrive():
        every(wq_late, late_recv, late_recv).wait_recv()

    def q_combine(p):
        block = pl.ds(p * rows, rows)
        x = acc[block, 2 * HD : 3 * HD]
        for half in range(2):
            x = x + jnp.dot(
                gath[2 + half, block, depth - LATE :], wq_late[half], preferred_element_type=jnp.float32
            )
        q_beside(p).wait_recv()
        q_give[2, block, :] = (x + q_got[1, block, :].astype(jnp.float32)).astype(jnp.bfloat16)
        q_along(p).start()

    kv_scale = jnp.concatenate([scale_ref[:, HD:], jnp.zeros((1, 128 - kv_cols), jnp.float32)], axis=1)
    kv_scale = spread(kv_scale)[0:kv_cols, :]
    qscale = scale_ref[:, 0:HD]

    def kv_copy(p, d):
        return pltpu.make_async_remote_copy(
            kv_own.at[p], kv_tail.at[me] if p == last else kv_all.at[core, chip, p], kv_send.at[int(p == last)], kv_recv.at[p],
            device_id={"tp": lax.rem(me + d, n)},
        )

    kv_final = kv_tail.at[pl.ds(1, n - 1)]
    kv_mine = kv_all.at[core, :, pl.ds(0, last)]
    kv_spread_all = pltpu.make_async_remote_copy(
        kv_mine, kv_mine, kv_send.at[2], kv_recv.at[GRID_PIECES], device_id={"tp": mate}
    )

    def kv_reduce(p):
        total = kvacc[p, 0:kv_cols, :]
        every(kv_got.at[:, p], pkv_send, pkv_recv.at[p]).wait_recv()
        for s in range(1, 4):
            total = total + kv_got[s - 1, p].astype(jnp.float32)
        mine = (total * inv_row[p : p + 1, :] * kv_scale).astype(jnp.bfloat16)
        kv_own[p] = mine
        if p == last:
            kv_tail[me] = mine
            lax.fori_loop(1, n, lambda d, c: (kv_copy(p, d).start(), c)[1], 0)
        else:
            kv_all[core, chip, p] = mine
            lax.fori_loop(1, n // 2, lambda d, c: (kv_copy(p, 2 * d).start(), c)[1], 0)

    def rotated(x, block):
        swapped = jnp.where(even, pltpu.roll(x, HD - 1, 1), pltpu.roll(x, 1, 1))
        return (x * cosine[block, :] + swapped * sine[block, :]).astype(jnp.bfloat16)

    def q_reduce(p):
        block = pl.ds(p * rows, rows)
        x = acc[block, 0:HD]
        q_along(p).wait_recv()
        x = x + q_got[0, block, :].astype(jnp.float32) + q_got[2, block, :].astype(jnp.float32)
        q_out[block, :] = rotated(x * inv_col[block, :] * qscale, block)

    def heads(p):
        block = pl.ds(p * rows, rows)
        if p == last:
            every(kv_final, kv_send.at[1], kv_recv.at[p]).wait_recv()
        elif p == 0:
            kv_spread_all.wait_recv()
        if p == last:
            pair = kv_tail[...].astype(jnp.float32)
        else:
            both = kv_all[:, :, p].astype(jnp.float32)
            pair = jnp.stack([both[0], both[1]], axis=1).reshape(n, kv_cols, 128)
        keys = jnp.transpose(pair[:, 0:KV_COLS_DEV, :].reshape(HD, 128))
        k_out[block, :] = rotated(keys, block)
        values = jnp.transpose(pair[:, KV_COLS_DEV:, :].reshape(HD, 128))
        v_out[block, :] = values.astype(jnp.bfloat16)

    @pl.when(is_mid)
    def _():
        for p in everyone:
            near(p)
        for p in everyone:
            far(p)
        for half in range(2):
            weights_late(half).start()
        for p in everyone:
            kv_reduce(p)
        late_arrive()
        for p in everyone:
            q_combine(p)

    @pl.when(is_end)
    def _():
        for p in everyone:
            act_across(p).wait_recv()
            act_pass(p).start()
            near(p)
            far(p)
            if p == last - 1:
                for half in range(2):
                    weights_late(half).start()
        for p in everyone:
            kv_reduce(p)
        late_arrive()
        for p in everyone:
            q_combine(p)

    for p in range(last):
        every(kv_all.at[0, pl.ds(1, n // 2 - 1), p], kv_recv.at[p], kv_recv.at[p]).wait_recv()
    kv_spread_all.start()
    for p in range(last):
        q_reduce(p)
    every(gath.at[0], act_send, act_send).wait_send()
    every(gath.at[pl.ds(0, 2)], mate_send, mate_send).wait_send()
    for i in (1, 4, 7):
        every(wkv.at[:, :, pl.ds(0, kv_cols)], w_send.at[i], w_send.at[i]).wait_send()
    every(wq.at[:, :, :, pl.ds(0, HD)], w_send.at[0], w_send.at[0]).wait_send()
    for i in (2, 5):
        for k in range(2):
            every(shared_q(k), w_send.at[i + k], w_send.at[i + k]).wait_send()
    every(wq_late, late_send, late_send).wait_send()
    for p in range(last):
        heads(p)
    q_reduce(last)
    every(kv_give, pkv_send, pkv_send).wait_send()
    every(q_give.at[pl.ds(0, 2)], pq_send.at[0], pq_send.at[0]).wait_send()
    every(q_give.at[2], pq_send.at[1], pq_send.at[1]).wait_send()
    every(kv_all.at[0, pl.ds(1, n // 2 - 1)], kv_send.at[0], kv_send.at[0]).wait_send()
    every(kv_final, kv_send.at[1], kv_send.at[1]).wait_send()
    kv_spread_all.wait_send()
    heads(last)


def grid_scratch(count, depth):
    dma = pltpu.SemaphoreType.DMA
    bf16, f32 = jnp.bfloat16, jnp.float32
    pieces, kv_cols = GRID_PIECES, 2 * KV_COLS_DEV
    rows = count // pieces
    return [
        pltpu.VMEM((4, count, depth), bf16),
        pltpu.VMEM((2, 2, depth, 4 * HD), bf16),
        pltpu.VMEM((2, 2, 4 * kv_cols, depth), bf16),
        pltpu.VMEM((2, LATE, HD), bf16),
        pltpu.VMEM((count, 4 * HD), f32),
        pltpu.VMEM((pieces, 4 * kv_cols, rows), f32),
        pltpu.VMEM((3, count, HD), bf16),
        pltpu.VMEM((3, count, HD), bf16),
        pltpu.VMEM((3, pieces, kv_cols, rows), bf16),
        pltpu.VMEM((3, pieces, kv_cols, rows), bf16),
        pltpu.VMEM((8, 128), f32),
        pltpu.VMEM((8, 128), f32),
        pltpu.VMEM((8, 8, 128), f32),
        pltpu.VMEM((pieces, kv_cols, rows), bf16),
        pltpu.VMEM((2, 8, pieces - 1, kv_cols, rows), bf16),
        pltpu.VMEM((16, kv_cols, rows), bf16),
        pltpu.VMEM((count // 128, 128), f32),
        pltpu.VMEM((count, HD), f32),
        pltpu.VMEM((count, HD), f32),
        pltpu.VMEM((count, HD), f32),
        pltpu.VMEM((count, depth), bf16),
        pltpu.VMEM((1, depth), f32),
        pltpu.VMEM((1, HD + kv_cols), f32),
        pltpu.VMEM((1, HD), f32),
        dma((count // 128 + 3,)),
        dma((2, 2)),
        dma,
        dma,
        dma((2,)),
        dma((2,)),
        dma((8,)),
        dma((2, 2, 2)),
        dma((2, 2)),
        dma((2, 2)),
        dma,
        dma((pieces,)),
        dma,
        dma((pieces + 1,)),
        dma((2,)),
        dma((2, pieces)),
        dma,
        dma((pieces,)),
        dma((3,)),
        dma((pieces + 1,)),
    ]


def finish_kernel(*refs):
    sources, targets, sems = refs[0:5], refs[5:10], refs[10]
    outs = [pltpu.make_async_copy(sources[i], targets[i], sems.at[i]) for i in range(5)]
    for copy in outs:
        copy.start()
    for copy in outs:
        copy.wait()


def finish(*arrays):
    return pl.pallas_call(
        finish_kernel,
        out_shape=tuple(jax.ShapeDtypeStruct(a.shape, a.dtype) for a in arrays),
        in_specs=[pl.BlockSpec(memory_space=pltpu.VMEM)] * 5,
        out_specs=(pl.BlockSpec(memory_space=pltpu.HBM),) * 5,
        scratch_shapes=[pltpu.SemaphoreType.DMA((5,))], compiler_params=pltpu.CompilerParams(vmem_limit_bytes=2 * 1024 * 1024),
    )(*arrays)


def local(n, groups, hidden, norm_gain, prefix, w_query, w_kv, w_scale):
    count, depth = hidden.shape
    chips = n // 2
    width = depth * n
    grid = n == 16 and groups == 2 and n * KV_COLS_DEV == HD and count == 128 * GRID_PIECES
    pair_index = np.arange(HD) // 2
    freq = jnp.asarray(np.power(rope_base, -(2.0 * pair_index) / HD)[None, :], jnp.float32)
    pieces = HD // KV_COLS_DEV
    vmem = pl.BlockSpec(memory_space=pltpu.VMEM)
    hbm = pl.BlockSpec(memory_space=pltpu.HBM if grid else pl.ANY)
    dma = pltpu.SemaphoreType.DMA
    bf16, f32 = jnp.bfloat16, jnp.float32
    queries, keys, values, payload, row_scale = pl.pallas_call(
        functools.partial(grid_kernel, width) if grid else functools.partial(kernel, n, width),
        out_shape=(
            pltpu.VMEM((count, HD), bf16),
            pltpu.VMEM((count, HD), bf16),
            pltpu.VMEM((count, HD), bf16),
            pltpu.VMEM((count, depth), bf16),
            pltpu.VMEM((count // 128, 128), f32),
        ),
        in_specs=[pl.BlockSpec(memory_space=pltpu.SMEM)]
        + ([hbm] * 6 if grid else [vmem] * 5 + [hbm] * 2),
        out_specs=(vmem,) * 5,
        scratch_shapes=grid_scratch(count, depth) if grid else [
            pltpu.VMEM((chips, count, depth), bf16),
            pltpu.VMEM((chips, depth, 2 * HD), bf16),
            pltpu.VMEM((chips, 32, depth), bf16),
            pltpu.VMEM((count, 2 * HD), f32),
            pltpu.VMEM((count, 32), f32),
            pltpu.VMEM((count, HD), f32),
            pltpu.VMEM((count, 32), f32),
            pltpu.VMEM((8, 128), f32),
            pltpu.VMEM((n, 8, 128), f32),
            pltpu.VMEM((2 * KV_COLS_DEV, count), bf16),
            pltpu.VMEM((pieces, 2 * KV_COLS_DEV, count), bf16),
            pltpu.VMEM((count, HD), f32),
            pltpu.VMEM((count, HD), f32),
            pltpu.VMEM((count, HD), f32),
            dma((chips, 2, PIECES)),
            dma((chips, 2, PIECES)),
            dma((n,)),
            dma((n,)),
            dma((pieces,)),
            dma((pieces,)),
            dma,
            dma((chips,)),
            dma,
            dma,
            dma((chips,)),
            dma((chips,)),
            dma((2,)),
            dma((2,)),
        ],
        compiler_params=pltpu.CompilerParams(
            collective_id=0, has_side_effects=True, vmem_limit_bytes=(60 if grid else 48) * 1024 * 1024
        ),
    )(
        prefix,
        hidden,
        norm_gain[None, :],
        freq,
        *([w_scale[None, :]] if grid else [w_scale[None, :HD], w_scale[None, HD:]]),
        w_query.reshape(n, depth, HD) if grid else w_query.reshape(chips, 2, depth, HD),
        w_kv,
    )
    queries, keys, values, payload, row_scale = finish(queries, keys, values, payload, row_scale)
    return queries, keys, values, payload, row_scale.reshape(count)


def solution(mesh):
    return jax.shard_map(
        functools.partial(local, mesh.shape["tp"], mesh.shape["grp"]),
        mesh=mesh,
        in_specs=(P("grp", "tp"), P("tp"), P("grp"), P(None, "tp"), P("tp", None), P("tp")),
        out_specs=(P("grp", "tp"), P("grp", "tp"), P("grp", "tp"), P("grp", "tp"), P("grp")),
        check_vma=False,
    )
```

```python
import functools

import jax
import jax.numpy as jnp
import numpy as np
from jax import lax
from jax.experimental import pallas as pl
from jax.experimental.pallas import tpu as pltpu
from jax.sharding import PartitionSpec as P

HD = 128
KV_COLS_DEV = 8
norm_eps = 1e-05
tiny_eps = 1e-06
rope_base = 500000.0
PIECES = 2
GRID_PIECES = 4
LATE = 256


def ring_order(chips):
    cols = 1
    while (2 * cols) * (2 * cols) <= chips and chips % (2 * cols) == 0:
        cols *= 2
    rows = chips // cols
    if cols < 2 or rows % 2:
        return list(range(chips))
    order = [0]
    for row in range(rows):
        span = range(1, cols) if row % 2 == 0 else range(cols - 1, 0, -1)
        order += [row * cols + col for col in span]
    order += [row * cols for row in range(rows - 1, 0, -1)]
    return order


def lookup(table, index):
    total = jnp.int32(0)
    for key, value in enumerate(table):
        total = total + jnp.where(index == key, jnp.int32(value), jnp.int32(0))
    return total


def spread(row):
    return jnp.transpose(jnp.broadcast_to(row, (128, 128)))


def kernel(
    n, width, prefix_ref, h_ref, gain_ref, freq_ref, qscale_ref, kvscale_ref, wq_hbm, wkv_hbm,
    q_out, k_out, v_out, payload_out, rs_out,
    gath, wq, wkv, acc, kvacc, part_q, part_kv, stat_own, stats, kv_own, kv_all, inv_col, cosine, sine,
    send_sem, recv_sem, st_send, st_recv, kv_send, kv_recv,
    wl_sem, wkl_sem, wr_send, wr_recv, wkr_send, wkr_recv, ex_send, ex_recv,
):
    me = lax.axis_index("tp")
    chips = n // 2
    core = lax.rem(me, 2)
    chip = me // 2
    mate = me + 1 - 2 * core
    count, depth = h_ref.shape
    half = count // 2
    rows = half // PIECES
    pieces = HD // KV_COLS_DEV
    kv_heads = n // pieces
    order = ring_order(chips)
    place = [order.index(c) for c in range(chips)]
    pos = lookup(place, chip)
    succ = 2 * lookup(order, lax.rem(pos + 1, chips)) + core
    pred = 2 * lookup(order, lax.rem(pos + chips - 1, chips)) + core

    barrier = pltpu.get_barrier_semaphore()

    def greet(d, carry):
        pl.semaphore_signal(barrier, inc=1, device_id={"tp": lax.rem(me + d, n)})
        return carry

    lax.fori_loop(1, n, greet, 0)

    own_wq = pltpu.make_async_copy(wq_hbm.at[:, core], wq.at[:, :, pl.ds(0, HD)], wl_sem)
    own_wq.start()

    def kv_local(k):
        cols = pl.ds(pl.multiple_of((2 * k + core) * depth, 128), depth)
        return pltpu.make_async_copy(wkv_hbm.at[:, cols], wkv.at[k, pl.ds(0, 16)], wkl_sem.at[k])

    def kv_remote(k):
        cols = pl.ds(pl.multiple_of((2 * k + 1 - core) * depth, 128), depth)
        return pltpu.make_async_remote_copy(
            wkv_hbm.at[:, cols], wkv.at[k, pl.ds(16, 16)], wkr_send.at[k], wkr_recv.at[k],
            device_id={"tp": mate},
        )

    mate_wq = pltpu.make_async_remote_copy(
        wq_hbm.at[:, 1 - core], wq.at[:, :, pl.ds(HD, HD)], wr_send, wr_recv, device_id={"tp": mate}
    )
    lax.fori_loop(0, chips, lambda k, c: (kv_local(k).start(), c)[1], 0)

    gain = gain_ref[...]
    for r in range(count // 128):
        block = pl.ds(r * 128, 128)
        wide = h_ref[block, :].astype(jnp.float32)
        weighted = wide * gain
        gath[0, block, :] = weighted.astype(jnp.bfloat16)
        square = jnp.sum(wide * wide, axis=1, keepdims=True)
        top = jnp.max(jnp.abs(weighted), axis=1, keepdims=True)
        stat_own[pl.ds(r, 1), :] = jnp.transpose(jnp.broadcast_to(square, (128, 128)))[0:1, :]
        stat_own[pl.ds(4 + r, 1), :] = jnp.transpose(jnp.broadcast_to(top, (128, 128)))[0:1, :]
    stats[me] = stat_own[...]

    pl.semaphore_wait(barrier, n - 1)

    def hop(step, way, piece):
        block = pl.ds(way * half + piece * rows, rows)
        return pltpu.make_async_remote_copy(
            gath.at[step, block], gath.at[step + 1, block],
            send_sem.at[step, way, piece], recv_sem.at[step, way, piece],
            device_id={"tp": succ if way == 0 else pred},
        )

    def multiply(step, way, piece):
        block = pl.ds(way * half + piece * rows, rows)
        shift = chips - step if way == 0 else step
        owner = lookup(order, lax.rem(pos + shift, chips))
        left = gath[step, block, :]
        acc[block, :] += jnp.dot(left, wq[owner], preferred_element_type=jnp.float32)
        kvacc[block, :] += lax.dot_general(
            left, wkv[owner], (((1,), (1,)), ((), ())), preferred_element_type=jnp.float32
        )

    for piece in range(PIECES):
        for way in range(2):
            hop(0, way, piece).start()
    mate_wq.start()
    lax.fori_loop(0, chips, lambda k, c: (kv_remote(k).start(), c)[1], 0)

    def stat_copy(d):
        return pltpu.make_async_remote_copy(
            stat_own, stats.at[me], st_send.at[d], st_recv.at[d], device_id={"tp": lax.rem(me + d, n)}
        )

    lax.fori_loop(1, n, lambda d, c: (stat_copy(d).start(), c)[1], 0)

    acc[...] = jnp.zeros_like(acc)
    kvacc[...] = jnp.zeros_like(kvacc)
    token = lax.broadcasted_iota(jnp.int32, (128, HD), 0) + prefix_ref[0]
    freq = freq_ref[...]
    even = lax.rem(lax.broadcasted_iota(jnp.int32, (128, HD), 1), 2) == 0
    for r in range(count // 128):
        angle = (token + r * 128).astype(jnp.float32) * freq
        cosine[pl.ds(r * 128, 128), :] = jnp.cos(angle)
        turn = jnp.sin(angle)
        sine[pl.ds(r * 128, 128), :] = jnp.where(even, -turn, turn)

    lax.fori_loop(1, n, lambda d, c: (stat_copy(d).wait(), c)[1], 0)
    everything = stats[...]
    inverse = 1.0 / jnp.sqrt(jnp.sum(everything[:, 0:4, :], axis=0) / width + norm_eps)
    row_scale = jnp.max(everything[:, 4:8, :], axis=0) * inverse + tiny_eps
    rs_out[...] = row_scale
    for r in range(count // 128):
        block = pl.ds(r * 128, 128)
        inv = spread(inverse[r : r + 1, :])
        inv_col[block, :] = inv
        scale = spread(row_scale[r : r + 1, :])
        for j in range(depth // 128):
            lanes = pl.ds(j * 128, 128)
            weighted = h_ref[block, lanes].astype(jnp.float32) * gain[:, j * 128 : j * 128 + 128]
            payload_out[block, lanes] = (weighted * inv / scale).astype(jnp.bfloat16)

    own_wq.wait()
    lax.fori_loop(0, chips, lambda k, c: (kv_local(k).wait(), c)[1], 0)
    mate_wq.wait()
    lax.fori_loop(0, chips, lambda k, c: (kv_remote(k).wait(), c)[1], 0)

    for piece in range(PIECES):
        for way in range(2):
            multiply(0, way, piece)

    def ring_step(step, carry):
        for piece in range(PIECES):
            for way in range(2):
                hop(step - 1, way, piece).wait_recv()
                hop(step, way, piece).start()
                multiply(step, way, piece)
        return carry

    lax.fori_loop(1, chips - 1, ring_step, 0)
    for piece in range(PIECES):
        for way in range(2):
            hop(chips - 2, way, piece).wait_recv()
            multiply(chips - 1, way, piece)

    ex_kv = pltpu.make_async_remote_copy(
        kvacc, part_kv, ex_send.at[0], ex_recv.at[0], device_id={"tp": mate}
    )
    ex_q = pltpu.make_async_remote_copy(
        acc.at[:, pl.ds(HD, HD)], part_q, ex_send.at[1], ex_recv.at[1], device_id={"tp": mate}
    )
    ex_kv.start()
    ex_q.start()

    def drain(step, carry):
        for piece in range(PIECES):
            for way in range(2):
                hop(step, way, piece).wait_send()
        return carry

    lax.fori_loop(0, chips - 1, drain, 0)
    ex_kv.wait()
    kvscale = kvscale_ref[...]
    for r in range(count // 128):
        block = pl.ds(r * 128, 128)
        cols = (kvacc[block, 0:16] + part_kv[block, 16:32]) * inv_col[block, 0:16] * kvscale
        cols = jnp.concatenate([cols, jnp.zeros((128, 112), jnp.float32)], axis=1)
        kv_own[:, block] = jnp.transpose(cols)[0:16, :].astype(jnp.bfloat16)

    my_head = me * kv_heads // n
    group = lax.rem(me, kv_heads)
    slot = me // kv_heads

    def kv_copy(i):
        return pltpu.make_async_remote_copy(
            kv_own, kv_all.at[slot], kv_send.at[i], kv_recv.at[slot],
            device_id={"tp": group * pieces + i},
        )

    def kv_arrival(i):
        return pltpu.make_async_remote_copy(
            kv_own, kv_all.at[i], kv_send.at[i], kv_recv.at[i], device_id={"tp": mate}
        )

    def kv_start(i, carry):
        @pl.when(group * pieces + i != me)
        def _():
            kv_copy(i).start()

        return carry

    def kv_wait(i, carry):
        @pl.when(group * pieces + i != me)
        def _():
            kv_copy(i).wait_send()

        @pl.when(i * kv_heads + my_head != me)
        def _():
            kv_arrival(i).wait_recv()

        return carry

    @pl.when(my_head == group)
    def _():
        kv_all[slot] = kv_own[...]

    lax.fori_loop(0, pieces, kv_start, 0)

    def rotated(x, block):
        swapped = jnp.where(even, pltpu.roll(x, HD - 1, 1), pltpu.roll(x, 1, 1))
        return (x * cosine[block, :] + swapped * sine[block, :]).astype(jnp.bfloat16)

    ex_q.wait()
    qscale = qscale_ref[...]
    for r in range(count // 128):
        block = pl.ds(r * 128, 128)
        x = (acc[block, 0:HD] + part_q[block, :]) * inv_col[block, :] * qscale
        q_out[block, :] = rotated(x, block)

    lax.fori_loop(0, pieces, kv_wait, 0)
    for r in range(count // 128):
        block = pl.ds(r * 128, 128)
        both = kv_all[:, :, block].astype(jnp.float32)
        keys = jnp.transpose(both[:, 0:KV_COLS_DEV, :].reshape(HD, 128))
        k_out[block, :] = rotated(keys, block)
        values = jnp.transpose(both[:, KV_COLS_DEV:, :].reshape(HD, 128))
        v_out[block, :] = values.astype(jnp.bfloat16)


def grid_kernel(
    width, prefix_ref, h_hbm, gain_hbm, freq_hbm, scale_hbm, wq_hbm, wkv_hbm,
    q_out, k_out, v_out, payload_out, rs_out,
    gath, wq, wkv, wq_late, acc, kvacc, q_give, q_got, kv_give, kv_got,
    stat_own, stat_mate, stats, kv_own, kv_all, kv_tail, inv_row, inv_col, cosine, sine,
    h_ref, gain_ref, scale_ref, freq_ref, in_sem, own_sem, late_send, late_recv, met,
    st_send, st_recv, w_send, w_recv, wx_recv, wy_recv, act_send, act_recv, mate_send, mate_recv,
    pq_send, pq_recv, pkv_send, pkv_recv, kv_send, kv_recv,
):
    n = 16
    me = lax.axis_index("tp")
    side = lax.axis_index("grp")
    core = lax.rem(me, 2)
    chip = me // 2
    y = lax.rem(chip, 2)
    z = chip // 2
    mate = me + 1 - 2 * core
    is_end = (z == 0) | (z == 3)
    is_mid = (z == 1) | (z == 2)
    inner = z + 1 - 2 * lax.rem(z, 2)
    across = me + 4 * (3 - 2 * z)
    beside = me + 2 - 4 * y
    peers = [me, beside, me + 4 * (inner - z), beside + 4 * (inner - z)]
    places = [(z, y), (z, 1 - y), (inner, y), (inner, 1 - y)]
    count, depth = h_ref.shape
    kv_cols = 2 * KV_COLS_DEV
    rows = count // GRID_PIECES
    everyone = range(GRID_PIECES)
    last = GRID_PIECES - 1

    barrier = pltpu.get_barrier_semaphore()

    for peer in [mate] + peers[1:]:
        pl.semaphore_signal(barrier, inc=1, device_id={"tp": peer})
    pl.semaphore_signal(barrier, inc=1, device_id={"grp": 1 - side, "tp": me})

    @pl.when(is_mid)
    def _():
        pl.semaphore_signal(barrier, inc=1, device_id={"tp": across})

    loads = [pltpu.make_async_copy(gain_hbm, gain_ref, in_sem.at[0])]
    for r in range(count // 128):
        block = pl.ds(r * 128, 128)
        loads.append(pltpu.make_async_copy(h_hbm.at[block], h_ref.at[block], in_sem.at[r + 1]))
    loads.append(pltpu.make_async_copy(scale_hbm, scale_ref, in_sem.at[count // 128 + 1]))
    loads.append(pltpu.make_async_copy(freq_hbm, freq_ref, in_sem.at[count // 128 + 2]))
    for load in loads:
        load.start()

    def weights(s, k, half, kv):
        zt, yt = places[s]
        block = 2 * (2 * (zt + k * (3 - 2 * zt)) + yt) + half
        if not kv:
            first = pl.ds(0, depth - LATE if s == 2 and k else depth)
            return wq_hbm.at[block, first], wq.at[k, half, first, pl.ds(s * HD, HD)]
        cols = pl.ds(pl.multiple_of(block * depth, 128), depth)
        return wkv_hbm.at[:, cols], wkv.at[k, half, pl.ds(s * kv_cols, kv_cols)]

    def weights_own(k, half, kv):
        source, target = weights(0, k, half, kv)
        return pltpu.make_async_copy(source, target, own_sem.at[k, kv])

    def weights_beside(k, half, kv):
        source, target = weights(1, k, half, kv)
        return pltpu.make_async_remote_copy(
            source, target, w_send.at[kv], wy_recv.at[k, kv], device_id={"tp": beside}
        )

    def weights_far(s, k, kv):
        source, target = weights(s, k, side, kv)
        return pltpu.make_async_remote_copy(
            source, target, w_send.at[4 if kv else 2 + k], w_recv.at[s - 2, k, kv], device_id={"tp": peers[s]}
        )

    def weights_twin(s, k, kv):
        piece = weights(s, k, side, kv)[1]
        return pltpu.make_async_remote_copy(
            piece, piece, w_send.at[7 if kv else 5 + k], wx_recv.at[k, kv], device_id={"grp": 1 - side, "tp": me}
        )

    def weights_late(half):
        block = 2 * (2 * (inner + 3 - 2 * inner) + y) + half
        return pltpu.make_async_remote_copy(
            wq_hbm.at[block, pl.ds(depth - LATE, LATE)], wq_late.at[half], late_send, late_recv,
            device_id={"tp": peers[2]},
        )

    def every(ref, send_sem, recv_sem):
        return pltpu.make_async_remote_copy(ref, ref, send_sem, recv_sem, device_id={"tp": mate})

    def shared_q(k):
        return wq.at[k, :, pl.ds(0, depth - k * LATE // 2), pl.ds(0, HD)]

    def weights_arrive(k):
        for kv in (1, 0):
            whole = wkv.at[k, :, pl.ds(0, kv_cols)] if kv else wq.at[k, :, :, pl.ds(0, HD)]
            for sem in (own_sem, wy_recv):
                every(whole, sem.at[k, kv], sem.at[k, kv]).wait_recv()
            every(whole if kv else shared_q(k), wx_recv.at[k, kv], wx_recv.at[k, kv]).wait_recv()

    for k in range(2):
        for half in range(2):
            for kv in range(2):
                weights_own(k, half, kv).start()

    wq[1, :, depth - LATE :, 2 * HD : 3 * HD] = jnp.zeros((2, LATE, HD), jnp.bfloat16)
    loads[0].wait()
    gain = gain_ref[...]
    for r in range(count // 128):
        block = pl.ds(r * 128, 128)
        loads[r + 1].wait()
        wide = h_ref[block, :].astype(jnp.float32)
        weighted = wide * gain
        gath[core, block, :] = weighted.astype(jnp.bfloat16)
        square = jnp.sum(wide * wide, axis=1, keepdims=True)
        top = jnp.max(jnp.abs(weighted), axis=1, keepdims=True)
        stat_own[pl.ds(r, 1), :] = jnp.transpose(jnp.broadcast_to(square, (128, 128)))[0:1, :]
        stat_own[pl.ds(4 + r, 1), :] = jnp.transpose(jnp.broadcast_to(top, (128, 128)))[0:1, :]
    loads[-2].wait()
    loads[-1].wait()

    @pl.when(is_mid)
    def _():
        pl.semaphore_wait(barrier, 6)

    @pl.when(is_end)
    def _():
        pl.semaphore_wait(barrier, 5)

    def stat_pair():
        return pltpu.make_async_remote_copy(
            stat_own, stat_mate, st_send.at[0], st_recv.at[0], device_id={"tp": mate}
        )

    def stat_copy(d):
        return pltpu.make_async_remote_copy(
            stats.at[chip], stats.at[chip], st_send.at[1], st_recv.at[1],
            device_id={"tp": lax.rem(me + 2 * d, n)},
        )

    def stat_all():
        others = stats.at[pl.ds(1, n // 2 - 1)]
        return pltpu.make_async_remote_copy(
            others, others, st_send.at[1], st_recv.at[1], device_id={"tp": mate}
        )

    def act_mate():
        return pltpu.make_async_remote_copy(
            gath.at[core], gath.at[core], mate_send, mate_recv.at[GRID_PIECES],
            device_id={"tp": mate},
        )

    def act_across(p):
        block = pl.ds(p * rows, rows)
        return pltpu.make_async_remote_copy(
            gath.at[core, block], gath.at[2 + core, block], act_send, act_recv.at[p],
            device_id={"tp": across},
        )

    def act_pass(p):
        block = pl.ds(p * rows, rows)
        piece = gath.at[2 + core, block]
        return pltpu.make_async_remote_copy(
            piece, piece, mate_send, mate_recv.at[p], device_id={"tp": mate}
        )

    forwarded = [(s, k, kv) for k in (0, 1) for kv in (1, 0) for s in (2, 3)]
    def weights_beside_all(k, kv):
        for half in range(2):
            weights_beside(k, half, kv).start()

    stat_pair().start()
    for each in forwarded[:4]:
        weights_far(*each).start()
    weights_beside_all(0, 1)

    @pl.when(is_mid)
    def _():
        for p in everyone:
            act_across(p).start()
        pl.semaphore_signal(met.at[1], inc=1, device_id={"tp": across})

    pl.semaphore_signal(met.at[0], inc=1, device_id={"tp": mate})
    pl.semaphore_wait(met.at[0], 1)

    @pl.when(is_mid)
    def _():
        pl.semaphore_wait(met.at[1], 1)

    pl.semaphore_signal(met.at[2], inc=1, device_id={"tp": mate})
    pl.semaphore_wait(met.at[2], 1)

    @pl.when(is_mid)
    def _():
        pl.semaphore_signal(met.at[3], inc=1, device_id={"tp": peers[2]})

    @pl.when(is_end)
    def _():
        pl.semaphore_wait(met.at[3], 1)

    stat_pair().wait()
    mine, other = stat_own[...], stat_mate[...]
    stats[chip, 0:4] = mine[0:4] + other[0:4]
    stats[chip, 4:8] = jnp.maximum(mine[4:8], other[4:8])
    lax.fori_loop(1, n // 2, lambda d, c: (stat_copy(d).start(), c)[1], 0)
    for each in forwarded[4:]:
        weights_far(*each).start()

    act_mate().start()
    weights_beside_all(0, 0)
    weights_beside_all(1, 1)
    weights_beside_all(1, 0)

    even = lax.rem(lax.broadcasted_iota(jnp.int32, (128, HD), 1), 2) == 0
    token = lax.broadcasted_iota(jnp.int32, (128, HD), 0) + prefix_ref[0]
    freq = freq_ref[...]
    for r in range(count // 128):
        angle = (token + r * 128).astype(jnp.float32) * freq
        cosine[pl.ds(r * 128, 128), :] = jnp.cos(angle)
        turn = jnp.sin(angle)
        sine[pl.ds(r * 128, 128), :] = jnp.where(even, -turn, turn)

    for each in forwarded:
        weights_far(*each).wait_recv()
        weights_twin(*each).start()

    @pl.when(is_end)
    def _():
        for p in everyone:
            act_across(p).start()


    stat_all().wait()
    everything = stats[...]
    inverse = 1.0 / jnp.sqrt(jnp.sum(everything[:, 0:4, :], axis=0) / width + norm_eps)
    row_scale = jnp.max(everything[:, 4:8, :], axis=0) * inverse + tiny_eps
    rs_out[...] = row_scale
    inv_row[...] = inverse
    for r in range(count // 128):
        block = pl.ds(r * 128, 128)
        inv = spread(inverse[r : r + 1, :])
        inv_col[block, :] = inv
        scale = spread(row_scale[r : r + 1, :])
        for j in range(depth // 128):
            lanes = pl.ds(j * 128, 128)
            weighted = h_ref[block, lanes].astype(jnp.float32) * gain_ref[:, lanes]
            payload_out[block, lanes] = (weighted * inv / scale).astype(jnp.bfloat16)

    @pl.when(is_mid)
    def _():
        for p in everyone:
            act_across(p).wait_recv()
            act_pass(p).start()

    act_mate().wait_recv()
    weights_arrive(0)

    def product(slot, block, k, half):
        return jnp.dot(gath[slot, block, :], wq[k, half], preferred_element_type=jnp.float32)

    def kv_product(slot, block, k, half):
        return lax.dot_general(
            wkv[k, half], gath[slot, block, :], (((1,), (1,)), ((), ())), preferred_element_type=jnp.float32
        )

    for p in everyone:
        block = pl.ds(p * rows, rows)
        kvacc[p] = kv_product(0, block, 0, 0) + kv_product(1, block, 0, 1)
        acc[block, :] = product(0, block, 0, 0) + product(1, block, 0, 1)

    weights_arrive(1)

    def q_beside(p):
        block = pl.ds(p * rows, rows)
        return pltpu.make_async_remote_copy(
            q_give.at[pl.ds(0, 2), block], q_got.at[pl.ds(0, 2), block], pq_send.at[0], pq_recv.at[0, p],
            device_id={"tp": beside},
        )

    def q_along(p):
        block = pl.ds(p * rows, rows)
        return pltpu.make_async_remote_copy(
            q_give.at[2, block], q_got.at[2, block], pq_send.at[1], pq_recv.at[1, p],
            device_id={"tp": peers[2]},
        )

    def kv_partial(s, p):
        return pltpu.make_async_remote_copy(
            kv_give.at[s - 1, p], kv_got.at[s - 1, p], pkv_send, pkv_recv.at[p],
            device_id={"tp": peers[s]},
        )

    def near(p):
        block = pl.ds(p * rows, rows)
        kvacc[p] += kv_product(2 + core, block, 1, core)
        acc[block, :] += product(2 + core, block, 1, core)

    def far(p):
        block = pl.ds(p * rows, rows)
        act_pass(p).wait_recv()
        pair = kvacc[p] + kv_product(3 - core, block, 1, 1 - core)
        kvacc[p] = pair
        for s in range(1, 4):
            kv_give[s - 1, p] = pair[s * kv_cols : (s + 1) * kv_cols, :].astype(jnp.bfloat16)
        for s in range(1, 4):
            kv_partial(s, p).start()
        whole = acc[block, :] + product(3 - core, block, 1, 1 - core)
        acc[block, :] = whole
        q_give[0, block, :] = whole[:, HD : 2 * HD].astype(jnp.bfloat16)
        q_give[1, block, :] = whole[:, 3 * HD :].astype(jnp.bfloat16)
        q_beside(p).start()

    def late_arrive():
        every(wq_late, late_recv, late_recv).wait_recv()

    def q_combine(p):
        block = pl.ds(p * rows, rows)
        x = acc[block, 2 * HD : 3 * HD]
        for half in range(2):
            x = x + jnp.dot(
                gath[2 + half, block, depth - LATE :], wq_late[half], preferred_element_type=jnp.float32
            )
        q_beside(p).wait_recv()
        q_give[2, block, :] = (x + q_got[1, block, :].astype(jnp.float32)).astype(jnp.bfloat16)
        q_along(p).start()

    kv_scale = jnp.concatenate([scale_ref[:, HD:], jnp.zeros((1, 128 - kv_cols), jnp.float32)], axis=1)
    kv_scale = spread(kv_scale)[0:kv_cols, :]
    qscale = scale_ref[:, 0:HD]

    def kv_copy(p, d):
        return pltpu.make_async_remote_copy(
            kv_own.at[p], kv_tail.at[me] if p == last else kv_all.at[core, chip, p], kv_send.at[int(p == last)], kv_recv.at[p],
            device_id={"tp": lax.rem(me + d, n)},
        )

    kv_final = kv_tail.at[pl.ds(1, n - 1)]
    kv_mine = kv_all.at[core, :, pl.ds(0, last)]
    kv_spread_all = pltpu.make_async_remote_copy(
        kv_mine, kv_mine, kv_send.at[2], kv_recv.at[GRID_PIECES], device_id={"tp": mate}
    )

    def kv_reduce(p):
        total = kvacc[p, 0:kv_cols, :]
        every(kv_got.at[:, p], pkv_send, pkv_recv.at[p]).wait_recv()
        for s in range(1, 4):
            total = total + kv_got[s - 1, p].astype(jnp.float32)
        mine = (total * inv_row[p : p + 1, :] * kv_scale).astype(jnp.bfloat16)
        kv_own[p] = mine
        if p == last:
            kv_tail[me] = mine
            lax.fori_loop(1, n, lambda d, c: (kv_copy(p, d).start(), c)[1], 0)
        else:
            kv_all[core, chip, p] = mine
            lax.fori_loop(1, n // 2, lambda d, c: (kv_copy(p, 2 * d).start(), c)[1], 0)

    def rotated(x, block):
        swapped = jnp.where(even, pltpu.roll(x, HD - 1, 1), pltpu.roll(x, 1, 1))
        return (x * cosine[block, :] + swapped * sine[block, :]).astype(jnp.bfloat16)

    def q_reduce(p):
        block = pl.ds(p * rows, rows)
        x = acc[block, 0:HD]
        q_along(p).wait_recv()
        x = x + q_got[0, block, :].astype(jnp.float32) + q_got[2, block, :].astype(jnp.float32)
        q_out[block, :] = rotated(x * inv_col[block, :] * qscale, block)

    def heads(p):
        block = pl.ds(p * rows, rows)
        if p == last:
            every(kv_final, kv_send.at[1], kv_recv.at[p]).wait_recv()
        elif p == 0:
            kv_spread_all.wait_recv()
        if p == last:
            pair = kv_tail[...].astype(jnp.float32)
        else:
            both = kv_all[:, :, p].astype(jnp.float32)
            pair = jnp.stack([both[0], both[1]], axis=1).reshape(n, kv_cols, 128)
        keys = jnp.transpose(pair[:, 0:KV_COLS_DEV, :].reshape(HD, 128))
        k_out[block, :] = rotated(keys, block)
        values = jnp.transpose(pair[:, KV_COLS_DEV:, :].reshape(HD, 128))
        v_out[block, :] = values.astype(jnp.bfloat16)

    @pl.when(is_mid)
    def _():
        for p in everyone:
            near(p)
        for p in everyone:
            far(p)
        for half in range(2):
            weights_late(half).start()
        for p in range(last):
            kv_reduce(p)
        late_arrive()
        for p in everyone:
            q_combine(p)
        kv_reduce(last)

    @pl.when(is_end)
    def _():
        for p in everyone:
            act_across(p).wait_recv()
            act_pass(p).start()
            near(p)
            far(p)
            if p == last - 1:
                for half in range(2):
                    weights_late(half).start()
        for p in everyone:
            kv_reduce(p)
        late_arrive()
        for p in everyone:
            q_combine(p)

    for p in range(last):
        every(kv_all.at[0, pl.ds(1, n // 2 - 1), p], kv_recv.at[p], kv_recv.at[p]).wait_recv()
    kv_spread_all.start()
    for p in range(last):
        q_reduce(p)
    every(gath.at[0], act_send, act_send).wait_send()
    every(gath.at[pl.ds(0, 2)], mate_send, mate_send).wait_send()
    for i in (1, 4, 7):
        every(wkv.at[:, :, pl.ds(0, kv_cols)], w_send.at[i], w_send.at[i]).wait_send()
    every(wq.at[:, :, :, pl.ds(0, HD)], w_send.at[0], w_send.at[0]).wait_send()
    for i in (2, 5):
        for k in range(2):
            every(shared_q(k), w_send.at[i + k], w_send.at[i + k]).wait_send()
    every(wq_late, late_send, late_send).wait_send()
    for p in range(last):
        heads(p)
    q_reduce(last)
    every(kv_give, pkv_send, pkv_send).wait_send()
    every(q_give.at[pl.ds(0, 2)], pq_send.at[0], pq_send.at[0]).wait_send()
    every(q_give.at[2], pq_send.at[1], pq_send.at[1]).wait_send()
    every(kv_all.at[0, pl.ds(1, n // 2 - 1)], kv_send.at[0], kv_send.at[0]).wait_send()
    every(kv_final, kv_send.at[1], kv_send.at[1]).wait_send()
    kv_spread_all.wait_send()
    heads(last)


def grid_scratch(count, depth):
    dma = pltpu.SemaphoreType.DMA
    bf16, f32 = jnp.bfloat16, jnp.float32
    pieces, kv_cols = GRID_PIECES, 2 * KV_COLS_DEV
    rows = count // pieces
    return [
        pltpu.VMEM((4, count, depth), bf16),
        pltpu.VMEM((2, 2, depth, 4 * HD), bf16),
        pltpu.VMEM((2, 2, 4 * kv_cols, depth), bf16),
        pltpu.VMEM((2, LATE, HD), bf16),
        pltpu.VMEM((count, 4 * HD), f32),
        pltpu.VMEM((pieces, 4 * kv_cols, rows), f32),
        pltpu.VMEM((3, count, HD), bf16),
        pltpu.VMEM((3, count, HD), bf16),
        pltpu.VMEM((3, pieces, kv_cols, rows), bf16),
        pltpu.VMEM((3, pieces, kv_cols, rows), bf16),
        pltpu.VMEM((8, 128), f32),
        pltpu.VMEM((8, 128), f32),
        pltpu.VMEM((8, 8, 128), f32),
        pltpu.VMEM((pieces, kv_cols, rows), bf16),
        pltpu.VMEM((2, 8, pieces - 1, kv_cols, rows), bf16),
        pltpu.VMEM((16, kv_cols, rows), bf16),
        pltpu.VMEM((count // 128, 128), f32),
        pltpu.VMEM((count, HD), f32),
        pltpu.VMEM((count, HD), f32),
        pltpu.VMEM((count, HD), f32),
        pltpu.VMEM((count, depth), bf16),
        pltpu.VMEM((1, depth), f32),
        pltpu.VMEM((1, HD + kv_cols), f32),
        pltpu.VMEM((1, HD), f32),
        dma((count // 128 + 3,)),
        dma((2, 2)),
        dma,
        dma,
        pltpu.SemaphoreType.REGULAR((4,)),
        dma((2,)),
        dma((2,)),
        dma((8,)),
        dma((2, 2, 2)),
        dma((2, 2)),
        dma((2, 2)),
        dma,
        dma((pieces,)),
        dma,
        dma((pieces + 1,)),
        dma((2,)),
        dma((2, pieces)),
        dma,
        dma((pieces,)),
        dma((3,)),
        dma((pieces + 1,)),
    ]


def finish_kernel(*refs):
    sources, targets, sems = refs[0:5], refs[5:10], refs[10]
    outs = [pltpu.make_async_copy(sources[i], targets[i], sems.at[i]) for i in range(5)]
    for copy in outs:
        copy.start()
    for copy in outs:
        copy.wait()


def finish(*arrays):
    return pl.pallas_call(
        finish_kernel,
        out_shape=tuple(jax.ShapeDtypeStruct(a.shape, a.dtype) for a in arrays),
        in_specs=[pl.BlockSpec(memory_space=pltpu.VMEM)] * 5,
        out_specs=(pl.BlockSpec(memory_space=pltpu.HBM),) * 5,
        scratch_shapes=[pltpu.SemaphoreType.DMA((5,))], compiler_params=pltpu.CompilerParams(vmem_limit_bytes=2 * 1024 * 1024),
    )(*arrays)


def local(n, groups, hidden, norm_gain, prefix, w_query, w_kv, w_scale):
    count, depth = hidden.shape
    chips = n // 2
    width = depth * n
    grid = n == 16 and groups == 2 and n * KV_COLS_DEV == HD and count == 128 * GRID_PIECES
    pair_index = np.arange(HD) // 2
    freq = jnp.asarray(np.power(rope_base, -(2.0 * pair_index) / HD)[None, :], jnp.float32)
    pieces = HD // KV_COLS_DEV
    vmem = pl.BlockSpec(memory_space=pltpu.VMEM)
    hbm = pl.BlockSpec(memory_space=pltpu.HBM if grid else pl.ANY)
    dma = pltpu.SemaphoreType.DMA
    bf16, f32 = jnp.bfloat16, jnp.float32
    queries, keys, values, payload, row_scale = pl.pallas_call(
        functools.partial(grid_kernel, width) if grid else functools.partial(kernel, n, width),
        out_shape=(
            pltpu.VMEM((count, HD), bf16),
            pltpu.VMEM((count, HD), bf16),
            pltpu.VMEM((count, HD), bf16),
            pltpu.VMEM((count, depth), bf16),
            pltpu.VMEM((count // 128, 128), f32),
        ),
        in_specs=[pl.BlockSpec(memory_space=pltpu.SMEM)]
        + ([hbm] * 6 if grid else [vmem] * 5 + [hbm] * 2),
        out_specs=(vmem,) * 5,
        scratch_shapes=grid_scratch(count, depth) if grid else [
            pltpu.VMEM((chips, count, depth), bf16),
            pltpu.VMEM((chips, depth, 2 * HD), bf16),
            pltpu.VMEM((chips, 32, depth), bf16),
            pltpu.VMEM((count, 2 * HD), f32),
            pltpu.VMEM((count, 32), f32),
            pltpu.VMEM((count, HD), f32),
            pltpu.VMEM((count, 32), f32),
            pltpu.VMEM((8, 128), f32),
            pltpu.VMEM((n, 8, 128), f32),
            pltpu.VMEM((2 * KV_COLS_DEV, count), bf16),
            pltpu.VMEM((pieces, 2 * KV_COLS_DEV, count), bf16),
            pltpu.VMEM((count, HD), f32),
            pltpu.VMEM((count, HD), f32),
            pltpu.VMEM((count, HD), f32),
            dma((chips, 2, PIECES)),
            dma((chips, 2, PIECES)),
            dma((n,)),
            dma((n,)),
            dma((pieces,)),
            dma((pieces,)),
            dma,
            dma((chips,)),
            dma,
            dma,
            dma((chips,)),
            dma((chips,)),
            dma((2,)),
            dma((2,)),
        ],
        compiler_params=pltpu.CompilerParams(
            collective_id=0, has_side_effects=True, vmem_limit_bytes=(60 if grid else 48) * 1024 * 1024
        ),
    )(
        prefix,
        hidden,
        norm_gain[None, :],
        freq,
        *([w_scale[None, :]] if grid else [w_scale[None, :HD], w_scale[None, HD:]]),
        w_query.reshape(n, depth, HD) if grid else w_query.reshape(chips, 2, depth, HD),
        w_kv,
    )
    queries, keys, values, payload, row_scale = finish(queries, keys, values, payload, row_scale)
    return queries, keys, values, payload, row_scale.reshape(count)


def solution(mesh):
    return jax.shard_map(
        functools.partial(local, mesh.shape["tp"], mesh.shape["grp"]),
        mesh=mesh,
        in_specs=(P("grp", "tp"), P("tp"), P("grp"), P(None, "tp"), P("tp", None), P("tp")),
        out_specs=(P("grp", "tp"), P("grp", "tp"), P("grp", "tp"), P("grp", "tp"), P("grp")),
        check_vma=False,
    )
```

```python
import functools

import jax
import jax.numpy as jnp
import numpy as np
from jax import lax
from jax.experimental import pallas as pl
from jax.experimental.pallas import tpu as pltpu
from jax.sharding import PartitionSpec as P

HD = 128
KV_COLS_DEV = 8
norm_eps = 1e-05
tiny_eps = 1e-06
rope_base = 500000.0
PIECES = 2
GRID_PIECES = 4
LATE = 256


def ring_order(chips):
    cols = 1
    while (2 * cols) * (2 * cols) <= chips and chips % (2 * cols) == 0:
        cols *= 2
    rows = chips // cols
    if cols < 2 or rows % 2:
        return list(range(chips))
    order = [0]
    for row in range(rows):
        span = range(1, cols) if row % 2 == 0 else range(cols - 1, 0, -1)
        order += [row * cols + col for col in span]
    order += [row * cols for row in range(rows - 1, 0, -1)]
    return order


def lookup(table, index):
    total = jnp.int32(0)
    for key, value in enumerate(table):
        total = total + jnp.where(index == key, jnp.int32(value), jnp.int32(0))
    return total


def spread(row):
    return jnp.transpose(jnp.broadcast_to(row, (128, 128)))


def kernel(
    n, width, prefix_ref, h_ref, gain_ref, freq_ref, qscale_ref, kvscale_ref, wq_hbm, wkv_hbm,
    q_out, k_out, v_out, payload_out, rs_out,
    gath, wq, wkv, acc, kvacc, part_q, part_kv, stat_own, stats, kv_own, kv_all, inv_col, cosine, sine,
    send_sem, recv_sem, st_send, st_recv, kv_send, kv_recv,
    wl_sem, wkl_sem, wr_send, wr_recv, wkr_send, wkr_recv, ex_send, ex_recv,
):
    me = lax.axis_index("tp")
    chips = n // 2
    core = lax.rem(me, 2)
    chip = me // 2
    mate = me + 1 - 2 * core
    count, depth = h_ref.shape
    half = count // 2
    rows = half // PIECES
    pieces = HD // KV_COLS_DEV
    kv_heads = n // pieces
    order = ring_order(chips)
    place = [order.index(c) for c in range(chips)]
    pos = lookup(place, chip)
    succ = 2 * lookup(order, lax.rem(pos + 1, chips)) + core
    pred = 2 * lookup(order, lax.rem(pos + chips - 1, chips)) + core

    barrier = pltpu.get_barrier_semaphore()

    def greet(d, carry):
        pl.semaphore_signal(barrier, inc=1, device_id={"tp": lax.rem(me + d, n)})
        return carry

    lax.fori_loop(1, n, greet, 0)

    own_wq = pltpu.make_async_copy(wq_hbm.at[:, core], wq.at[:, :, pl.ds(0, HD)], wl_sem)
    own_wq.start()

    def kv_local(k):
        cols = pl.ds(pl.multiple_of((2 * k + core) * depth, 128), depth)
        return pltpu.make_async_copy(wkv_hbm.at[:, cols], wkv.at[k, pl.ds(0, 16)], wkl_sem.at[k])

    def kv_remote(k):
        cols = pl.ds(pl.multiple_of((2 * k + 1 - core) * depth, 128), depth)
        return pltpu.make_async_remote_copy(
            wkv_hbm.at[:, cols], wkv.at[k, pl.ds(16, 16)], wkr_send.at[k], wkr_recv.at[k],
            device_id={"tp": mate},
        )

    mate_wq = pltpu.make_async_remote_copy(
        wq_hbm.at[:, 1 - core], wq.at[:, :, pl.ds(HD, HD)], wr_send, wr_recv, device_id={"tp": mate}
    )
    lax.fori_loop(0, chips, lambda k, c: (kv_local(k).start(), c)[1], 0)

    gain = gain_ref[...]
    for r in range(count // 128):
        block = pl.ds(r * 128, 128)
        wide = h_ref[block, :].astype(jnp.float32)
        weighted = wide * gain
        gath[0, block, :] = weighted.astype(jnp.bfloat16)
        square = jnp.sum(wide * wide, axis=1, keepdims=True)
        top = jnp.max(jnp.abs(weighted), axis=1, keepdims=True)
        stat_own[pl.ds(r, 1), :] = jnp.transpose(jnp.broadcast_to(square, (128, 128)))[0:1, :]
        stat_own[pl.ds(4 + r, 1), :] = jnp.transpose(jnp.broadcast_to(top, (128, 128)))[0:1, :]
    stats[me] = stat_own[...]

    pl.semaphore_wait(barrier, n - 1)

    def hop(step, way, piece):
        block = pl.ds(way * half + piece * rows, rows)
        return pltpu.make_async_remote_copy(
            gath.at[step, block], gath.at[step + 1, block],
            send_sem.at[step, way, piece], recv_sem.at[step, way, piece],
            device_id={"tp": succ if way == 0 else pred},
        )

    def multiply(step, way, piece):
        block = pl.ds(way * half + piece * rows, rows)
        shift = chips - step if way == 0 else step
        owner = lookup(order, lax.rem(pos + shift, chips))
        left = gath[step, block, :]
        acc[block, :] += jnp.dot(left, wq[owner], preferred_element_type=jnp.float32)
        kvacc[block, :] += lax.dot_general(
            left, wkv[owner], (((1,), (1,)), ((), ())), preferred_element_type=jnp.float32
        )

    for piece in range(PIECES):
        for way in range(2):
            hop(0, way, piece).start()
    mate_wq.start()
    lax.fori_loop(0, chips, lambda k, c: (kv_remote(k).start(), c)[1], 0)

    def stat_copy(d):
        return pltpu.make_async_remote_copy(
            stat_own, stats.at[me], st_send.at[d], st_recv.at[d], device_id={"tp": lax.rem(me + d, n)}
        )

    lax.fori_loop(1, n, lambda d, c: (stat_copy(d).start(), c)[1], 0)

    acc[...] = jnp.zeros_like(acc)
    kvacc[...] = jnp.zeros_like(kvacc)
    token = lax.broadcasted_iota(jnp.int32, (128, HD), 0) + prefix_ref[0]
    freq = freq_ref[...]
    even = lax.rem(lax.broadcasted_iota(jnp.int32, (128, HD), 1), 2) == 0
    for r in range(count // 128):
        angle = (token + r * 128).astype(jnp.float32) * freq
        cosine[pl.ds(r * 128, 128), :] = jnp.cos(angle)
        turn = jnp.sin(angle)
        sine[pl.ds(r * 128, 128), :] = jnp.where(even, -turn, turn)

    lax.fori_loop(1, n, lambda d, c: (stat_copy(d).wait(), c)[1], 0)
    everything = stats[...]
    inverse = 1.0 / jnp.sqrt(jnp.sum(everything[:, 0:4, :], axis=0) / width + norm_eps)
    row_scale = jnp.max(everything[:, 4:8, :], axis=0) * inverse + tiny_eps
    rs_out[...] = row_scale
    for r in range(count // 128):
        block = pl.ds(r * 128, 128)
        inv = spread(inverse[r : r + 1, :])
        inv_col[block, :] = inv
        scale = spread(row_scale[r : r + 1, :])
        for j in range(depth // 128):
            lanes = pl.ds(j * 128, 128)
            weighted = h_ref[block, lanes].astype(jnp.float32) * gain[:, j * 128 : j * 128 + 128]
            payload_out[block, lanes] = (weighted * inv / scale).astype(jnp.bfloat16)

    own_wq.wait()
    lax.fori_loop(0, chips, lambda k, c: (kv_local(k).wait(), c)[1], 0)
    mate_wq.wait()
    lax.fori_loop(0, chips, lambda k, c: (kv_remote(k).wait(), c)[1], 0)

    for piece in range(PIECES):
        for way in range(2):
            multiply(0, way, piece)

    def ring_step(step, carry):
        for piece in range(PIECES):
            for way in range(2):
                hop(step - 1, way, piece).wait_recv()
                hop(step, way, piece).start()
                multiply(step, way, piece)
        return carry

    lax.fori_loop(1, chips - 1, ring_step, 0)
    for piece in range(PIECES):
        for way in range(2):
            hop(chips - 2, way, piece).wait_recv()
            multiply(chips - 1, way, piece)

    ex_kv = pltpu.make_async_remote_copy(
        kvacc, part_kv, ex_send.at[0], ex_recv.at[0], device_id={"tp": mate}
    )
    ex_q = pltpu.make_async_remote_copy(
        acc.at[:, pl.ds(HD, HD)], part_q, ex_send.at[1], ex_recv.at[1], device_id={"tp": mate}
    )
    ex_kv.start()
    ex_q.start()

    def drain(step, carry):
        for piece in range(PIECES):
            for way in range(2):
                hop(step, way, piece).wait_send()
        return carry

    lax.fori_loop(0, chips - 1, drain, 0)
    ex_kv.wait()
    kvscale = kvscale_ref[...]
    for r in range(count // 128):
        block = pl.ds(r * 128, 128)
        cols = (kvacc[block, 0:16] + part_kv[block, 16:32]) * inv_col[block, 0:16] * kvscale
        cols = jnp.concatenate([cols, jnp.zeros((128, 112), jnp.float32)], axis=1)
        kv_own[:, block] = jnp.transpose(cols)[0:16, :].astype(jnp.bfloat16)

    my_head = me * kv_heads // n
    group = lax.rem(me, kv_heads)
    slot = me // kv_heads

    def kv_copy(i):
        return pltpu.make_async_remote_copy(
            kv_own, kv_all.at[slot], kv_send.at[i], kv_recv.at[slot],
            device_id={"tp": group * pieces + i},
        )

    def kv_arrival(i):
        return pltpu.make_async_remote_copy(
            kv_own, kv_all.at[i], kv_send.at[i], kv_recv.at[i], device_id={"tp": mate}
        )

    def kv_start(i, carry):
        @pl.when(group * pieces + i != me)
        def _():
            kv_copy(i).start()

        return carry

    def kv_wait(i, carry):
        @pl.when(group * pieces + i != me)
        def _():
            kv_copy(i).wait_send()

        @pl.when(i * kv_heads + my_head != me)
        def _():
            kv_arrival(i).wait_recv()

        return carry

    @pl.when(my_head == group)
    def _():
        kv_all[slot] = kv_own[...]

    lax.fori_loop(0, pieces, kv_start, 0)

    def rotated(x, block):
        swapped = jnp.where(even, pltpu.roll(x, HD - 1, 1), pltpu.roll(x, 1, 1))
        return (x * cosine[block, :] + swapped * sine[block, :]).astype(jnp.bfloat16)

    ex_q.wait()
    qscale = qscale_ref[...]
    for r in range(count // 128):
        block = pl.ds(r * 128, 128)
        x = (acc[block, 0:HD] + part_q[block, :]) * inv_col[block, :] * qscale
        q_out[block, :] = rotated(x, block)

    lax.fori_loop(0, pieces, kv_wait, 0)
    for r in range(count // 128):
        block = pl.ds(r * 128, 128)
        both = kv_all[:, :, block].astype(jnp.float32)
        keys = jnp.transpose(both[:, 0:KV_COLS_DEV, :].reshape(HD, 128))
        k_out[block, :] = rotated(keys, block)
        values = jnp.transpose(both[:, KV_COLS_DEV:, :].reshape(HD, 128))
        v_out[block, :] = values.astype(jnp.bfloat16)


def grid_kernel(
    width, prefix_ref, h_hbm, gain_hbm, freq_hbm, scale_hbm, wq_hbm, wkv_hbm,
    q_out, k_out, v_out, payload_out, rs_out,
    gath, wq, wkv, wq_late, acc, kvacc, q_give, q_got, kv_give, kv_got,
    stat_own, stat_mate, stats, kv_own, kv_all, kv_tail, inv_row, inv_col, cosine, sine,
    h_ref, gain_ref, scale_ref, freq_ref, in_sem, own_sem, late_send, late_recv, met,
    st_send, st_recv, w_send, w_recv, wx_recv, wy_recv, act_send, act_recv, mate_send, mate_recv,
    pq_send, pq_recv, pkv_send, pkv_recv, kv_send, kv_recv,
):
    n = 16
    me = lax.axis_index("tp")
    side = lax.axis_index("grp")
    core = lax.rem(me, 2)
    chip = me // 2
    y = lax.rem(chip, 2)
    z = chip // 2
    mate = me + 1 - 2 * core
    is_end = (z == 0) | (z == 3)
    is_mid = (z == 1) | (z == 2)
    inner = z + 1 - 2 * lax.rem(z, 2)
    across = me + 4 * (3 - 2 * z)
    beside = me + 2 - 4 * y
    peers = [me, beside, me + 4 * (inner - z), beside + 4 * (inner - z)]
    places = [(z, y), (z, 1 - y), (inner, y), (inner, 1 - y)]
    count, depth = h_ref.shape
    kv_cols = 2 * KV_COLS_DEV
    rows = count // GRID_PIECES
    everyone = range(GRID_PIECES)
    last = GRID_PIECES - 1

    barrier = pltpu.get_barrier_semaphore()

    for peer in [mate] + peers[1:3]:
        pl.semaphore_signal(barrier, inc=1, device_id={"tp": peer})
    pl.semaphore_signal(barrier, inc=1, device_id={"grp": 1 - side, "tp": me})

    @pl.when(is_mid)
    def _():
        pl.semaphore_signal(barrier, inc=1, device_id={"tp": across})

    loads = [pltpu.make_async_copy(gain_hbm, gain_ref, in_sem.at[0])]
    for r in range(count // 128):
        block = pl.ds(r * 128, 128)
        loads.append(pltpu.make_async_copy(h_hbm.at[block], h_ref.at[block], in_sem.at[r + 1]))
    loads.append(pltpu.make_async_copy(scale_hbm, scale_ref, in_sem.at[count // 128 + 1]))
    loads.append(pltpu.make_async_copy(freq_hbm, freq_ref, in_sem.at[count // 128 + 2]))
    for load in loads:
        load.start()

    def weights(s, k, half, kv):
        zt, yt = places[s]
        block = 2 * (2 * (zt + k * (3 - 2 * zt)) + yt) + half
        if not kv:
            first = pl.ds(0, depth - LATE if s == 2 and k else depth)
            return wq_hbm.at[block, first], wq.at[k, half, first, pl.ds(s * HD, HD)]
        cols = pl.ds(pl.multiple_of(block * depth, 128), depth)
        return wkv_hbm.at[:, cols], wkv.at[k, half, pl.ds(s * kv_cols, kv_cols)]

    def weights_own(k, half, kv):
        source, target = weights(0, k, half, kv)
        return pltpu.make_async_copy(source, target, own_sem.at[k, kv])

    def weights_beside(k, half, kv):
        source, target = weights(1, k, half, kv)
        return pltpu.make_async_remote_copy(
            source, target, w_send.at[kv], wy_recv.at[k, kv], device_id={"tp": beside}
        )

    def weights_far(s, k, kv):
        source, target = weights(s, k, side, kv)
        return pltpu.make_async_remote_copy(
            source, target, w_send.at[4 if kv else 2 + k], w_recv.at[s - 2, k, kv], device_id={"tp": peers[s]}
        )

    def weights_twin(s, k, kv):
        piece = weights(s, k, side, kv)[1]
        return pltpu.make_async_remote_copy(
            piece, piece, w_send.at[7 if kv else 5 + k], wx_recv.at[k, kv], device_id={"grp": 1 - side, "tp": me}
        )

    def weights_late(half):
        block = 2 * (2 * (inner + 3 - 2 * inner) + y) + half
        return pltpu.make_async_remote_copy(
            wq_hbm.at[block, pl.ds(depth - LATE, LATE)], wq_late.at[half], late_send, late_recv,
            device_id={"tp": peers[2]},
        )

    def every(ref, send_sem, recv_sem):
        return pltpu.make_async_remote_copy(ref, ref, send_sem, recv_sem, device_id={"tp": mate})

    def shared_q(k):
        return wq.at[k, :, pl.ds(0, depth - k * LATE // 2), pl.ds(0, HD)]

    def weights_arrive(k):
        for kv in (1, 0):
            whole = wkv.at[k, :, pl.ds(0, kv_cols)] if kv else wq.at[k, :, :, pl.ds(0, HD)]
            for sem in (own_sem, wy_recv):
                every(whole, sem.at[k, kv], sem.at[k, kv]).wait_recv()
            every(whole if kv else shared_q(k), wx_recv.at[k, kv], wx_recv.at[k, kv]).wait_recv()

    for k in range(2):
        for half in range(2):
            for kv in range(2):
                weights_own(k, half, kv).start()

    wq[1, :, depth - LATE :, 2 * HD : 3 * HD] = jnp.zeros((2, LATE, HD), jnp.bfloat16)
    @pl.when(is_mid)
    def _():
        pl.semaphore_wait(barrier, 5)

    @pl.when(is_end)
    def _():
        pl.semaphore_wait(barrier, 4)

    forwarded = [(2, 0, 1), (2, 0, 0), (3, 0, 1), (3, 0, 0), (2, 1, 1), (3, 1, 1), (2, 1, 0), (3, 1, 0)]

    def weights_beside_all(k, kv):
        for half in range(2):
            weights_beside(k, half, kv).start()

    for each in forwarded[:2]:
        weights_far(*each).start()
    weights_beside_all(0, 1)
    pl.semaphore_signal(met.at[0], inc=1, device_id={"tp": mate})
    pl.semaphore_signal(met.at[4], inc=1, device_id={"tp": beside})

    loads[0].wait()
    gain = gain_ref[...]
    for r in range(count // 128):
        block = pl.ds(r * 128, 128)
        loads[r + 1].wait()
        wide = h_ref[block, :].astype(jnp.float32)
        weighted = wide * gain
        gath[core, block, :] = weighted.astype(jnp.bfloat16)
        square = jnp.sum(wide * wide, axis=1, keepdims=True)
        top = jnp.max(jnp.abs(weighted), axis=1, keepdims=True)
        stat_own[pl.ds(r, 1), :] = jnp.transpose(jnp.broadcast_to(square, (128, 128)))[0:1, :]
        stat_own[pl.ds(4 + r, 1), :] = jnp.transpose(jnp.broadcast_to(top, (128, 128)))[0:1, :]
    loads[-2].wait()
    loads[-1].wait()

    def stat_pair():
        return pltpu.make_async_remote_copy(
            stat_own, stat_mate, st_send.at[0], st_recv.at[0], device_id={"tp": mate}
        )

    def stat_copy(d):
        return pltpu.make_async_remote_copy(
            stats.at[chip], stats.at[chip], st_send.at[1], st_recv.at[1],
            device_id={"tp": lax.rem(me + 2 * d, n)},
        )

    def stat_all():
        others = stats.at[pl.ds(1, n // 2 - 1)]
        return pltpu.make_async_remote_copy(
            others, others, st_send.at[1], st_recv.at[1], device_id={"tp": mate}
        )

    def act_mate():
        return pltpu.make_async_remote_copy(
            gath.at[core], gath.at[core], mate_send, mate_recv.at[GRID_PIECES],
            device_id={"tp": mate},
        )

    def act_across(p):
        block = pl.ds(p * rows, rows)
        return pltpu.make_async_remote_copy(
            gath.at[core, block], gath.at[2 + core, block], act_send, act_recv.at[p],
            device_id={"tp": across},
        )

    def act_pass(p):
        block = pl.ds(p * rows, rows)
        piece = gath.at[2 + core, block]
        return pltpu.make_async_remote_copy(
            piece, piece, mate_send, mate_recv.at[p], device_id={"tp": mate}
        )

    stat_pair().start()
    pl.semaphore_wait(met.at[4], 1)
    for each in forwarded[2:4]:
        weights_far(*each).start()

    @pl.when(is_mid)
    def _():
        pl.semaphore_signal(met.at[1], inc=1, device_id={"tp": across})
        for p in everyone:
            act_across(p).start()

    pl.semaphore_wait(met.at[0], 1)

    @pl.when(is_mid)
    def _():
        pl.semaphore_wait(met.at[1], 1)

    pl.semaphore_signal(met.at[2], inc=1, device_id={"tp": mate})
    pl.semaphore_wait(met.at[2], 1)

    @pl.when(is_mid)
    def _():
        pl.semaphore_signal(met.at[3], inc=1, device_id={"tp": peers[2]})

    @pl.when(is_end)
    def _():
        pl.semaphore_wait(met.at[3], 1)

    stat_pair().wait()
    mine, other = stat_own[...], stat_mate[...]
    stats[chip, 0:4] = mine[0:4] + other[0:4]
    stats[chip, 4:8] = jnp.maximum(mine[4:8], other[4:8])
    lax.fori_loop(1, n // 2, lambda d, c: (stat_copy(d).start(), c)[1], 0)
    for each in forwarded[4:]:
        weights_far(*each).start()

    act_mate().start()
    weights_beside_all(0, 0)
    weights_beside_all(1, 1)
    weights_beside_all(1, 0)

    even = lax.rem(lax.broadcasted_iota(jnp.int32, (128, HD), 1), 2) == 0
    token = lax.broadcasted_iota(jnp.int32, (128, HD), 0) + prefix_ref[0]
    freq = freq_ref[...]
    for r in range(count // 128):
        angle = (token + r * 128).astype(jnp.float32) * freq
        cosine[pl.ds(r * 128, 128), :] = jnp.cos(angle)
        turn = jnp.sin(angle)
        sine[pl.ds(r * 128, 128), :] = jnp.where(even, -turn, turn)

    for each in forwarded:
        weights_far(*each).wait_recv()
        weights_twin(*each).start()

    @pl.when(is_end)
    def _():
        for p in everyone:
            act_across(p).start()


    stat_all().wait()
    everything = stats[...]
    inverse = 1.0 / jnp.sqrt(jnp.sum(everything[:, 0:4, :], axis=0) / width + norm_eps)
    row_scale = jnp.max(everything[:, 4:8, :], axis=0) * inverse + tiny_eps
    rs_out[...] = row_scale
    inv_row[...] = inverse
    for r in range(count // 128):
        block = pl.ds(r * 128, 128)
        inv = spread(inverse[r : r + 1, :])
        inv_col[block, :] = inv
        scale = spread(row_scale[r : r + 1, :])
        for j in range(depth // 128):
            lanes = pl.ds(j * 128, 128)
            weighted = h_ref[block, lanes].astype(jnp.float32) * gain_ref[:, lanes]
            payload_out[block, lanes] = (weighted * inv / scale).astype(jnp.bfloat16)

    @pl.when(is_mid)
    def _():
        for p in everyone:
            act_across(p).wait_recv()
            act_pass(p).start()

    act_mate().wait_recv()
    weights_arrive(0)

    def product(slot, block, k, half):
        return jnp.dot(gath[slot, block, :], wq[k, half], preferred_element_type=jnp.float32)

    def kv_product(slot, block, k, half):
        return lax.dot_general(
            wkv[k, half], gath[slot, block, :], (((1,), (1,)), ((), ())), preferred_element_type=jnp.float32
        )

    for p in everyone:
        block = pl.ds(p * rows, rows)
        kvacc[p] = kv_product(0, block, 0, 0) + kv_product(1, block, 0, 1)
        acc[block, :] = product(0, block, 0, 0) + product(1, block, 0, 1)

    weights_arrive(1)

    def q_beside(p):
        block = pl.ds(p * rows, rows)
        return pltpu.make_async_remote_copy(
            q_give.at[pl.ds(0, 2), block], q_got.at[pl.ds(0, 2), block], pq_send.at[0], pq_recv.at[0, p],
            device_id={"tp": beside},
        )

    def q_along(p):
        block = pl.ds(p * rows, rows)
        return pltpu.make_async_remote_copy(
            q_give.at[2, block], q_got.at[2, block], pq_send.at[1], pq_recv.at[1, p],
            device_id={"tp": peers[2]},
        )

    def kv_partial(s, p):
        return pltpu.make_async_remote_copy(
            kv_give.at[s - 1, p], kv_got.at[s - 1, p], pkv_send, pkv_recv.at[p],
            device_id={"tp": peers[s]},
        )

    def near(p):
        block = pl.ds(p * rows, rows)
        kvacc[p] += kv_product(2 + core, block, 1, core)
        acc[block, :] += product(2 + core, block, 1, core)

    def far(p):
        block = pl.ds(p * rows, rows)
        act_pass(p).wait_recv()
        pair = kvacc[p] + kv_product(3 - core, block, 1, 1 - core)
        kvacc[p] = pair
        for s in range(1, 4):
            kv_give[s - 1, p] = pair[s * kv_cols : (s + 1) * kv_cols, :].astype(jnp.bfloat16)
        for s in range(1, 4):
            kv_partial(s, p).start()
        whole = acc[block, :] + product(3 - core, block, 1, 1 - core)
        acc[block, :] = whole
        q_give[0, block, :] = whole[:, HD : 2 * HD].astype(jnp.bfloat16)
        q_give[1, block, :] = whole[:, 3 * HD :].astype(jnp.bfloat16)
        q_beside(p).start()

    def late_arrive():
        every(wq_late, late_recv, late_recv).wait_recv()

    def q_combine(p):
        block = pl.ds(p * rows, rows)
        x = acc[block, 2 * HD : 3 * HD]
        for half in range(2):
            x = x + jnp.dot(
                gath[2 + half, block, depth - LATE :], wq_late[half], preferred_element_type=jnp.float32
            )
        q_beside(p).wait_recv()
        q_give[2, block, :] = (x + q_got[1, block, :].astype(jnp.float32)).astype(jnp.bfloat16)
        q_along(p).start()

    kv_scale = jnp.concatenate([scale_ref[:, HD:], jnp.zeros((1, 128 - kv_cols), jnp.float32)], axis=1)
    kv_scale = spread(kv_scale)[0:kv_cols, :]
    qscale = scale_ref[:, 0:HD]

    def kv_copy(p, d):
        return pltpu.make_async_remote_copy(
            kv_own.at[p], kv_tail.at[me] if p == last else kv_all.at[core, chip, p], kv_send.at[int(p == last)], kv_recv.at[p],
            device_id={"tp": lax.rem(me + d, n)},
        )

    kv_final = kv_tail.at[pl.ds(1, n - 1)]
    kv_mine = kv_all.at[core, :, pl.ds(0, last)]
    kv_spread_all = pltpu.make_async_remote_copy(
        kv_mine, kv_mine, kv_send.at[2], kv_recv.at[GRID_PIECES], device_id={"tp": mate}
    )

    def kv_reduce(p):
        total = kvacc[p, 0:kv_cols, :]
        every(kv_got.at[:, p], pkv_send, pkv_recv.at[p]).wait_recv()
        for s in range(1, 4):
            total = total + kv_got[s - 1, p].astype(jnp.float32)
        mine = (total * inv_row[p : p + 1, :] * kv_scale).astype(jnp.bfloat16)
        kv_own[p] = mine
        if p == last:
            kv_tail[me] = mine
            lax.fori_loop(1, n, lambda d, c: (kv_copy(p, d).start(), c)[1], 0)
        else:
            kv_all[core, chip, p] = mine
            lax.fori_loop(1, n // 2, lambda d, c: (kv_copy(p, 2 * d).start(), c)[1], 0)

    def rotated(x, block):
        swapped = jnp.where(even, pltpu.roll(x, HD - 1, 1), pltpu.roll(x, 1, 1))
        return (x * cosine[block, :] + swapped * sine[block, :]).astype(jnp.bfloat16)

    def q_reduce(p):
        block = pl.ds(p * rows, rows)
        x = acc[block, 0:HD]
        q_along(p).wait_recv()
        x = x + q_got[0, block, :].astype(jnp.float32) + q_got[2, block, :].astype(jnp.float32)
        q_out[block, :] = rotated(x * inv_col[block, :] * qscale, block)

    def heads(p):
        block = pl.ds(p * rows, rows)
        if p == last:
            every(kv_final, kv_send.at[1], kv_recv.at[p]).wait_recv()
        elif p == 0:
            kv_spread_all.wait_recv()
        if p == last:
            pair = kv_tail[...].astype(jnp.float32)
        else:
            both = kv_all[:, :, p].astype(jnp.float32)
            pair = jnp.stack([both[0], both[1]], axis=1).reshape(n, kv_cols, 128)
        keys = jnp.transpose(pair[:, 0:KV_COLS_DEV, :].reshape(HD, 128))
        k_out[block, :] = rotated(keys, block)
        values = jnp.transpose(pair[:, KV_COLS_DEV:, :].reshape(HD, 128))
        v_out[block, :] = values.astype(jnp.bfloat16)

    @pl.when(is_mid)
    def _():
        for p in everyone:
            near(p)
        for p in everyone:
            far(p)
        for half in range(2):
            weights_late(half).start()
        for p in range(last):
            kv_reduce(p)
        late_arrive()
        for p in everyone:
            q_combine(p)
        kv_reduce(last)

    @pl.when(is_end)
    def _():
        for p in everyone:
            act_across(p).wait_recv()
            act_pass(p).start()
            near(p)
            far(p)
            if p == last - 1:
                for half in range(2):
                    weights_late(half).start()
        for p in everyone:
            kv_reduce(p)
        late_arrive()
        for p in everyone:
            q_combine(p)

    for p in range(last):
        every(kv_all.at[0, pl.ds(1, n // 2 - 1), p], kv_recv.at[p], kv_recv.at[p]).wait_recv()
    kv_spread_all.start()
    for p in range(last):
        q_reduce(p)
    every(gath.at[0], act_send, act_send).wait_send()
    every(gath.at[pl.ds(0, 2)], mate_send, mate_send).wait_send()
    for i in (1, 4, 7):
        every(wkv.at[:, :, pl.ds(0, kv_cols)], w_send.at[i], w_send.at[i]).wait_send()
    every(wq.at[:, :, :, pl.ds(0, HD)], w_send.at[0], w_send.at[0]).wait_send()
    for i in (2, 5):
        for k in range(2):
            every(shared_q(k), w_send.at[i + k], w_send.at[i + k]).wait_send()
    every(wq_late, late_send, late_send).wait_send()
    for p in range(last):
        heads(p)
    q_reduce(last)
    every(kv_give, pkv_send, pkv_send).wait_send()
    every(q_give.at[pl.ds(0, 2)], pq_send.at[0], pq_send.at[0]).wait_send()
    every(q_give.at[2], pq_send.at[1], pq_send.at[1]).wait_send()
    every(kv_all.at[0, pl.ds(1, n // 2 - 1)], kv_send.at[0], kv_send.at[0]).wait_send()
    every(kv_final, kv_send.at[1], kv_send.at[1]).wait_send()
    kv_spread_all.wait_send()
    heads(last)


def grid_scratch(count, depth):
    dma = pltpu.SemaphoreType.DMA
    bf16, f32 = jnp.bfloat16, jnp.float32
    pieces, kv_cols = GRID_PIECES, 2 * KV_COLS_DEV
    rows = count // pieces
    return [
        pltpu.VMEM((4, count, depth), bf16),
        pltpu.VMEM((2, 2, depth, 4 * HD), bf16),
        pltpu.VMEM((2, 2, 4 * kv_cols, depth), bf16),
        pltpu.VMEM((2, LATE, HD), bf16),
        pltpu.VMEM((count, 4 * HD), f32),
        pltpu.VMEM((pieces, 4 * kv_cols, rows), f32),
        pltpu.VMEM((3, count, HD), bf16),
        pltpu.VMEM((3, count, HD), bf16),
        pltpu.VMEM((3, pieces, kv_cols, rows), bf16),
        pltpu.VMEM((3, pieces, kv_cols, rows), bf16),
        pltpu.VMEM((8, 128), f32),
        pltpu.VMEM((8, 128), f32),
        pltpu.VMEM((8, 8, 128), f32),
        pltpu.VMEM((pieces, kv_cols, rows), bf16),
        pltpu.VMEM((2, 8, pieces - 1, kv_cols, rows), bf16),
        pltpu.VMEM((16, kv_cols, rows), bf16),
        pltpu.VMEM((count // 128, 128), f32),
        pltpu.VMEM((count, HD), f32),
        pltpu.VMEM((count, HD), f32),
        pltpu.VMEM((count, HD), f32),
        pltpu.VMEM((count, depth), bf16),
        pltpu.VMEM((1, depth), f32),
        pltpu.VMEM((1, HD + kv_cols), f32),
        pltpu.VMEM((1, HD), f32),
        dma((count // 128 + 3,)),
        dma((2, 2)),
        dma,
        dma,
        pltpu.SemaphoreType.REGULAR((5,)),
        dma((2,)),
        dma((2,)),
        dma((8,)),
        dma((2, 2, 2)),
        dma((2, 2)),
        dma((2, 2)),
        dma,
        dma((pieces,)),
        dma,
        dma((pieces + 1,)),
        dma((2,)),
        dma((2, pieces)),
        dma,
        dma((pieces,)),
        dma((3,)),
        dma((pieces + 1,)),
    ]


def finish_kernel(*refs):
    sources, targets, sems = refs[0:5], refs[5:10], refs[10]
    outs = [pltpu.make_async_copy(sources[i], targets[i], sems.at[i]) for i in range(5)]
    for copy in outs:
        copy.start()
    for copy in outs:
        copy.wait()


def finish(*arrays):
    return pl.pallas_call(
        finish_kernel,
        out_shape=tuple(jax.ShapeDtypeStruct(a.shape, a.dtype) for a in arrays),
        in_specs=[pl.BlockSpec(memory_space=pltpu.VMEM)] * 5,
        out_specs=(pl.BlockSpec(memory_space=pltpu.HBM),) * 5,
        scratch_shapes=[pltpu.SemaphoreType.DMA((5,))], compiler_params=pltpu.CompilerParams(vmem_limit_bytes=2 * 1024 * 1024),
    )(*arrays)


def local(n, groups, hidden, norm_gain, prefix, w_query, w_kv, w_scale):
    count, depth = hidden.shape
    chips = n // 2
    width = depth * n
    grid = n == 16 and groups == 2 and n * KV_COLS_DEV == HD and count == 128 * GRID_PIECES
    pair_index = np.arange(HD) // 2
    freq = jnp.asarray(np.power(rope_base, -(2.0 * pair_index) / HD)[None, :], jnp.float32)
    pieces = HD // KV_COLS_DEV
    vmem = pl.BlockSpec(memory_space=pltpu.VMEM)
    hbm = pl.BlockSpec(memory_space=pltpu.HBM if grid else pl.ANY)
    dma = pltpu.SemaphoreType.DMA
    bf16, f32 = jnp.bfloat16, jnp.float32
    queries, keys, values, payload, row_scale = pl.pallas_call(
        functools.partial(grid_kernel, width) if grid else functools.partial(kernel, n, width),
        out_shape=(
            pltpu.VMEM((count, HD), bf16),
            pltpu.VMEM((count, HD), bf16),
            pltpu.VMEM((count, HD), bf16),
            pltpu.VMEM((count, depth), bf16),
            pltpu.VMEM((count // 128, 128), f32),
        ),
        in_specs=[pl.BlockSpec(memory_space=pltpu.SMEM)]
        + ([hbm] * 6 if grid else [vmem] * 5 + [hbm] * 2),
        out_specs=(vmem,) * 5,
        scratch_shapes=grid_scratch(count, depth) if grid else [
            pltpu.VMEM((chips, count, depth), bf16),
            pltpu.VMEM((chips, depth, 2 * HD), bf16),
            pltpu.VMEM((chips, 32, depth), bf16),
            pltpu.VMEM((count, 2 * HD), f32),
            pltpu.VMEM((count, 32), f32),
            pltpu.VMEM((count, HD), f32),
            pltpu.VMEM((count, 32), f32),
            pltpu.VMEM((8, 128), f32),
            pltpu.VMEM((n, 8, 128), f32),
            pltpu.VMEM((2 * KV_COLS_DEV, count), bf16),
            pltpu.VMEM((pieces, 2 * KV_COLS_DEV, count), bf16),
            pltpu.VMEM((count, HD), f32),
            pltpu.VMEM((count, HD), f32),
            pltpu.VMEM((count, HD), f32),
            dma((chips, 2, PIECES)),
            dma((chips, 2, PIECES)),
            dma((n,)),
            dma((n,)),
            dma((pieces,)),
            dma((pieces,)),
            dma,
            dma((chips,)),
            dma,
            dma,
            dma((chips,)),
            dma((chips,)),
            dma((2,)),
            dma((2,)),
        ],
        compiler_params=pltpu.CompilerParams(
            collective_id=0, has_side_effects=True, vmem_limit_bytes=(60 if grid else 48) * 1024 * 1024
        ),
    )(
        prefix,
        hidden,
        norm_gain[None, :],
        freq,
        *([w_scale[None, :]] if grid else [w_scale[None, :HD], w_scale[None, HD:]]),
        w_query.reshape(n, depth, HD) if grid else w_query.reshape(chips, 2, depth, HD),
        w_kv,
    )
    queries, keys, values, payload, row_scale = finish(queries, keys, values, payload, row_scale)
    return queries, keys, values, payload, row_scale.reshape(count)


def solution(mesh):
    return jax.shard_map(
        functools.partial(local, mesh.shape["tp"], mesh.shape["grp"]),
        mesh=mesh,
        in_specs=(P("grp", "tp"), P("tp"), P("grp"), P(None, "tp"), P("tp", None), P("tp")),
        out_specs=(P("grp", "tp"), P("grp", "tp"), P("grp", "tp"), P("grp", "tp"), P("grp")),
        check_vma=False,
    )
```

```python
import functools

import jax
import jax.numpy as jnp
import numpy as np
from jax import lax
from jax.experimental import pallas as pl
from jax.experimental.pallas import tpu as pltpu
from jax.sharding import PartitionSpec as P

HD = 128
KV_COLS_DEV = 8
norm_eps = 1e-05
tiny_eps = 1e-06
rope_base = 500000.0
PIECES = 2
GRID_PIECES = 4
LATE = 128


def ring_order(chips):
    cols = 1
    while (2 * cols) * (2 * cols) <= chips and chips % (2 * cols) == 0:
        cols *= 2
    rows = chips // cols
    if cols < 2 or rows % 2:
        return list(range(chips))
    order = [0]
    for row in range(rows):
        span = range(1, cols) if row % 2 == 0 else range(cols - 1, 0, -1)
        order += [row * cols + col for col in span]
    order += [row * cols for row in range(rows - 1, 0, -1)]
    return order


def lookup(table, index):
    total = jnp.int32(0)
    for key, value in enumerate(table):
        total = total + jnp.where(index == key, jnp.int32(value), jnp.int32(0))
    return total


def spread(row):
    return jnp.transpose(jnp.broadcast_to(row, (128, 128)))


def kernel(
    n, width, prefix_ref, h_ref, gain_ref, freq_ref, qscale_ref, kvscale_ref, wq_hbm, wkv_hbm,
    q_out, k_out, v_out, payload_out, rs_out,
    gath, wq, wkv, acc, kvacc, part_q, part_kv, stat_own, stats, kv_own, kv_all, inv_col, cosine, sine,
    send_sem, recv_sem, st_send, st_recv, kv_send, kv_recv,
    wl_sem, wkl_sem, wr_send, wr_recv, wkr_send, wkr_recv, ex_send, ex_recv,
):
    me = lax.axis_index("tp")
    chips = n // 2
    core = lax.rem(me, 2)
    chip = me // 2
    mate = me + 1 - 2 * core
    count, depth = h_ref.shape
    half = count // 2
    rows = half // PIECES
    pieces = HD // KV_COLS_DEV
    kv_heads = n // pieces
    order = ring_order(chips)
    place = [order.index(c) for c in range(chips)]
    pos = lookup(place, chip)
    succ = 2 * lookup(order, lax.rem(pos + 1, chips)) + core
    pred = 2 * lookup(order, lax.rem(pos + chips - 1, chips)) + core

    barrier = pltpu.get_barrier_semaphore()

    def greet(d, carry):
        pl.semaphore_signal(barrier, inc=1, device_id={"tp": lax.rem(me + d, n)})
        return carry

    lax.fori_loop(1, n, greet, 0)

    own_wq = pltpu.make_async_copy(wq_hbm.at[:, core], wq.at[:, :, pl.ds(0, HD)], wl_sem)
    own_wq.start()

    def kv_local(k):
        cols = pl.ds(pl.multiple_of((2 * k + core) * depth, 128), depth)
        return pltpu.make_async_copy(wkv_hbm.at[:, cols], wkv.at[k, pl.ds(0, 16)], wkl_sem.at[k])

    def kv_remote(k):
        cols = pl.ds(pl.multiple_of((2 * k + 1 - core) * depth, 128), depth)
        return pltpu.make_async_remote_copy(
            wkv_hbm.at[:, cols], wkv.at[k, pl.ds(16, 16)], wkr_send.at[k], wkr_recv.at[k],
            device_id={"tp": mate},
        )

    mate_wq = pltpu.make_async_remote_copy(
        wq_hbm.at[:, 1 - core], wq.at[:, :, pl.ds(HD, HD)], wr_send, wr_recv, device_id={"tp": mate}
    )
    lax.fori_loop(0, chips, lambda k, c: (kv_local(k).start(), c)[1], 0)

    gain = gain_ref[...]
    for r in range(count // 128):
        block = pl.ds(r * 128, 128)
        wide = h_ref[block, :].astype(jnp.float32)
        weighted = wide * gain
        gath[0, block, :] = weighted.astype(jnp.bfloat16)
        square = jnp.sum(wide * wide, axis=1, keepdims=True)
        top = jnp.max(jnp.abs(weighted), axis=1, keepdims=True)
        stat_own[pl.ds(r, 1), :] = jnp.transpose(jnp.broadcast_to(square, (128, 128)))[0:1, :]
        stat_own[pl.ds(4 + r, 1), :] = jnp.transpose(jnp.broadcast_to(top, (128, 128)))[0:1, :]
    stats[me] = stat_own[...]

    pl.semaphore_wait(barrier, n - 1)

    def hop(step, way, piece):
        block = pl.ds(way * half + piece * rows, rows)
        return pltpu.make_async_remote_copy(
            gath.at[step, block], gath.at[step + 1, block],
            send_sem.at[step, way, piece], recv_sem.at[step, way, piece],
            device_id={"tp": succ if way == 0 else pred},
        )

    def multiply(step, way, piece):
        block = pl.ds(way * half + piece * rows, rows)
        shift = chips - step if way == 0 else step
        owner = lookup(order, lax.rem(pos + shift, chips))
        left = gath[step, block, :]
        acc[block, :] += jnp.dot(left, wq[owner], preferred_element_type=jnp.float32)
        kvacc[block, :] += lax.dot_general(
            left, wkv[owner], (((1,), (1,)), ((), ())), preferred_element_type=jnp.float32
        )

    for piece in range(PIECES):
        for way in range(2):
            hop(0, way, piece).start()
    mate_wq.start()
    lax.fori_loop(0, chips, lambda k, c: (kv_remote(k).start(), c)[1], 0)

    def stat_copy(d):
        return pltpu.make_async_remote_copy(
            stat_own, stats.at[me], st_send.at[d], st_recv.at[d], device_id={"tp": lax.rem(me + d, n)}
        )

    lax.fori_loop(1, n, lambda d, c: (stat_copy(d).start(), c)[1], 0)

    acc[...] = jnp.zeros_like(acc)
    kvacc[...] = jnp.zeros_like(kvacc)
    token = lax.broadcasted_iota(jnp.int32, (128, HD), 0) + prefix_ref[0]
    freq = freq_ref[...]
    even = lax.rem(lax.broadcasted_iota(jnp.int32, (128, HD), 1), 2) == 0
    for r in range(count // 128):
        angle = (token + r * 128).astype(jnp.float32) * freq
        cosine[pl.ds(r * 128, 128), :] = jnp.cos(angle)
        turn = jnp.sin(angle)
        sine[pl.ds(r * 128, 128), :] = jnp.where(even, -turn, turn)

    lax.fori_loop(1, n, lambda d, c: (stat_copy(d).wait(), c)[1], 0)
    everything = stats[...]
    inverse = 1.0 / jnp.sqrt(jnp.sum(everything[:, 0:4, :], axis=0) / width + norm_eps)
    row_scale = jnp.max(everything[:, 4:8, :], axis=0) * inverse + tiny_eps
    rs_out[...] = row_scale
    for r in range(count // 128):
        block = pl.ds(r * 128, 128)
        inv = spread(inverse[r : r + 1, :])
        inv_col[block, :] = inv
        scale = spread(row_scale[r : r + 1, :])
        for j in range(depth // 128):
            lanes = pl.ds(j * 128, 128)
            weighted = h_ref[block, lanes].astype(jnp.float32) * gain[:, j * 128 : j * 128 + 128]
            payload_out[block, lanes] = (weighted * inv / scale).astype(jnp.bfloat16)

    own_wq.wait()
    lax.fori_loop(0, chips, lambda k, c: (kv_local(k).wait(), c)[1], 0)
    mate_wq.wait()
    lax.fori_loop(0, chips, lambda k, c: (kv_remote(k).wait(), c)[1], 0)

    for piece in range(PIECES):
        for way in range(2):
            multiply(0, way, piece)

    def ring_step(step, carry):
        for piece in range(PIECES):
            for way in range(2):
                hop(step - 1, way, piece).wait_recv()
                hop(step, way, piece).start()
                multiply(step, way, piece)
        return carry

    lax.fori_loop(1, chips - 1, ring_step, 0)
    for piece in range(PIECES):
        for way in range(2):
            hop(chips - 2, way, piece).wait_recv()
            multiply(chips - 1, way, piece)

    ex_kv = pltpu.make_async_remote_copy(
        kvacc, part_kv, ex_send.at[0], ex_recv.at[0], device_id={"tp": mate}
    )
    ex_q = pltpu.make_async_remote_copy(
        acc.at[:, pl.ds(HD, HD)], part_q, ex_send.at[1], ex_recv.at[1], device_id={"tp": mate}
    )
    ex_kv.start()
    ex_q.start()

    def drain(step, carry):
        for piece in range(PIECES):
            for way in range(2):
                hop(step, way, piece).wait_send()
        return carry

    lax.fori_loop(0, chips - 1, drain, 0)
    ex_kv.wait()
    kvscale = kvscale_ref[...]
    for r in range(count // 128):
        block = pl.ds(r * 128, 128)
        cols = (kvacc[block, 0:16] + part_kv[block, 16:32]) * inv_col[block, 0:16] * kvscale
        cols = jnp.concatenate([cols, jnp.zeros((128, 112), jnp.float32)], axis=1)
        kv_own[:, block] = jnp.transpose(cols)[0:16, :].astype(jnp.bfloat16)

    my_head = me * kv_heads // n
    group = lax.rem(me, kv_heads)
    slot = me // kv_heads

    def kv_copy(i):
        return pltpu.make_async_remote_copy(
            kv_own, kv_all.at[slot], kv_send.at[i], kv_recv.at[slot],
            device_id={"tp": group * pieces + i},
        )

    def kv_arrival(i):
        return pltpu.make_async_remote_copy(
            kv_own, kv_all.at[i], kv_send.at[i], kv_recv.at[i], device_id={"tp": mate}
        )

    def kv_start(i, carry):
        @pl.when(group * pieces + i != me)
        def _():
            kv_copy(i).start()

        return carry

    def kv_wait(i, carry):
        @pl.when(group * pieces + i != me)
        def _():
            kv_copy(i).wait_send()

        @pl.when(i * kv_heads + my_head != me)
        def _():
            kv_arrival(i).wait_recv()

        return carry

    @pl.when(my_head == group)
    def _():
        kv_all[slot] = kv_own[...]

    lax.fori_loop(0, pieces, kv_start, 0)

    def rotated(x, block):
        swapped = jnp.where(even, pltpu.roll(x, HD - 1, 1), pltpu.roll(x, 1, 1))
        return (x * cosine[block, :] + swapped * sine[block, :]).astype(jnp.bfloat16)

    ex_q.wait()
    qscale = qscale_ref[...]
    for r in range(count // 128):
        block = pl.ds(r * 128, 128)
        x = (acc[block, 0:HD] + part_q[block, :]) * inv_col[block, :] * qscale
        q_out[block, :] = rotated(x, block)

    lax.fori_loop(0, pieces, kv_wait, 0)
    for r in range(count // 128):
        block = pl.ds(r * 128, 128)
        both = kv_all[:, :, block].astype(jnp.float32)
        keys = jnp.transpose(both[:, 0:KV_COLS_DEV, :].reshape(HD, 128))
        k_out[block, :] = rotated(keys, block)
        values = jnp.transpose(both[:, KV_COLS_DEV:, :].reshape(HD, 128))
        v_out[block, :] = values.astype(jnp.bfloat16)


def grid_kernel(
    width, prefix_ref, h_hbm, gain_hbm, freq_hbm, scale_hbm, wq_hbm, wkv_hbm,
    q_out, k_out, v_out, payload_out, rs_out,
    gath, wq, wkv, wq_late, acc, kvacc, q_give, q_got, kv_give, kv_got,
    stat_own, stat_mate, stats, kv_own, kv_all, kv_tail, inv_row, inv_col, cosine, sine,
    h_ref, gain_ref, scale_ref, freq_ref, in_sem, own_sem, late_send, late_recv, met,
    st_send, st_recv, w_send, w_recv, wx_recv, wy_recv, act_send, act_recv, mate_send, mate_recv,
    pq_send, pq_recv, pkv_send, pkv_recv, kv_send, kv_recv,
):
    n = 16
    me = lax.axis_index("tp")
    side = lax.axis_index("grp")
    core = lax.rem(me, 2)
    chip = me // 2
    y = lax.rem(chip, 2)
    z = chip // 2
    mate = me + 1 - 2 * core
    is_end = (z == 0) | (z == 3)
    is_mid = (z == 1) | (z == 2)
    inner = z + 1 - 2 * lax.rem(z, 2)
    across = me + 4 * (3 - 2 * z)
    beside = me + 2 - 4 * y
    peers = [me, beside, me + 4 * (inner - z), beside + 4 * (inner - z)]
    places = [(z, y), (z, 1 - y), (inner, y), (inner, 1 - y)]
    count, depth = h_ref.shape
    kv_cols = 2 * KV_COLS_DEV
    rows = count // GRID_PIECES
    everyone = range(GRID_PIECES)
    last = GRID_PIECES - 1

    barrier = pltpu.get_barrier_semaphore()

    for peer in [mate] + peers[1:3]:
        pl.semaphore_signal(barrier, inc=1, device_id={"tp": peer})
    pl.semaphore_signal(barrier, inc=1, device_id={"grp": 1 - side, "tp": me})

    @pl.when(is_mid)
    def _():
        pl.semaphore_signal(barrier, inc=1, device_id={"tp": across})

    loads = [pltpu.make_async_copy(gain_hbm, gain_ref, in_sem.at[0])]
    for r in range(count // 128):
        block = pl.ds(r * 128, 128)
        loads.append(pltpu.make_async_copy(h_hbm.at[block], h_ref.at[block], in_sem.at[r + 1]))
    loads.append(pltpu.make_async_copy(scale_hbm, scale_ref, in_sem.at[count // 128 + 1]))
    loads.append(pltpu.make_async_copy(freq_hbm, freq_ref, in_sem.at[count // 128 + 2]))
    for load in loads:
        load.start()

    def weights(s, k, half, kv):
        zt, yt = places[s]
        block = 2 * (2 * (zt + k * (3 - 2 * zt)) + yt) + half
        if not kv:
            first = pl.ds(0, depth - LATE if s == 2 and k else depth)
            return wq_hbm.at[block, first], wq.at[k, half, first, pl.ds(s * HD, HD)]
        cols = pl.ds(pl.multiple_of(block * depth, 128), depth)
        return wkv_hbm.at[:, cols], wkv.at[k, half, pl.ds(s * kv_cols, kv_cols)]

    def weights_own(k, half, kv):
        source, target = weights(0, k, half, kv)
        return pltpu.make_async_copy(source, target, own_sem.at[k, kv])

    def weights_beside(k, half, kv):
        source, target = weights(1, k, half, kv)
        return pltpu.make_async_remote_copy(
            source, target, w_send.at[kv], wy_recv.at[k, kv], device_id={"tp": beside}
        )

    def weights_far(s, k, kv):
        source, target = weights(s, k, side, kv)
        return pltpu.make_async_remote_copy(
            source, target, w_send.at[4 if kv else 2 + k], w_recv.at[s - 2, k, kv], device_id={"tp": peers[s]}
        )

    def weights_twin(s, k, kv):
        piece = weights(s, k, side, kv)[1]
        return pltpu.make_async_remote_copy(
            piece, piece, w_send.at[7 if kv else 5 + k], wx_recv.at[k, kv], device_id={"grp": 1 - side, "tp": me}
        )

    def weights_late(half):
        block = 2 * (2 * (inner + 3 - 2 * inner) + y) + half
        return pltpu.make_async_remote_copy(
            wq_hbm.at[block, pl.ds(depth - LATE, LATE)], wq_late.at[half], late_send, late_recv,
            device_id={"tp": peers[2]},
        )

    def every(ref, send_sem, recv_sem):
        return pltpu.make_async_remote_copy(ref, ref, send_sem, recv_sem, device_id={"tp": mate})

    def shared_q(k):
        return wq.at[k, :, pl.ds(0, depth - k * LATE // 2), pl.ds(0, HD)]

    def weights_arrive(k):
        for kv in (1, 0):
            whole = wkv.at[k, :, pl.ds(0, kv_cols)] if kv else wq.at[k, :, :, pl.ds(0, HD)]
            for sem in (own_sem, wy_recv):
                every(whole, sem.at[k, kv], sem.at[k, kv]).wait_recv()
            every(whole if kv else shared_q(k), wx_recv.at[k, kv], wx_recv.at[k, kv]).wait_recv()

    for k in range(2):
        for half in range(2):
            for kv in range(2):
                weights_own(k, half, kv).start()

    wq[1, :, depth - LATE :, 2 * HD : 3 * HD] = jnp.zeros((2, LATE, HD), jnp.bfloat16)
    @pl.when(is_mid)
    def _():
        pl.semaphore_wait(barrier, 5)

    @pl.when(is_end)
    def _():
        pl.semaphore_wait(barrier, 4)

    forwarded = [(2, 0, 1), (2, 0, 0), (3, 0, 1), (3, 0, 0), (2, 1, 1), (3, 1, 1), (2, 1, 0), (3, 1, 0)]

    def weights_beside_all(k, kv):
        for half in range(2):
            weights_beside(k, half, kv).start()

    for each in forwarded[:2]:
        weights_far(*each).start()
    weights_beside_all(0, 1)
    pl.semaphore_signal(met.at[0], inc=1, device_id={"tp": mate})
    pl.semaphore_signal(met.at[4], inc=1, device_id={"tp": beside})

    loads[0].wait()
    gain = gain_ref[...]
    for r in range(count // 128):
        block = pl.ds(r * 128, 128)
        loads[r + 1].wait()
        wide = h_ref[block, :].astype(jnp.float32)
        weighted = wide * gain
        gath[core, block, :] = weighted.astype(jnp.bfloat16)
        square = jnp.sum(wide * wide, axis=1, keepdims=True)
        top = jnp.max(jnp.abs(weighted), axis=1, keepdims=True)
        stat_own[pl.ds(r, 1), :] = jnp.transpose(jnp.broadcast_to(square, (128, 128)))[0:1, :]
        stat_own[pl.ds(4 + r, 1), :] = jnp.transpose(jnp.broadcast_to(top, (128, 128)))[0:1, :]
    loads[-2].wait()
    loads[-1].wait()

    def stat_pair():
        return pltpu.make_async_remote_copy(
            stat_own, stat_mate, st_send.at[0], st_recv.at[0], device_id={"tp": mate}
        )

    def stat_copy(d):
        return pltpu.make_async_remote_copy(
            stats.at[chip], stats.at[chip], st_send.at[1], st_recv.at[1],
            device_id={"tp": lax.rem(me + 2 * d, n)},
        )

    def stat_all():
        others = stats.at[pl.ds(1, n // 2 - 1)]
        return pltpu.make_async_remote_copy(
            others, others, st_send.at[1], st_recv.at[1], device_id={"tp": mate}
        )

    def act_mate():
        return pltpu.make_async_remote_copy(
            gath.at[core], gath.at[core], mate_send, mate_recv.at[GRID_PIECES],
            device_id={"tp": mate},
        )

    def act_across(p):
        block = pl.ds(p * rows, rows)
        return pltpu.make_async_remote_copy(
            gath.at[core, block], gath.at[2 + core, block], act_send, act_recv.at[p],
            device_id={"tp": across},
        )

    def act_pass(p):
        block = pl.ds(p * rows, rows)
        piece = gath.at[2 + core, block]
        return pltpu.make_async_remote_copy(
            piece, piece, mate_send, mate_recv.at[p], device_id={"tp": mate}
        )

    stat_pair().start()
    pl.semaphore_wait(met.at[4], 1)
    for each in forwarded[2:4]:
        weights_far(*each).start()

    @pl.when(is_mid)
    def _():
        pl.semaphore_signal(met.at[1], inc=1, device_id={"tp": across})
        for p in everyone:
            act_across(p).start()

    pl.semaphore_wait(met.at[0], 1)

    @pl.when(is_mid)
    def _():
        pl.semaphore_wait(met.at[1], 1)

    pl.semaphore_signal(met.at[2], inc=1, device_id={"tp": mate})
    pl.semaphore_wait(met.at[2], 1)

    @pl.when(is_mid)
    def _():
        pl.semaphore_signal(met.at[3], inc=1, device_id={"tp": peers[2]})

    @pl.when(is_end)
    def _():
        pl.semaphore_wait(met.at[3], 1)

    stat_pair().wait()
    mine, other = stat_own[...], stat_mate[...]
    stats[chip, 0:4] = mine[0:4] + other[0:4]
    stats[chip, 4:8] = jnp.maximum(mine[4:8], other[4:8])
    lax.fori_loop(1, n // 2, lambda d, c: (stat_copy(d).start(), c)[1], 0)
    for each in forwarded[4:]:
        weights_far(*each).start()

    act_mate().start()
    weights_beside_all(0, 0)
    weights_beside_all(1, 1)
    weights_beside_all(1, 0)

    even = lax.rem(lax.broadcasted_iota(jnp.int32, (128, HD), 1), 2) == 0
    token = lax.broadcasted_iota(jnp.int32, (128, HD), 0) + prefix_ref[0]
    freq = freq_ref[...]
    for r in range(count // 128):
        angle = (token + r * 128).astype(jnp.float32) * freq
        cosine[pl.ds(r * 128, 128), :] = jnp.cos(angle)
        turn = jnp.sin(angle)
        sine[pl.ds(r * 128, 128), :] = jnp.where(even, -turn, turn)

    for each in forwarded:
        weights_far(*each).wait_recv()
        weights_twin(*each).start()

    @pl.when(is_end)
    def _():
        for p in everyone:
            act_across(p).start()


    stat_all().wait()
    everything = stats[...]
    inverse = 1.0 / jnp.sqrt(jnp.sum(everything[:, 0:4, :], axis=0) / width + norm_eps)
    row_scale = jnp.max(everything[:, 4:8, :], axis=0) * inverse + tiny_eps
    rs_out[...] = row_scale
    inv_row[...] = inverse
    for r in range(count // 128):
        block = pl.ds(r * 128, 128)
        inv = spread(inverse[r : r + 1, :])
        inv_col[block, :] = inv
        scale = spread(row_scale[r : r + 1, :])
        for j in range(depth // 128):
            lanes = pl.ds(j * 128, 128)
            weighted = h_ref[block, lanes].astype(jnp.float32) * gain_ref[:, lanes]
            payload_out[block, lanes] = (weighted * inv / scale).astype(jnp.bfloat16)

    @pl.when(is_mid)
    def _():
        for p in everyone:
            act_across(p).wait_recv()
            act_pass(p).start()

    act_mate().wait_recv()
    weights_arrive(0)

    def product(slot, block, k, half):
        return jnp.dot(gath[slot, block, :], wq[k, half], preferred_element_type=jnp.float32)

    def kv_product(slot, block, k, half):
        return lax.dot_general(
            wkv[k, half], gath[slot, block, :], (((1,), (1,)), ((), ())), preferred_element_type=jnp.float32
        )

    for p in everyone:
        block = pl.ds(p * rows, rows)
        kvacc[p] = kv_product(0, block, 0, 0) + kv_product(1, block, 0, 1)
        acc[block, :] = product(0, block, 0, 0) + product(1, block, 0, 1)

    weights_arrive(1)

    def q_beside(p):
        block = pl.ds(p * rows, rows)
        return pltpu.make_async_remote_copy(
            q_give.at[pl.ds(0, 2), block], q_got.at[pl.ds(0, 2), block], pq_send.at[0], pq_recv.at[0, p],
            device_id={"tp": beside},
        )

    def q_along(p):
        block = pl.ds(p * rows, rows)
        return pltpu.make_async_remote_copy(
            q_give.at[2, block], q_got.at[2, block], pq_send.at[1], pq_recv.at[1, p],
            device_id={"tp": peers[2]},
        )

    def kv_partial(s, p):
        return pltpu.make_async_remote_copy(
            kv_give.at[s - 1, p], kv_got.at[s - 1, p], pkv_send, pkv_recv.at[p],
            device_id={"tp": peers[s]},
        )

    def near(p):
        block = pl.ds(p * rows, rows)
        kvacc[p] += kv_product(2 + core, block, 1, core)
        acc[block, :] += product(2 + core, block, 1, core)

    def far(p):
        block = pl.ds(p * rows, rows)
        act_pass(p).wait_recv()
        pair = kvacc[p] + kv_product(3 - core, block, 1, 1 - core)
        kvacc[p] = pair
        for s in range(1, 4):
            kv_give[s - 1, p] = pair[s * kv_cols : (s + 1) * kv_cols, :].astype(jnp.bfloat16)
        for s in range(1, 4):
            kv_partial(s, p).start()
        whole = acc[block, :] + product(3 - core, block, 1, 1 - core)
        acc[block, :] = whole
        q_give[0, block, :] = whole[:, HD : 2 * HD].astype(jnp.bfloat16)
        q_give[1, block, :] = whole[:, 3 * HD :].astype(jnp.bfloat16)
        q_beside(p).start()

    def late_arrive():
        every(wq_late, late_recv, late_recv).wait_recv()

    def q_combine(p):
        block = pl.ds(p * rows, rows)
        x = acc[block, 2 * HD : 3 * HD]
        for half in range(2):
            x = x + jnp.dot(
                gath[2 + half, block, depth - LATE :], wq_late[half], preferred_element_type=jnp.float32
            )
        q_beside(p).wait_recv()
        q_give[2, block, :] = (x + q_got[1, block, :].astype(jnp.float32)).astype(jnp.bfloat16)
        q_along(p).start()

    kv_scale = jnp.concatenate([scale_ref[:, HD:], jnp.zeros((1, 128 - kv_cols), jnp.float32)], axis=1)
    kv_scale = spread(kv_scale)[0:kv_cols, :]
    qscale = scale_ref[:, 0:HD]

    def kv_copy(p, d):
        return pltpu.make_async_remote_copy(
            kv_own.at[p], kv_tail.at[me] if p == last else kv_all.at[core, chip, p], kv_send.at[int(p == last)], kv_recv.at[p],
            device_id={"tp": lax.rem(me + d, n)},
        )

    kv_final = kv_tail.at[pl.ds(1, n - 1)]
    kv_mine = kv_all.at[core, :, pl.ds(0, last)]
    kv_spread_all = pltpu.make_async_remote_copy(
        kv_mine, kv_mine, kv_send.at[2], kv_recv.at[GRID_PIECES], device_id={"tp": mate}
    )

    def kv_reduce(p):
        total = kvacc[p, 0:kv_cols, :]
        every(kv_got.at[:, p], pkv_send, pkv_recv.at[p]).wait_recv()
        for s in range(1, 4):
            total = total + kv_got[s - 1, p].astype(jnp.float32)
        mine = (total * inv_row[p : p + 1, :] * kv_scale).astype(jnp.bfloat16)
        kv_own[p] = mine
        if p == last:
            kv_tail[me] = mine
            lax.fori_loop(1, n, lambda d, c: (kv_copy(p, d).start(), c)[1], 0)
        else:
            kv_all[core, chip, p] = mine
            lax.fori_loop(1, n // 2, lambda d, c: (kv_copy(p, 2 * d).start(), c)[1], 0)

    def rotated(x, block):
        swapped = jnp.where(even, pltpu.roll(x, HD - 1, 1), pltpu.roll(x, 1, 1))
        return (x * cosine[block, :] + swapped * sine[block, :]).astype(jnp.bfloat16)

    def q_reduce(p):
        block = pl.ds(p * rows, rows)
        x = acc[block, 0:HD]
        q_along(p).wait_recv()
        x = x + q_got[0, block, :].astype(jnp.float32) + q_got[2, block, :].astype(jnp.float32)
        q_out[block, :] = rotated(x * inv_col[block, :] * qscale, block)

    def heads(p):
        block = pl.ds(p * rows, rows)
        if p == last:
            every(kv_final, kv_send.at[1], kv_recv.at[p]).wait_recv()
        elif p == 0:
            kv_spread_all.wait_recv()
        if p == last:
            pair = kv_tail[...].astype(jnp.float32)
        else:
            both = kv_all[:, :, p].astype(jnp.float32)
            pair = jnp.stack([both[0], both[1]], axis=1).reshape(n, kv_cols, 128)
        keys = jnp.transpose(pair[:, 0:KV_COLS_DEV, :].reshape(HD, 128))
        k_out[block, :] = rotated(keys, block)
        values = jnp.transpose(pair[:, KV_COLS_DEV:, :].reshape(HD, 128))
        v_out[block, :] = values.astype(jnp.bfloat16)

    @pl.when(is_mid)
    def _():
        for p in everyone:
            near(p)
        for p in everyone:
            far(p)
        for half in range(2):
            weights_late(half).start()
        for p in range(last):
            kv_reduce(p)
        late_arrive()
        for p in everyone:
            q_combine(p)
        kv_reduce(last)

    @pl.when(is_end)
    def _():
        for p in everyone:
            act_across(p).wait_recv()
            act_pass(p).start()
            near(p)
            far(p)
            if p == last - 1:
                for half in range(2):
                    weights_late(half).start()
        for p in everyone:
            kv_reduce(p)
        late_arrive()
        for p in everyone:
            q_combine(p)

    for p in range(last):
        every(kv_all.at[0, pl.ds(1, n // 2 - 1), p], kv_recv.at[p], kv_recv.at[p]).wait_recv()
    kv_spread_all.start()
    for p in range(last):
        q_reduce(p)
    every(gath.at[0], act_send, act_send).wait_send()
    every(gath.at[pl.ds(0, 2)], mate_send, mate_send).wait_send()
    for i in (1, 4, 7):
        every(wkv.at[:, :, pl.ds(0, kv_cols)], w_send.at[i], w_send.at[i]).wait_send()
    every(wq.at[:, :, :, pl.ds(0, HD)], w_send.at[0], w_send.at[0]).wait_send()
    for i in (2, 5):
        for k in range(2):
            every(shared_q(k), w_send.at[i + k], w_send.at[i + k]).wait_send()
    every(wq_late, late_send, late_send).wait_send()
    for p in range(last):
        heads(p)
    q_reduce(last)
    every(kv_give, pkv_send, pkv_send).wait_send()
    every(q_give.at[pl.ds(0, 2)], pq_send.at[0], pq_send.at[0]).wait_send()
    every(q_give.at[2], pq_send.at[1], pq_send.at[1]).wait_send()
    every(kv_all.at[0, pl.ds(1, n // 2 - 1)], kv_send.at[0], kv_send.at[0]).wait_send()
    every(kv_final, kv_send.at[1], kv_send.at[1]).wait_send()
    kv_spread_all.wait_send()
    heads(last)


def grid_scratch(count, depth):
    dma = pltpu.SemaphoreType.DMA
    bf16, f32 = jnp.bfloat16, jnp.float32
    pieces, kv_cols = GRID_PIECES, 2 * KV_COLS_DEV
    rows = count // pieces
    return [
        pltpu.VMEM((4, count, depth), bf16),
        pltpu.VMEM((2, 2, depth, 4 * HD), bf16),
        pltpu.VMEM((2, 2, 4 * kv_cols, depth), bf16),
        pltpu.VMEM((2, LATE, HD), bf16),
        pltpu.VMEM((count, 4 * HD), f32),
        pltpu.VMEM((pieces, 4 * kv_cols, rows), f32),
        pltpu.VMEM((3, count, HD), bf16),
        pltpu.VMEM((3, count, HD), bf16),
        pltpu.VMEM((3, pieces, kv_cols, rows), bf16),
        pltpu.VMEM((3, pieces, kv_cols, rows), bf16),
        pltpu.VMEM((8, 128), f32),
        pltpu.VMEM((8, 128), f32),
        pltpu.VMEM((8, 8, 128), f32),
        pltpu.VMEM((pieces, kv_cols, rows), bf16),
        pltpu.VMEM((2, 8, pieces - 1, kv_cols, rows), bf16),
        pltpu.VMEM((16, kv_cols, rows), bf16),
        pltpu.VMEM((count // 128, 128), f32),
        pltpu.VMEM((count, HD), f32),
        pltpu.VMEM((count, HD), f32),
        pltpu.VMEM((count, HD), f32),
        pltpu.VMEM((count, depth), bf16),
        pltpu.VMEM((1, depth), f32),
        pltpu.VMEM((1, HD + kv_cols), f32),
        pltpu.VMEM((1, HD), f32),
        dma((count // 128 + 3,)),
        dma((2, 2)),
        dma,
        dma,
        pltpu.SemaphoreType.REGULAR((5,)),
        dma((2,)),
        dma((2,)),
        dma((8,)),
        dma((2, 2, 2)),
        dma((2, 2)),
        dma((2, 2)),
        dma,
        dma((pieces,)),
        dma,
        dma((pieces + 1,)),
        dma((2,)),
        dma((2, pieces)),
        dma,
        dma((pieces,)),
        dma((3,)),
        dma((pieces + 1,)),
    ]


def finish_kernel(*refs):
    sources, targets, sems = refs[0:5], refs[5:10], refs[10]
    outs = [pltpu.make_async_copy(sources[i], targets[i], sems.at[i]) for i in range(5)]
    for copy in outs:
        copy.start()
    for copy in outs:
        copy.wait()


def finish(*arrays):
    return pl.pallas_call(
        finish_kernel,
        out_shape=tuple(jax.ShapeDtypeStruct(a.shape, a.dtype) for a in arrays),
        in_specs=[pl.BlockSpec(memory_space=pltpu.VMEM)] * 5,
        out_specs=(pl.BlockSpec(memory_space=pltpu.HBM),) * 5,
        scratch_shapes=[pltpu.SemaphoreType.DMA((5,))], compiler_params=pltpu.CompilerParams(vmem_limit_bytes=2 * 1024 * 1024),
    )(*arrays)


def local(n, groups, hidden, norm_gain, prefix, w_query, w_kv, w_scale):
    count, depth = hidden.shape
    chips = n // 2
    width = depth * n
    grid = n == 16 and groups == 2 and n * KV_COLS_DEV == HD and count == 128 * GRID_PIECES
    pair_index = np.arange(HD) // 2
    freq = jnp.asarray(np.power(rope_base, -(2.0 * pair_index) / HD)[None, :], jnp.float32)
    pieces = HD // KV_COLS_DEV
    vmem = pl.BlockSpec(memory_space=pltpu.VMEM)
    hbm = pl.BlockSpec(memory_space=pltpu.HBM if grid else pl.ANY)
    dma = pltpu.SemaphoreType.DMA
    bf16, f32 = jnp.bfloat16, jnp.float32
    queries, keys, values, payload, row_scale = pl.pallas_call(
        functools.partial(grid_kernel, width) if grid else functools.partial(kernel, n, width),
        out_shape=(
            pltpu.VMEM((count, HD), bf16),
            pltpu.VMEM((count, HD), bf16),
            pltpu.VMEM((count, HD), bf16),
            pltpu.VMEM((count, depth), bf16),
            pltpu.VMEM((count // 128, 128), f32),
        ),
        in_specs=[pl.BlockSpec(memory_space=pltpu.SMEM)]
        + ([hbm] * 6 if grid else [vmem] * 5 + [hbm] * 2),
        out_specs=(vmem,) * 5,
        scratch_shapes=grid_scratch(count, depth) if grid else [
            pltpu.VMEM((chips, count, depth), bf16),
            pltpu.VMEM((chips, depth, 2 * HD), bf16),
            pltpu.VMEM((chips, 32, depth), bf16),
            pltpu.VMEM((count, 2 * HD), f32),
            pltpu.VMEM((count, 32), f32),
            pltpu.VMEM((count, HD), f32),
            pltpu.VMEM((count, 32), f32),
            pltpu.VMEM((8, 128), f32),
            pltpu.VMEM((n, 8, 128), f32),
            pltpu.VMEM((2 * KV_COLS_DEV, count), bf16),
            pltpu.VMEM((pieces, 2 * KV_COLS_DEV, count), bf16),
            pltpu.VMEM((count, HD), f32),
            pltpu.VMEM((count, HD), f32),
            pltpu.VMEM((count, HD), f32),
            dma((chips, 2, PIECES)),
            dma((chips, 2, PIECES)),
            dma((n,)),
            dma((n,)),
            dma((pieces,)),
            dma((pieces,)),
            dma,
            dma((chips,)),
            dma,
            dma,
            dma((chips,)),
            dma((chips,)),
            dma((2,)),
            dma((2,)),
        ],
        compiler_params=pltpu.CompilerParams(
            collective_id=0, has_side_effects=True, vmem_limit_bytes=(60 if grid else 48) * 1024 * 1024
        ),
    )(
        prefix,
        hidden,
        norm_gain[None, :],
        freq,
        *([w_scale[None, :]] if grid else [w_scale[None, :HD], w_scale[None, HD:]]),
        w_query.reshape(n, depth, HD) if grid else w_query.reshape(chips, 2, depth, HD),
        w_kv,
    )
    queries, keys, values, payload, row_scale = finish(queries, keys, values, payload, row_scale)
    return queries, keys, values, payload, row_scale.reshape(count)


def solution(mesh):
    return jax.shard_map(
        functools.partial(local, mesh.shape["tp"], mesh.shape["grp"]),
        mesh=mesh,
        in_specs=(P("grp", "tp"), P("tp"), P("grp"), P(None, "tp"), P("tp", None), P("tp")),
        out_specs=(P("grp", "tp"), P("grp", "tp"), P("grp", "tp"), P("grp", "tp"), P("grp")),
        check_vma=False,
    )
```
